32 devices in a mesh: row: 16 (over z, y, x), col: 2 (over core).
Axes of the slice: x: 2, y: 2, z: 4, core: 2. Of those that a mesh axis runs over, the one named last changes fastest.
Arguments:
- eri_cols: float32 [8192, 512], P('row'), as said below
- old_factor: float32 [8192, 1024], P('row', 'col')
- residual_diag: float32 [8192], P('row'), as said below
- pivots: int32 [4, 128], replicated, may hold values from 0 to 8191, as said below
- row_ids: int32 [8192], P('row'), may hold values from 0 to 8191, as said below
Outputs:
- panels: float32 [8192, 512], P('row')
- new_diag: float32 [8192], P('row')
The draws below stay inside these ranges and needn't reach their ends.
Inputs may be any that keep to these rules, and one draw needn't show every extreme that they name: `pivots`: 512 distinct pair indices, each held by some stored row. `row_ids`: every pair index held by exactly one stored row. `eri_cols`: the pair matrix minus the earlier factor's product is symmetric positive definite on the pivots, with smallest eigenvalue 0.25 or more. `residual_diag`: the diagonal of the same residual matrix whose pivot columns eri_cols holds.
All inputs are finite; a program needn't handle non-finite values.
Results may differ from the reference program's by a relative error of at most 0.0003.
Values sent between devices are 32-bit elements; how exact they have to be, the bound alone decides.
A program may use at most 64 MiB of HBM per device.

```python
import math
import jax
import jax.numpy as jnp
from jax import lax

NB = 128
STEPS = 4
KOLD = 1024
PAIRS = 8192
PIVOTS = 512
RANK_W = 640


def integer_parts(key):
    row_ids = jax.random.permutation(jax.random.fold_in(key, 11), PAIRS).astype(jnp.int32)
    places = jax.random.permutation(jax.random.fold_in(key, 12), PAIRS)[:PIVOTS].astype(jnp.int32)
    pivots = row_ids[places].reshape(STEPS, NB)
    return (row_ids, places, pivots)


def float_parts(key):
    row_ids, places, pivots = integer_parts(key)
    old = jax.random.normal(jax.random.fold_in(key, 22), (PAIRS, KOLD)) / math.sqrt(KOLD)
    remain = jax.random.normal(jax.random.fold_in(key, 25), (PAIRS, RANK_W)) / math.sqrt(RANK_W)
    exact = lax.Precision.HIGHEST
    ident = (jnp.arange(PAIRS, dtype=jnp.int32)[:, None] == places[None, :]).astype(jnp.float32)
    eri = jnp.dot(old, old[places].T, precision=exact) + jnp.dot(remain, remain[places].T, precision=exact) + 0.25 * ident
    diagonal = jnp.sum(remain * remain, axis=1) + 0.25
    return (eri.astype(jnp.float32), old.astype(jnp.float32), diagonal.astype(jnp.float32))


def draw_eri_cols(key, part):
    return float_parts(key)[0]


def draw_old_factor(key, part):
    return float_parts(key)[1]


def draw_residual_diag(key, part):
    return float_parts(key)[2]


def draw_pivots(key, part):
    return integer_parts(key)[2]


def draw_row_ids(key, part):
    return integer_parts(key)[0]


def setup_inputs(seed: int = 0) -> dict:
    keys = jax.random.split(jax.random.key(seed), 6)
    eri_cols = draw_eri_cols(jax.random.fold_in(keys[5], 71), 0)
    old_factor = draw_old_factor(jax.random.fold_in(keys[5], 71), 0)
    residual_diag = draw_residual_diag(jax.random.fold_in(keys[5], 71), 0)
    pivots = draw_pivots(jax.random.fold_in(keys[5], 71), 0)
    row_ids = draw_row_ids(jax.random.fold_in(keys[5], 71), 0)
    return dict(eri_cols=eri_cols, old_factor=old_factor, residual_diag=residual_diag, pivots=pivots, row_ids=row_ids)


def reference(eri_cols, old_factor, residual_diag, pivots, row_ids):
    exact = lax.Precision.HIGHEST
    pairs = row_ids.shape[0]
    inverse = jnp.zeros((pairs,), jnp.int32).at[row_ids].set(jnp.arange(pairs, dtype=jnp.int32))
    places = inverse[pivots.reshape(-1).astype(jnp.int32)].astype(jnp.int32)
    old_rows = old_factor[places]
    reduced = eri_cols - jnp.dot(old_factor.astype(jnp.float32), old_rows.T.astype(jnp.float32), precision=exact, preferred_element_type=jnp.float32)
    width = pivots.shape[1]
    diagonal = residual_diag
    outputs = []
    for step in range(pivots.shape[0]):
        wanted = places[step * width:(step + 1) * width]
        columns = reduced[:, step * width:(step + 1) * width]
        if step > 0:
            earlier = jnp.concatenate(outputs, axis=1)
            columns = columns - jnp.dot(earlier.astype(jnp.float32), earlier[wanted].T.astype(jnp.float32), precision=exact, preferred_element_type=jnp.float32)
        factor_block = jnp.linalg.cholesky(columns[wanted])
        new_panel = lax.linalg.triangular_solve(factor_block, columns, left_side=False, lower=True, transpose_a=True)
        diagonal = diagonal - jnp.sum(new_panel * new_panel, axis=1)
        outputs.append(new_panel)
    return (jnp.concatenate(outputs, axis=1), diagonal)
```

```python
import functools
import jax
import jax.numpy as jnp
from jax import lax
from jax.experimental import pallas as pl
from jax.experimental.pallas import tpu as pltpu
from jax.sharding import PartitionSpec as P

ROWS_T = (((1,), (1,)), ((), ()))
COLS_T = (((0,), (0,)), ((), ()))
SUB = 8
LANES = 128
MESH = pl.DeviceIdType.MESH
VMEM = pl.BlockSpec(memory_space=pltpu.VMEM)
SMEM = pl.BlockSpec(memory_space=pltpu.SMEM)
F32 = jnp.float32
BF16 = jnp.bfloat16


def split(x):
    hi = x.astype(BF16)
    return hi, (x - hi.astype(F32)).astype(BF16)


def dot_t(a, b):
    f = functools.partial(
        lax.dot_general, dimension_numbers=ROWS_T, preferred_element_type=F32
    )
    return f(a[0], b[0]) + (f(a[0], b[1]) + f(a[1], b[0]))


def inverse_factor(a):
    n = a.shape[0]
    groups = n // SUB
    row = lax.broadcasted_iota(jnp.int32, (SUB, n), 0)
    lane = lax.broadcasted_iota(jnp.int32, (SUB, n), 1)
    A = [a[SUB * i : SUB * i + SUB, :] for i in range(groups)]
    W = [jnp.where(lane == row + SUB * i, 1.0, 0.0) for i in range(groups)]
    out = []
    wide = lambda v: jnp.broadcast_to(v, (SUB, n))
    for g in range(groups):
        j = SUB * g
        C = [[wide(A[i][:, j + k : j + k + 1]) for k in range(SUB)] for i in range(g, groups)]
        D = [[wide(C[0][l][k : k + 1, :]) for l in range(k + 1)] for k in range(SUB)]
        r = [wide(A[g][k : k + 1, :]) for k in range(SUB)]
        w = [wide(W[g][k : k + 1, :]) for k in range(SUB)]
        inv, m = [], [[None] * SUB for _ in range(SUB)]
        done = jnp.zeros((SUB, n), F32)
        for k in range(SUB):
            root = lax.rsqrt(D[k][k])
            inv.append(root * root)
            done = jnp.where(row == k, w[k] * root, done)
            for i in range(k + 1, SUB):
                m[i][k] = D[i][k] * inv[k]
            for i in range(k + 1, SUB):
                for l in range(k + 1, i + 1):
                    D[i][l] = D[i][l] - m[i][k] * D[l][k]
                r[i] = r[i] - m[i][k] * r[k]
                w[i] = w[i] - m[i][k] * w[k]
        out.append(done)
        if g + 1 == groups:
            break
        s, t = [None] * SUB, [None] * SUB
        for k in reversed(range(SUB)):
            s[k], t[k] = r[k] * inv[k], w[k] * inv[k]
            for i in reversed(range(k + 1, SUB)):
                s[k] = s[k] - m[i][k] * s[i]
                t[k] = t[k] - m[i][k] * t[i]
        for i in range(g + 1, groups):
            c = C[i - g]
            for k in range(SUB):
                A[i] = A[i] - c[k] * s[k]
                W[i] = W[i] - c[k] * t[k]
    return jnp.concatenate(out, axis=0)


def pack_kernel(cap, window_ref, pivot_ref, ids_ref, old_ref, eri_ref, out_ref):
    steps, width = pivot_ref.shape
    slots = out_ref.shape[1]
    part = out_ref.shape[2]
    groups = ids_ref.shape[0]
    half = eri_ref.shape[1] // 2
    ids = ids_ref[...]

    def find(j, at):
        return jnp.where(ids == pivot_ref[j // width, j % width], j + 1, at)

    at = lax.fori_loop(0, steps * width, find, jnp.zeros_like(ids), unroll=16)
    owned = jnp.where(at > 0, 1.0, 0.0)
    below = lax.broadcasted_iota(jnp.int32, (LANES, LANES), 0)
    right = lax.broadcasted_iota(jnp.int32, (LANES, LANES), 1)
    ahead = jnp.where(below < right, 1.0, 0.0).astype(BF16)
    rank = lax.dot_general(
        owned.astype(BF16), ahead, (((1,), (0,)), ((), ())), preferred_element_type=F32
    )
    first = window_ref[0] * cap
    slot = lax.broadcasted_iota(jnp.int32, (slots, LANES), 0)
    passed = jnp.zeros((1, 1), F32)
    picks, numbers = [], []
    for g in range(groups):
        here = (rank[g : g + 1] + passed).astype(jnp.int32) - first
        passed = passed + jnp.sum(owned[g : g + 1], axis=1, keepdims=True)
        here = jnp.where((owned[g : g + 1] > 0) & (here >= 0) & (here < cap), here, -1)
        picks.append(jnp.where(slot == here, 1.0, 0.0))
        numbers.append(at[g : g + 1])
    pick = jnp.concatenate(picks, axis=1).astype(BF16)
    number = jnp.concatenate(numbers, axis=1)
    pair = jnp.concatenate([number // 16, number % 16] + [jnp.zeros_like(number)] * 6, axis=0)
    pair = pair.astype(F32).astype(BF16)
    lines = lax.dot_general(pair, pick, ROWS_T, preferred_element_type=F32)
    line = lines[0:1] * 16.0 + lines[1:2]
    lane = lax.broadcasted_iota(jnp.int32, (1, LANES), 1)
    line = jnp.concatenate([line, jnp.zeros((1, LANES - slots), F32)], axis=1)
    line = jnp.where(lane == LANES - 1, passed, line)

    def take(x):
        f = functools.partial(
            lax.dot_general,
            dimension_numbers=(((1,), (0,)), ((), ())),
            preferred_element_type=F32,
        )
        hi, lo = split(x)
        return f(pick, hi) + f(pick, lo)

    core = lax.axis_index("col")
    out_ref[0] = take(old_ref[:, :part])
    out_ref[0, slots - 1 : slots, :LANES] = line
    rest = old_ref.shape[1] - part
    out_ref[1, :, :rest] = take(old_ref[:, part:])
    out_ref[1, :, rest:] = take(eri_ref[:, pl.ds(pl.multiple_of(core * half, LANES), half)])


def pack(window, pivots, ids, old, eri, slots):
    width = (old.shape[1] + eri.shape[1] // 2) // 2
    return pl.pallas_call(
        functools.partial(pack_kernel, slots - 1),
        out_shape=jax.ShapeDtypeStruct((2, slots, width), F32),
        in_specs=[SMEM, SMEM, VMEM, VMEM, VMEM],
        out_specs=VMEM,
        name="pack",
    )(window, pivots, ids, old, eri)


def spread_kernel(grid, mine_ref, old_ref, all_ref, other_ref, *sems):
    deep, high, wide = grid
    fine = deep * high * wide <= 16
    own_sem, first_send, near_send, far_send, core_send = sems[:5]
    first_recv, recv, core_recv, old_sems = sems[5:]
    me = lax.axis_index("row")
    core = lax.axis_index("col")
    z, y, x = me // (high * wide), me // wide % high, me % wide
    chip = lambda z, y, x: (z * high + y) * wide + x
    steps = lambda at, size: [lax.rem(at + o, size) for o in range(1, size)]
    partner = (me, 1 - core)

    barrier = pltpu.get_barrier_semaphore()
    greet = [(chip(o, y, x), core) for o in steps(z, deep)]
    greet += [(chip(z, o, x), core) for o in steps(y, high)]
    greet += [(chip(z, y, o), core) for o in steps(x, wide)]
    greet.append(partner)
    for device in greet:
        pl.semaphore_signal(barrier, inc=1, device_id=device, device_id_type=MESH)
    pl.semaphore_wait(barrier, len(greet))

    flying = []

    def send(src, dst, send_sem, recv_sem, device):
        copy = pltpu.make_async_remote_copy(
            src_ref=src, dst_ref=dst, send_sem=send_sem, recv_sem=recv_sem,
            device_id=device, device_id_type=MESH,
        )
        copy.start()
        flying.append(copy)

    def await_block(ref, sem):
        pltpu.make_async_remote_copy(
            src_ref=ref, dst_ref=ref, send_sem=sem, recv_sem=sem,
            device_id=partner, device_id_type=MESH,
        ).wait_recv()

    def block(colour, zs, y, x):
        return all_ref.at[core, colour, zs, y, x]

    own = [
        pltpu.make_async_copy(mine_ref.at[k], all_ref.at[core, k, z, y, x], own_sem.at[k])
        for k in range(2)
    ]
    for k in range(2):
        own[k].start()
    for k in range(2):
        for i, o in enumerate(steps(z, deep)):
            send(mine_ref.at[k], block(k, z, y, x), first_send.at[k, i], first_recv.at[k, z], (chip(o, y, x), core))

    chunks = [z] + steps(z, deep) if fine else [None]
    near = lambda k: [(y, o) for o in steps(x, wide)] if k == 0 else [(o, x) for o in steps(y, high)]
    far = lambda k: [(o, x) for o in steps(y, high)] if k == 0 else [(y, o) for o in steps(x, wide)]

    def to_core(k, q, i, zs, y, x):
        ref = block(k, zs, y, x)
        send(ref, ref, core_send.at[k, q, i], core_recv.at[k, chunk_at(zs), y, x], partner)

    def chunk_at(zs):
        return zs if fine else 0

    def rows(zs):
        return zs if fine else slice(None)

    for q, at in enumerate(chunks):
        zs = rows(at)
        mine = fine and q == 0
        for k in range(2):
            if q == 0:
                if not fine:
                    for o in steps(z, deep):
                        await_block(block(k, o, y, x), first_recv.at[k, o])
                    own[k].wait()
            else:
                await_block(block(k, zs, y, x), first_recv.at[k, zs])
            src = mine_ref.at[k] if mine else block(k, zs, y, x)
            sem = recv.at[k, chunk_at(zs), y, x]
            for i, (b, c) in enumerate(near(k)):
                send(src, block(k, zs, y, x), near_send.at[k, q, i], sem, (chip(z, b, c), core))
            for i, (b, c) in enumerate(far(k)):
                send(src, block(k, zs, y, x), far_send.at[k, q, 0, i], sem, (chip(z, b, c), core))
            send(src, block(k, zs, y, x), core_send.at[k, q, 0], core_recv.at[k, chunk_at(zs), y, x], partner)
    old_copy = pltpu.make_async_remote_copy(
        src_ref=old_ref, dst_ref=other_ref, send_sem=old_sems.at[0], recv_sem=old_sems.at[1],
        device_id=partner, device_id_type=MESH,
    )
    old_copy.start()
    flying.append(old_copy)
    for q, at in enumerate(chunks):
        zs = rows(at)
        for k in range(2):
            for n, (b, c) in enumerate(near(k)):
                ref = block(k, zs, b, c)
                await_block(ref, recv.at[k, chunk_at(zs), b, c])
                for i, (fb, fc) in enumerate(far(k)):
                    send(ref, ref, far_send.at[k, q, 1 + n, i], recv.at[k, chunk_at(zs), b, c], (chip(z, fb, fc), core))
                to_core(k, q, 1 + n, zs, b, c)
    for q, at in enumerate(chunks):
        zs = rows(at)
        for k in range(2):
            index = 1 + len(near(k))
            for fb, fc in far(k):
                for b, c in [(y, x)] + near(k):
                    there = (fb, c) if k == 0 else (b, fc)
                    ref = block(k, zs, *there)
                    await_block(ref, recv.at[k, chunk_at(zs), *there])
                    to_core(k, q, index, zs, *there)
                    index += 1
    if fine:
        for k in range(2):
            own[k].wait()
    for q, at in enumerate(chunks):
        zs = rows(at)
        for k in range(2):
            for b in range(high):
                for c in range(wide):
                    ref = all_ref.at[1 - core, k, zs, b, c]
                    await_block(ref, core_recv.at[k, chunk_at(zs), b, c])
    old_copy.wait_recv()
    for copy in flying:
        copy.wait_send()


def spread(grid, mine, old):
    deep, high, wide = grid
    _, slots, width = mine.shape
    chunks = deep if deep * high * wide <= 16 else 1
    cells = high * wide
    peers = max(high, wide)
    sem = pltpu.SemaphoreType.DMA
    return pl.pallas_call(
        functools.partial(spread_kernel, grid),
        out_shape=(
            jax.ShapeDtypeStruct((2, 2, deep, high, wide, slots, width), F32),
            jax.ShapeDtypeStruct(old.shape, F32),
        ),
        in_specs=[pl.BlockSpec(memory_space=pl.ANY)] * 2,
        out_specs=(VMEM, pl.BlockSpec(memory_space=pl.ANY)),
        scratch_shapes=[
            sem((2,)),
            sem((2, max(deep - 1, 1))),
            sem((2, chunks, max(peers - 1, 1))),
            sem((2, chunks, peers, max(peers - 1, 1))),
            sem((2, chunks, cells)),
            sem((2, deep)),
            sem((2, chunks, high, wide)),
            sem((2, chunks, high, wide)),
            sem((2,)),
        ],
        compiler_params=pltpu.CompilerParams(
            collective_id=0, has_side_effects=True, vmem_limit_bytes=48 * 1024 * 1024
        ),
        name="spread",
    )(mine, old)


def finish_kernel(
    steps, chips, all_ref, own_ref, other_ref, eri_ref, diag_ref, panel_ref, new_ref,
    work, old_hi, old_lo,
):
    rows, piv = eri_ref.shape
    width = piv // steps
    part = all_ref.shape[3]
    slots = all_ref.shape[2] // chips
    half = own_ref.shape[1]
    core = lax.axis_index("col")
    f = functools.partial(lax.dot_general, preferred_element_type=F32)

    line = [all_ref[0, 0, slots * i + slots - 1 : slots * (i + 1), :LANES] for i in range(chips)]
    if chips < LANES:
        line.append(jnp.zeros((LANES - chips, LANES), F32))
    line = jnp.concatenate(line, axis=0)
    held = jnp.transpose(line)
    number = lax.broadcasted_iota(jnp.int32, (slots, piv), 1).astype(F32) + 1.0
    place = jnp.concatenate(
        [
            jnp.where(jnp.broadcast_to(held[:slots, i : i + 1], (slots, piv)) == number, 1.0, 0.0)
            for i in range(chips)
        ],
        axis=0,
    ).astype(BF16)
    for c in range(2):
        for k in range(2):
            hi, lo = split(all_ref[c, k])
            hi = f(place, hi, COLS_T)
            lo = f(place, lo, COLS_T)
            if k == 0:
                old_hi[c, :, :part] = hi.astype(BF16)
                old_lo[c, :, :part] = lo.astype(BF16)
            else:
                rest = half - part
                old_hi[c, :, part:] = hi[:, :rest].astype(BF16)
                old_lo[c, :, part:] = lo[:, :rest].astype(BF16)
                eri = piv // 2
                work[:piv, c * eri : (c + 1) * eri] = hi[:, rest:] + lo[:, rest:]
    both = [(old_hi[c], old_lo[c]) for c in range(2)]
    work[:piv, :] = work[:piv, :] - (dot_t(both[0], both[0]) + dot_t(both[1], both[1]))
    mine = (old_hi[core], old_lo[core])
    theirs = (old_hi[1 - core], old_lo[1 - core])
    work[piv:, :] = eri_ref[...] - (
        dot_t(split(own_ref[...]), mine) + dot_t(split(other_ref[...]), theirs)
    )
    new_ref[...] = diag_ref[...]
    ones = jnp.ones((SUB, width), BF16)

    def step(s, carry):
        at = pl.ds(pl.multiple_of(s * width, width), width)
        inv = split(inverse_factor(work[at, at]))
        solved = dot_t(split(work[:, at]), inv)
        own = solved[piv:]
        panel_ref[:, at] = own
        hi, lo = split(own * own)
        new_ref[...] -= (f(ones, hi, ROWS_T) + f(ones, lo, ROWS_T))[:1]

        @pl.when(s < steps - 1)
        def _():
            both = split(solved)
            work[...] -= dot_t(both, (both[0][:piv], both[1][:piv]))

        return carry

    lax.fori_loop(0, steps, step, 0)


def finish(steps, chips, everything, own, other, eri, diagonal):
    rows, piv = eri.shape
    panels, new = pl.pallas_call(
        functools.partial(finish_kernel, steps, chips),
        out_shape=(
            jax.ShapeDtypeStruct((rows, piv), F32),
            jax.ShapeDtypeStruct((1, rows), F32),
        ),
        in_specs=[VMEM] * 5,
        out_specs=[VMEM] * 2,
        scratch_shapes=[
            pltpu.VMEM((piv + rows, piv), F32),
            pltpu.VMEM((2, piv, own.shape[1]), BF16),
            pltpu.VMEM((2, piv, own.shape[1]), BF16),
        ],
        compiler_params=pltpu.CompilerParams(vmem_limit_bytes=56 * 1024 * 1024),
        name="finish",
    )(everything, own, other, eri, diagonal[None, :])
    return panels, new[0]


def torus(chips):
    side = 1
    while 2 * (side + 1) ** 3 <= chips:
        side += 1
    return (2 * side, side, side) if 2 * side**3 == chips else (chips, 1, 1)


def slots_for(pivots, chips):
    mean = -(-pivots // chips)
    return min(LANES - 8, -(-(mean + max(12, mean // 2)) // 16) * 16)


def on_device(grid, eri_cols, old_factor, residual_diag, pivots, row_ids):
    steps, width = pivots.shape
    piv = steps * width
    chips = grid[0] * grid[1] * grid[2]
    slots = slots_for(piv, chips)
    cap = slots - 1
    ids = row_ids.reshape(-1, LANES)

    def gather(window):
        mine = pack(jnp.full((1,), window, jnp.int32), pivots, ids, old_factor, eri_cols, slots)
        everything, other = spread(grid, mine, old_factor)
        return everything.reshape(2, 2, chips * slots, -1), other

    def line_of(everything):
        return everything[0, 0].reshape(chips, slots, -1)[:, slots - 1, :LANES]

    everything, other = gather(0)
    most = jnp.max(line_of(everything)[:, LANES - 1]).astype(jnp.int32)
    windows = (most + cap - 1) // cap

    def placed(everything):
        number = line_of(everything)[:, :slots].reshape(-1)
        one = lax.broadcasted_iota(jnp.int32, (piv, chips * slots), 0) + 1 == number[None, :].astype(jnp.int32)
        filled = jnp.arange(chips * slots) % slots < cap
        dot = functools.partial(jnp.einsum, "ps,abse->abpe", precision=lax.Precision.HIGHEST)
        return dot(jnp.where(one & filled[None, :], 1.0, 0.0), everything)

    def more(state):
        _, everything = state
        rows = lax.fori_loop(
            1, windows, lambda w, rows: rows + placed(gather(w)[0]), placed(everything)
        )
        rows = jnp.pad(rows, ((0, 0), (0, 0), (0, chips * cap - piv), (0, 0)))
        rows = rows.reshape(2, 2, chips, cap, -1)
        number = jnp.arange(chips * cap) + 1
        number = jnp.where(number <= piv, number, 0).reshape(chips, cap).astype(F32)
        line = jnp.pad(number, ((0, 0), (0, rows.shape[-1] - cap)))
        line = jnp.broadcast_to(line[None, None, :, None], (2, 2, chips, 1, rows.shape[-1]))
        rows = jnp.concatenate([rows, line], axis=3)
        return jnp.bool_(False), rows.reshape(everything.shape)

    _, everything = lax.while_loop(lambda s: s[0], more, (windows > 1, everything))
    return finish(steps, chips, everything, old_factor, other, eri_cols, residual_diag)


def solution(mesh):
    grid = torus(mesh.shape["row"])
    placed = (P("row", None), P("row", "col"), P("row"), P(), P("row"))
    return jax.shard_map(
        functools.partial(on_device, grid),
        mesh=mesh, in_specs=placed, out_specs=(P("row", None), P("row")), check_vma=False,
    )
```

```python
import functools
import jax
import jax.numpy as jnp
from jax import lax
from jax.experimental import pallas as pl
from jax.experimental.pallas import tpu as pltpu
from jax.sharding import PartitionSpec as P

ROWS_T = (((1,), (1,)), ((), ()))
COLS_T = (((0,), (0,)), ((), ()))
SUB = 8
LANES = 128
MESH = pl.DeviceIdType.MESH
VMEM = pl.BlockSpec(memory_space=pltpu.VMEM)
SMEM = pl.BlockSpec(memory_space=pltpu.SMEM)
F32 = jnp.float32
BF16 = jnp.bfloat16


def split(x):
    hi = x.astype(BF16)
    return hi, (x - hi.astype(F32)).astype(BF16)


def dot_t(a, b):
    f = functools.partial(
        lax.dot_general, dimension_numbers=ROWS_T, preferred_element_type=F32
    )
    return f(a[0], b[0]) + (f(a[0], b[1]) + f(a[1], b[0]))


def inverse_factor(a):
    n = a.shape[0]
    groups = n // SUB
    row = lax.broadcasted_iota(jnp.int32, (SUB, n), 0)
    lane = lax.broadcasted_iota(jnp.int32, (SUB, n), 1)
    M = [a[SUB * i : SUB * i + SUB, :] for i in range(groups)]
    over = lambda v, k: jnp.broadcast_to(v[k : k + 1, :], (SUB, n))
    columns = lambda v, j: [jnp.broadcast_to(v[:, j + k : j + k + 1], (SUB, n)) for k in range(SUB)]
    out = []
    V = columns(M[0], 0)
    for g in range(groups):
        j = SUB * g
        ahead = g + 1 < groups
        if ahead:
            U = columns(M[g + 1], j)
            N = columns(M[g + 1], j + SUB)
        here = (lane >= j) & (lane < j + SUB)
        M[g] = jnp.where(here, jnp.where(lane == row + j, 1.0, 0.0), M[g])
        if ahead:
            M[g + 1] = jnp.where(here, 0.0, M[g + 1])
        roots = jnp.zeros((SUB, n), F32)
        invs = jnp.zeros((SUB, n), F32)
        for k in range(SUB):
            root = lax.rsqrt(over(V[k], k))
            inv = root * root
            roots = jnp.where(row == k, root, roots)
            invs = jnp.where(row == k, inv, invs)
            down = jnp.where(row > k, V[k], 0.0)
            top = [None] * SUB
            for l in range(k + 1, SUB):
                top[l] = over(V[k], l)
                V[l] = V[l] - (down * top[l]) * inv
            r = over(M[g], k)
            M[g] = M[g] - (down * inv) * r
            if ahead:
                u = U[k] * inv
                for l in range(k + 1, SUB):
                    U[l] = U[l] - u * top[l]
                M[g + 1] = M[g + 1] - u * r
                for l in range(SUB):
                    N[l] = N[l] - u * over(U[k], l)
        out.append(jnp.where(lane < j + SUB, M[g] * roots, 0.0))
        if not ahead:
            break
        if g + 2 < groups:
            S = M[g] * invs
            for i in reversed(range(1, SUB)):
                S = S - (jnp.where(row < i, V[i], 0.0) * invs) * over(S, i)
            S = [over(S, k) for k in range(SUB)]
            for i in range(g + 2, groups):
                C = columns(M[i], j)
                M[i] = jnp.where(here, 0.0, M[i])
                for k in range(SUB):
                    M[i] = M[i] - C[k] * S[k]
        V = N
    return jnp.concatenate(out, axis=0)


def pack_kernel(cap, window_ref, pivot_ref, ids_ref, old_ref, eri_ref, out_ref):
    steps, width = pivot_ref.shape
    slots = out_ref.shape[1]
    part = out_ref.shape[2]
    groups = ids_ref.shape[0]
    half = eri_ref.shape[1] // 2
    ids = ids_ref[...]

    def find(j, at):
        return jnp.where(ids == pivot_ref[j // width, j % width], j + 1, at)

    at = lax.fori_loop(0, steps * width, find, jnp.zeros_like(ids), unroll=16)
    owned = jnp.where(at > 0, 1.0, 0.0)
    below = lax.broadcasted_iota(jnp.int32, (LANES, LANES), 0)
    right = lax.broadcasted_iota(jnp.int32, (LANES, LANES), 1)
    ahead = jnp.where(below < right, 1.0, 0.0).astype(BF16)
    rank = lax.dot_general(
        owned.astype(BF16), ahead, (((1,), (0,)), ((), ())), preferred_element_type=F32
    )
    first = window_ref[0] * cap
    slot = lax.broadcasted_iota(jnp.int32, (slots, LANES), 0)
    passed = jnp.zeros((1, 1), F32)
    picks, numbers = [], []
    for g in range(groups):
        here = (rank[g : g + 1] + passed).astype(jnp.int32) - first
        passed = passed + jnp.sum(owned[g : g + 1], axis=1, keepdims=True)
        here = jnp.where((owned[g : g + 1] > 0) & (here >= 0) & (here < cap), here, -1)
        picks.append(jnp.where(slot == here, 1.0, 0.0))
        numbers.append(at[g : g + 1])
    pick = jnp.concatenate(picks, axis=1).astype(BF16)
    number = jnp.concatenate(numbers, axis=1)
    pair = jnp.concatenate([number // 16, number % 16] + [jnp.zeros_like(number)] * 6, axis=0)
    pair = pair.astype(F32).astype(BF16)
    lines = lax.dot_general(pair, pick, ROWS_T, preferred_element_type=F32)
    line = lines[0:1] * 16.0 + lines[1:2]
    line = jnp.concatenate([line, jnp.zeros((1, LANES - slots), F32)], axis=1)

    def take(x):
        f = functools.partial(
            lax.dot_general,
            dimension_numbers=(((1,), (0,)), ((), ())),
            preferred_element_type=F32,
        )
        hi, lo = split(x)
        return f(pick, hi) + f(pick, lo)

    core = lax.axis_index("col")
    out_ref[0] = take(old_ref[:, :part])
    out_ref[0, slots - 1 : slots, :LANES] = line
    rest = old_ref.shape[1] - part
    out_ref[1, :, :rest] = take(old_ref[:, part:])
    out_ref[1, :, rest:] = take(eri_ref[:, pl.ds(pl.multiple_of(core * half, LANES), half)])


def pack(window, pivots, ids, old, eri, slots):
    width = (old.shape[1] + eri.shape[1] // 2) // 2
    return pl.pallas_call(
        functools.partial(pack_kernel, slots - 1),
        out_shape=jax.ShapeDtypeStruct((2, slots, width), F32),
        in_specs=[SMEM, SMEM, VMEM, VMEM, VMEM],
        out_specs=VMEM,
        name="pack",
    )(window, pivots, ids, old, eri)


def spread_kernel(grid, mine_ref, old_ref, all_ref, other_ref, *sems):
    deep, high, wide = grid
    fine = deep * high * wide <= 16
    own_sem, first_send, near_send, far_send, core_send = sems[:5]
    first_recv, recv, core_recv, old_sems = sems[5:]
    me = lax.axis_index("row")
    core = lax.axis_index("col")
    z, y, x = me // (high * wide), me // wide % high, me % wide
    chip = lambda z, y, x: (z * high + y) * wide + x
    steps = lambda at, size: [lax.rem(at + o, size) for o in range(1, size)]
    partner = (me, 1 - core)

    barrier = pltpu.get_barrier_semaphore()
    greet = [(chip(o, y, x), core) for o in steps(z, deep)]
    greet += [(chip(z, o, x), core) for o in steps(y, high)]
    greet += [(chip(z, y, o), core) for o in steps(x, wide)]
    greet.append(partner)
    for device in greet:
        pl.semaphore_signal(barrier, inc=1, device_id=device, device_id_type=MESH)
    pl.semaphore_wait(barrier, len(greet))

    flying = []

    def send(src, dst, send_sem, recv_sem, device):
        copy = pltpu.make_async_remote_copy(
            src_ref=src, dst_ref=dst, send_sem=send_sem, recv_sem=recv_sem,
            device_id=device, device_id_type=MESH,
        )
        copy.start()
        flying.append(copy)

    def await_block(ref, sem):
        pltpu.make_async_remote_copy(
            src_ref=ref, dst_ref=ref, send_sem=sem, recv_sem=sem,
            device_id=partner, device_id_type=MESH,
        ).wait_recv()

    def block(colour, zs, y, x):
        return all_ref.at[core, colour, zs, y, x]

    own = [
        pltpu.make_async_copy(mine_ref.at[k], all_ref.at[core, k, z, y, x], own_sem.at[k])
        for k in range(2)
    ]
    for k in range(2):
        own[k].start()
    for k in range(2):
        for i, o in enumerate(steps(z, deep)):
            send(mine_ref.at[k], block(k, z, y, x), first_send.at[k, i], first_recv.at[k, z], (chip(o, y, x), core))

    chunks = [z] + steps(z, deep) if fine else [None]
    near = lambda k: [(y, o) for o in steps(x, wide)] if k == 0 else [(o, x) for o in steps(y, high)]
    far = lambda k: [(o, x) for o in steps(y, high)] if k == 0 else [(y, o) for o in steps(x, wide)]

    def to_core(k, q, i, zs, y, x):
        ref = block(k, zs, y, x)
        send(ref, ref, core_send.at[k, q, i], core_recv.at[k, chunk_at(zs), y, x], partner)

    def chunk_at(zs):
        return zs if fine else 0

    def rows(zs):
        return zs if fine else slice(None)

    for q, at in enumerate(chunks):
        zs = rows(at)
        mine = fine and q == 0
        for k in range(2):
            if q == 0:
                if not fine:
                    for o in steps(z, deep):
                        await_block(block(k, o, y, x), first_recv.at[k, o])
                    own[k].wait()
            else:
                await_block(block(k, zs, y, x), first_recv.at[k, zs])
            src = mine_ref.at[k] if mine else block(k, zs, y, x)
            sem = recv.at[k, chunk_at(zs), y, x]
            for i, (b, c) in enumerate(near(k)):
                send(src, block(k, zs, y, x), near_send.at[k, q, i], sem, (chip(z, b, c), core))
            for i, (b, c) in enumerate(far(k)):
                send(src, block(k, zs, y, x), far_send.at[k, q, 0, i], sem, (chip(z, b, c), core))
            send(src, block(k, zs, y, x), core_send.at[k, q, 0], core_recv.at[k, chunk_at(zs), y, x], partner)
    old_copy = pltpu.make_async_remote_copy(
        src_ref=old_ref, dst_ref=other_ref, send_sem=old_sems.at[0], recv_sem=old_sems.at[1],
        device_id=partner, device_id_type=MESH,
    )
    old_copy.start()
    flying.append(old_copy)
    for q, at in enumerate(chunks):
        zs = rows(at)
        for k in range(2):
            for n, (b, c) in enumerate(near(k)):
                ref = block(k, zs, b, c)
                await_block(ref, recv.at[k, chunk_at(zs), b, c])
                for i, (fb, fc) in enumerate(far(k)):
                    send(ref, ref, far_send.at[k, q, 1 + n, i], recv.at[k, chunk_at(zs), b, c], (chip(z, fb, fc), core))
                to_core(k, q, 1 + n, zs, b, c)
    for q, at in enumerate(chunks):
        zs = rows(at)
        for k in range(2):
            index = 1 + len(near(k))
            for fb, fc in far(k):
                for b, c in [(y, x)] + near(k):
                    there = (fb, c) if k == 0 else (b, fc)
                    ref = block(k, zs, *there)
                    await_block(ref, recv.at[k, chunk_at(zs), *there])
                    to_core(k, q, index, zs, *there)
                    index += 1
    if fine:
        for k in range(2):
            own[k].wait()
    for q, at in enumerate(chunks):
        zs = rows(at)
        for k in range(2):
            for b in range(high):
                for c in range(wide):
                    ref = all_ref.at[1 - core, k, zs, b, c]
                    await_block(ref, core_recv.at[k, chunk_at(zs), b, c])
    old_copy.wait_recv()
    for copy in flying:
        copy.wait_send()


def spread(grid, mine, old):
    deep, high, wide = grid
    _, slots, width = mine.shape
    chunks = deep if deep * high * wide <= 16 else 1
    cells = high * wide
    peers = max(high, wide)
    sem = pltpu.SemaphoreType.DMA
    return pl.pallas_call(
        functools.partial(spread_kernel, grid),
        out_shape=(
            jax.ShapeDtypeStruct((2, 2, deep, high, wide, slots, width), F32),
            jax.ShapeDtypeStruct(old.shape, F32),
        ),
        in_specs=[pl.BlockSpec(memory_space=pl.ANY)] * 2,
        out_specs=(VMEM, pl.BlockSpec(memory_space=pl.ANY)),
        scratch_shapes=[
            sem((2,)),
            sem((2, max(deep - 1, 1))),
            sem((2, chunks, max(peers - 1, 1))),
            sem((2, chunks, peers, max(peers - 1, 1))),
            sem((2, chunks, cells)),
            sem((2, deep)),
            sem((2, chunks, high, wide)),
            sem((2, chunks, high, wide)),
            sem((2,)),
        ],
        compiler_params=pltpu.CompilerParams(
            collective_id=0, has_side_effects=True, vmem_limit_bytes=48 * 1024 * 1024
        ),
        name="spread",
    )(mine, old)


def gather_kernel(
    grid, pivot_ref, ids_ref, old_hbm, eri_hbm,
    gram_ref, hi_ref, lo_ref, old_hi_ref, old_lo_ref, most_ref,
    old, other, eri, mine, every,
    in_sems, own_sem, z_send, near_send, far_send, core_send, recv, core_recv, old_sems,
):
    deep, high, wide = grid
    cells = high * wide
    slots, width = mine.shape
    cap = slots - 1
    part = width // 2
    half = old.shape[1]
    piv = gram_ref.shape[0]
    groups = ids_ref.shape[0]
    pages = pivot_ref.shape[0]
    me = lax.axis_index("row")
    core = lax.axis_index("col")
    z, y, x = me // cells, me // wide % high, me % wide
    partner = (me, 1 - core)
    chip = lambda z, y, x: ((z * high + y) * wide + x, core)
    around = lambda at, size: [lax.rem(at + o, size) for o in range(1, size)]

    barrier = pltpu.get_barrier_semaphore()
    signal = functools.partial(pl.semaphore_signal, barrier, inc=1, device_id_type=MESH)
    beside = [chip(z, o, x) for o in around(y, high)] + [chip(z, y, o) for o in around(x, wide)]
    for device in beside + [partner]:
        signal(device_id=device)

    @pl.when(z > 0)
    def _():
        signal(device_id=chip(z - 1, y, x))

    @pl.when(z < deep - 1)
    def _():
        signal(device_id=chip(z + 1, y, x))

    loads = [
        pltpu.make_async_copy(old_hbm, old, in_sems.at[0]),
        pltpu.make_async_copy(eri_hbm, eri, in_sems.at[1]),
    ]
    for load in loads:
        load.start()

    dot = functools.partial(
        lax.dot_general, dimension_numbers=(((1,), (0,)), ((), ())), preferred_element_type=F32
    )
    wanted = [
        jnp.transpose(jnp.broadcast_to(pivot_ref[b : b + 1].astype(F32), (LANES, LANES)))
        for b in range(pages)
    ]
    count = lax.broadcasted_iota(jnp.int32, (LANES, LANES), 0).astype(F32) + 1.0
    at = []
    for g in range(groups):
        ids = jnp.broadcast_to(ids_ref[g : g + 1].astype(F32), (LANES, LANES))
        found = [jnp.where(wanted[b] == ids, count + float(LANES * b), 0.0) for b in range(pages)]
        at.append(jnp.sum(functools.reduce(jnp.add, found), axis=0, keepdims=True))
    owned = [jnp.where(v > 0, 1.0, 0.0) for v in at]
    below = lax.broadcasted_iota(jnp.int32, (LANES, LANES), 0)
    right = lax.broadcasted_iota(jnp.int32, (LANES, LANES), 1)
    ahead = jnp.where(below < right, 1.0, 0.0).astype(BF16)
    rank = dot(jnp.concatenate(owned + [jnp.zeros((-groups % 8, LANES), F32)], axis=0).astype(BF16), ahead)
    passed = jnp.zeros((1, 1), F32)
    heres = []
    for g in range(groups):
        here = rank[g : g + 1] + passed
        passed = passed + jnp.sum(owned[g], axis=1, keepdims=True)
        heres.append(jnp.where((owned[g] > 0) & (here < cap), here, -1.0 - slots * cells))
    here = jnp.concatenate(heres, axis=1)
    number = jnp.concatenate(at, axis=1)
    rows = here.shape[1]
    slot = lax.broadcasted_iota(jnp.int32, (slots, rows), 0).astype(F32)
    pick = jnp.where(slot == here, 1.0, 0.0).astype(BF16)
    place = lax.broadcasted_iota(jnp.int32, (slots * cells, rows), 0)
    first = (lax.rem(me, cells) * slots).astype(F32)
    seat = jnp.where(place.astype(F32) == here + first, 1.0, 0.0).astype(BF16)
    high_part = jnp.floor(number * (1.0 / 16.0))
    pair = jnp.concatenate([high_part, number - 16.0 * high_part, jnp.zeros((6, rows), F32)], axis=0)
    lines = lax.dot_general(pair.astype(BF16), seat, ROWS_T, preferred_element_type=F32)
    line = lines[0:1] * 16.0 + lines[1:2]
    line = jnp.concatenate([line, jnp.broadcast_to(passed, (1, part - slots * cells))], axis=1)

    def take(v):
        hi, lo = split(v)
        return dot(pick, hi) + dot(pick, lo)

    loads[0].wait()
    mine[:, :half] = take(old[...])
    mine[slots - 1 : slots, :part] = line
    loads[1].wait()
    mine[:, half:] = take(eri[:, pl.ds(pl.multiple_of(core * (piv // 2), LANES), piv // 2)])

    ends = (z + deep - 1) // deep + (2 * deep - 2 - z) // deep
    pl.semaphore_wait(barrier, len(beside) + 1 + ends)

    colour = [slice(0, part), slice(part, width)]

    def block(k, zz, b, c):
        return every.at[core, zz, b, c, :, colour[k]]

    def remote(src, dst, send_sem, recv_sem, device):
        return pltpu.make_async_remote_copy(
            src_ref=src, dst_ref=dst, send_sem=send_sem, recv_sem=recv_sem,
            device_id=device, device_id_type=MESH,
        )

    def await_block(ref, sem):
        remote(ref, ref, sem, sem, partner).wait_recv()

    near = [[(y, o) for o in around(x, wide)], [(o, x) for o in around(y, high)]]
    far = [near[1], near[0]]

    def upward(k, zz, src):
        return remote(src, block(k, zz, y, x), z_send.at[k, 0, zz], recv.at[k, zz, y, x], chip(z + 1, y, x))

    def downward(k, zz, src):
        return remote(src, block(k, zz, y, x), z_send.at[k, 1, zz], recv.at[k, zz, y, x], chip(z - 1, y, x))

    def line_sends(k, zz, src):
        out = []
        for i, (b, c) in enumerate(near[k]):
            out.append(remote(src, block(k, zz, y, x), near_send.at[k, zz, i], recv.at[k, zz, y, x], chip(z, b, c)))
        for i, (b, c) in enumerate(far[k]):
            out.append(remote(src, block(k, zz, y, x), far_send.at[k, zz, 0, i], recv.at[k, zz, y, x], chip(z, b, c)))
        return out

    def onward(k, zz, n, b, c):
        ref = block(k, zz, b, c)
        return [
            remote(ref, ref, far_send.at[k, zz, 1 + n, i], recv.at[k, zz, b, c], chip(z, fb, fc))
            for i, (fb, fc) in enumerate(far[k])
        ]

    def across(zz, b, c, src=None):
        ref = every.at[core, zz, b, c]
        return remote(ref if src is None else src, ref, core_send.at[zz, b, c], core_recv.at[zz, b, c], partner)

    own = pltpu.make_async_copy(mine, every.at[core, z, y, x], own_sem)
    old_copy = remote(old, other, old_sems.at[0], old_sems.at[1], partner)

    def start(copies):
        for copy in copies:
            copy.start()

    def line_copies(zz, src_of):
        return [copy for k in range(2) for copy in line_sends(k, zz, src_of(k))]

    mine_of = lambda k: mine.at[:, colour[k]]
    held_of = lambda zz: lambda k: block(k, zz, y, x)

    @pl.when(z > 0)
    def _():
        start([downward(k, z, mine_of(k)) for k in range(2)])

    @pl.when(z < deep - 1)
    def _():
        start([upward(k, z, mine_of(k)) for k in range(2)])

    start(line_copies(z, mine_of))
    own.start()
    start([across(z, y, x, mine), old_copy])

    def lines_at(t):
        if t == 0:
            return [(z, None, None)]
        return [
            (z - t, z >= t, (upward, z < deep - 1)),
            (z + t, z < deep - t, (downward, z > 0)),
        ]

    def guarded(test, body):
        if test is None:
            body()
        else:
            pl.when(test)(body)

    def stage_line(t):
        for zz, test, (go, further) in lines_at(t):

            def body(zz=zz, go=go, further=further):
                for k in range(2):
                    await_block(block(k, zz, y, x), recv.at[k, zz, y, x])
                    pl.when(further)(lambda k=k: go(k, zz, block(k, zz, y, x)).start())
                    start(line_sends(k, zz, block(k, zz, y, x)))
                across(zz, y, x).start()

            guarded(test, body)

    def stage_near(t):
        for zz, test, _ in lines_at(t):

            def body(zz=zz):
                for k in range(2):
                    for n, (b, c) in enumerate(near[k]):
                        await_block(block(k, zz, b, c), recv.at[k, zz, b, c])
                        start(onward(k, zz, n, b, c))
                for k in range(2):
                    for b, c in far[k]:
                        await_block(block(k, zz, b, c), recv.at[k, zz, b, c])
                        across(zz, b, c).start()

            guarded(test, body)

    corner = [(b, c) for b in around(y, high) for c in around(x, wide)]

    def stage_far(t):
        for zz, test, _ in lines_at(t):

            def body(zz=zz):
                for b, c in corner:
                    for k in range(2):
                        await_block(block(k, zz, b, c), recv.at[k, zz, b, c])
                    across(zz, b, c).start()

            guarded(test, body)

    if deep == 4:
        order = [z, z + 1 - 2 * lax.rem(z, 2), 2 - z // 2, 3 - 3 * (z // 2)]
    else:
        order = [z] + around(z, deep)
    pivot = lax.broadcasted_iota(jnp.int32, (piv, slots * cells), 0).astype(F32) + 1.0
    most = []

    def put(i):
        zz = order[i]
        for b in range(high):
            for c in range(wide):
                ref = every.at[1 - core, zz, b, c]
                remote(ref, ref, core_recv.at[zz, b, c], core_recv.at[zz, b, c], partner).wait_recv()
        lines = [every[0, zz, b, c, slots - 1 : slots, :part] for b in range(high) for c in range(wide)]
        most.append(functools.reduce(jnp.maximum, [v[:, part - LANES :] for v in lines]))
        line = functools.reduce(jnp.add, [v[:, : slots * cells] for v in lines])
        seats = jnp.where(pivot == line, 1.0, 0.0).astype(BF16)
        for c in range(2):
            hi, lo = split(every[c, zz].reshape(cells * slots, width))
            hi, lo = dot(seats, hi), dot(seats, lo)
            cut = slice(c * (piv // 2), (c + 1) * (piv // 2))
            if i == 0:
                hi_ref[c] = hi[:, :half].astype(BF16)
                lo_ref[c] = lo[:, :half].astype(BF16)
                gram_ref[:, cut] = hi[:, half:] + lo[:, half:]
            else:
                hi_ref[c] += hi[:, :half].astype(BF16)
                lo_ref[c] += lo[:, :half].astype(BF16)
                gram_ref[:, cut] += hi[:, half:] + lo[:, half:]

    def keep_old():
        old_hi_ref[core], old_lo_ref[core] = split(old[...])
        old_copy.wait_recv()
        old_hi_ref[1 - core], old_lo_ref[1 - core] = split(other[...])

    for t in range(deep + 3):
        if 1 <= t < deep:
            stage_line(t)
        if 0 <= t - 1 < deep:
            stage_near(t - 1)
        if 0 <= t - 2 < deep:
            stage_far(t - 2)
        if t == 1:
            keep_old()
        if t == 2:
            own.wait()
        if 0 <= t - 3 < deep:
            put(t - 3)

    most_ref[...] = jnp.broadcast_to(functools.reduce(jnp.maximum, most), most_ref.shape)
    for s in range(piv // LANES):
        here, upto = slice(s * LANES, (s + 1) * LANES), slice(0, (s + 1) * LANES)
        both = [
            dot_t((hi_ref[c, here], lo_ref[c, here]), (hi_ref[c, upto], lo_ref[c, upto])) for c in range(2)
        ]
        gram_ref[here, upto] -= both[0] + both[1]

    old_copy.wait_send()

    @pl.when(z > 0)
    def _():
        for k in range(2):
            downward(k, z, mine_of(k)).wait_send()

    @pl.when(z < deep - 1)
    def _():
        for k in range(2):
            upward(k, z, mine_of(k)).wait_send()

    for t in range(deep):
        for zz, test, go in lines_at(t):

            def body(zz=zz, go=go, t=t):
                for k in range(2):
                    src = mine_of(k) if t == 0 else block(k, zz, y, x)
                    if t:
                        pl.when(go[1])(lambda k=k: go[0](k, zz, block(k, zz, y, x)).wait_send())
                    for copy in line_sends(k, zz, src):
                        copy.wait_send()
                    for n, (b, c) in enumerate(near[k]):
                        for copy in onward(k, zz, n, b, c):
                            copy.wait_send()
                for b in range(high):
                    for c in range(wide):
                        across(zz, b, c).wait_send()

            guarded(test, body)


def gather(grid, pivots, ids, old, eri, slots):
    deep, high, wide = grid
    piv = eri.shape[1]
    width = old.shape[1] + piv // 2
    peers = max(high, wide)
    sem = pltpu.SemaphoreType.DMA
    wide_bf16 = jax.ShapeDtypeStruct((2, piv, old.shape[1]), BF16)
    any_space = pl.BlockSpec(memory_space=pl.ANY)
    return pl.pallas_call(
        functools.partial(gather_kernel, grid),
        out_shape=(
            jax.ShapeDtypeStruct((piv, piv), F32),
            wide_bf16,
            wide_bf16,
            jax.ShapeDtypeStruct((2, *old.shape), BF16),
            jax.ShapeDtypeStruct((2, *old.shape), BF16),
            jax.ShapeDtypeStruct((SUB, LANES), F32),
        ),
        in_specs=[VMEM, VMEM, any_space, any_space],
        out_specs=[VMEM] * 6,
        scratch_shapes=[
            pltpu.VMEM(old.shape, F32),
            pltpu.VMEM(old.shape, F32),
            pltpu.VMEM(eri.shape, F32),
            pltpu.VMEM((slots, width), F32),
            pltpu.VMEM((2, deep, high, wide, slots, width), F32),
            sem((2,)),
            sem,
            sem((2, 2, deep)),
            sem((2, deep, max(peers - 1, 1))),
            sem((2, deep, peers, max(peers - 1, 1))),
            sem((deep, high, wide)),
            sem((2, deep, high, wide)),
            sem((deep, high, wide)),
            sem((2,)),
        ],
        compiler_params=pltpu.CompilerParams(
            collective_id=1, has_side_effects=True, vmem_limit_bytes=40 * 1024 * 1024
        ),
        name="gather",
    )(pivots, ids, old, eri)


def finish_kernel(
    steps, gram_ref, hi_ref, lo_ref, old_hi_ref, old_lo_ref, eri_hbm, diag_ref, panel_hbm, new_ref,
    gram, work, panel, sems,
):
    piv = gram.shape[0]
    width = piv // steps
    f = functools.partial(lax.dot_general, preferred_element_type=F32)
    load = pltpu.make_async_copy(eri_hbm, work, sems.at[steps])
    load.start()
    gram[...] = gram_ref[...]
    rows = [(hi_ref[c], lo_ref[c]) for c in range(2)]
    old = [(old_hi_ref[c], old_lo_ref[c]) for c in range(2)]
    load.wait()
    ones = jnp.ones((SUB, width), BF16)
    new = diag_ref[...]
    stores = []
    for s in range(steps):
        at = slice(s * width, (s + 1) * width)
        inv = split(inverse_factor(gram[at, at]))
        later = [slice(t * width, (t + 1) * width) for t in range(s + 1, steps)]
        below = [split(dot_t(split(gram[t, at]), inv)) for t in later]
        for i, t in enumerate(later):
            for u in range(i + 1):
                gram[t, later[u]] -= dot_t(below[i], below[u])
        if s == 0:
            work[...] -= dot_t(old[0], rows[0]) + dot_t(old[1], rows[1])
        own = dot_t(split(work[:, at]), inv)
        panel[:, at] = own
        stores.append(pltpu.make_async_copy(panel.at[:, at], panel_hbm.at[:, at], sems.at[s]))
        stores[-1].start()
        hi, lo = split(own * own)
        new = new - (f(ones, hi, ROWS_T) + f(ones, lo, ROWS_T))[:1]
        own = split(own)
        for i, t in enumerate(later):
            work[:, t] -= dot_t(own, below[i])
    new_ref[...] = new
    for store in stores:
        store.wait()


def finish(steps, gathered, eri, diagonal):
    rows, piv = eri.shape
    any_space = pl.BlockSpec(memory_space=pl.ANY)
    panels, new = pl.pallas_call(
        functools.partial(finish_kernel, steps),
        out_shape=(
            jax.ShapeDtypeStruct((rows, piv), F32),
            jax.ShapeDtypeStruct((1, rows), F32),
        ),
        in_specs=[VMEM] * 5 + [any_space, VMEM],
        out_specs=[any_space, VMEM],
        scratch_shapes=[
            pltpu.VMEM((piv, piv), F32),
            pltpu.VMEM((rows, piv), F32),
            pltpu.VMEM((rows, piv), F32),
            pltpu.SemaphoreType.DMA((steps + 1,)),
        ],
        compiler_params=pltpu.CompilerParams(vmem_limit_bytes=24 * 1024 * 1024),
        name="finish",
    )(*gathered, eri, diagonal[None, :])
    return panels, new[0]


def place_kernel(line_ref, every_ref, out_ref):
    pivot = lax.broadcasted_iota(jnp.int32, (out_ref.shape[2], line_ref.shape[1]), 0).astype(F32) + 1.0
    seats = jnp.where(pivot == line_ref[...], 1.0, 0.0).astype(BF16)
    dot = functools.partial(
        lax.dot_general, dimension_numbers=(((1,), (0,)), ((), ())), preferred_element_type=F32
    )

    def put(i, carry):
        hi, lo = split(every_ref[i // 2, i % 2])
        out_ref[i // 2, i % 2] = dot(seats, hi) + dot(seats, lo)
        return carry

    lax.fori_loop(0, 4, put, 0)


def place(line, every, piv):
    return pl.pallas_call(
        place_kernel,
        out_shape=jax.ShapeDtypeStruct((2, 2, piv, every.shape[-1]), F32),
        in_specs=[VMEM] * 2,
        out_specs=VMEM,
        compiler_params=pltpu.CompilerParams(vmem_limit_bytes=40 * 1024 * 1024),
        name="place",
    )(line, every)


def rolled_inverse(a):
    n = a.shape[0]
    row = lax.broadcasted_iota(jnp.int32, (n, n), 0)
    lane = lax.broadcasted_iota(jnp.int32, (n, n), 1)

    def pivot(j, held):
        a, w = held
        of_row = lambda v: jnp.sum(jnp.where(row == j, v, 0.0), axis=0, keepdims=True)
        column = jnp.sum(jnp.where(lane == j, a, 0.0), axis=1, keepdims=True)
        root = lax.rsqrt(jnp.sum(jnp.where((row == j) & (lane == j), a, 0.0), keepdims=True))
        m = jnp.where(row > j, column, 0.0) * (root * root)
        return a - m * of_row(a), jnp.where(row == j, w * root, w - m * of_row(w))

    return lax.fori_loop(0, n, pivot, (a, jnp.where(row == lane, 1.0, 0.0)))[1]


def rolled_kernel(
    steps, parts_ref, own_ref, other_ref, eri_ref, diag_ref, panel_ref, new_ref,
    hi, lo, work, solved,
):
    rows, piv = eri_ref.shape
    width = piv // steps
    half = own_ref.shape[1]
    core = lax.axis_index("col")
    for c in range(2):
        both = jnp.concatenate([parts_ref[c, 0], parts_ref[c, 1]], axis=1)
        hi[c], lo[c] = split(both[:, :half])
        work[:piv, c * (piv // 2) : (c + 1) * (piv // 2)] = both[:, half:]
    at_block = lambda b: pl.ds(pl.multiple_of(b * LANES, LANES), LANES)

    def gram(b, carry):
        at = at_block(b)
        work[at, :] -= dot_t((hi[0, at], lo[0, at]), (hi[0], lo[0])) + dot_t((hi[1, at], lo[1, at]), (hi[1], lo[1]))
        return carry

    def reduce(b, carry):
        at = at_block(b)
        work[pl.ds(pl.multiple_of(piv + b * LANES, LANES), LANES), :] = eri_ref[at, :] - (
            dot_t(split(own_ref[at, :]), (hi[core], lo[core]))
            + dot_t(split(other_ref[at, :]), (hi[1 - core], lo[1 - core]))
        )
        return carry

    lax.fori_loop(0, piv // LANES, gram, 0)
    lax.fori_loop(0, rows // LANES, reduce, 0)
    new_ref[...] = diag_ref[...]
    ones = jnp.ones((SUB, width), BF16)
    f = functools.partial(lax.dot_general, dimension_numbers=ROWS_T, preferred_element_type=F32)

    def step(s, carry):
        at = pl.ds(pl.multiple_of(s * width, width), width)
        inv = split(rolled_inverse(work[at, at]))

        def solve(b, carry):
            solved[at_block(b), :] = dot_t(split(work[at_block(b), at]), inv)
            return carry

        lax.fori_loop(0, (piv + rows) // LANES, solve, 0)
        own = solved[piv:, :]
        panel_ref[:, at] = own
        high, low = split(own * own)
        new_ref[...] -= (f(ones, high) + f(ones, low))[:1]
        above = split(solved[:piv, :])

        def update(b, carry):
            work[at_block(b), :] -= dot_t(split(solved[at_block(b), :]), above)
            return carry

        lax.fori_loop(0, (piv + rows) // LANES, update, 0)
        return carry

    lax.fori_loop(0, steps, step, 0)


def rolled(steps, parts, own, other, eri, diagonal):
    rows, piv = eri.shape
    panels, new = pl.pallas_call(
        functools.partial(rolled_kernel, steps),
        out_shape=(
            jax.ShapeDtypeStruct((rows, piv), F32),
            jax.ShapeDtypeStruct((1, rows), F32),
        ),
        in_specs=[VMEM] * 5,
        out_specs=[VMEM] * 2,
        scratch_shapes=[
            pltpu.VMEM((2, piv, own.shape[1]), BF16),
            pltpu.VMEM((2, piv, own.shape[1]), BF16),
            pltpu.VMEM((piv + rows, piv), F32),
            pltpu.VMEM((piv + rows, piv // steps), F32),
        ],
        compiler_params=pltpu.CompilerParams(vmem_limit_bytes=40 * 1024 * 1024),
        name="rolled",
    )(parts, own, other, eri, diagonal[None, :])
    return panels, new[0]


def torus(chips):
    side = 1
    while 2 * (side + 1) ** 3 <= chips:
        side += 1
    return (2 * side, side, side) if 2 * side**3 == chips else (chips, 1, 1)


def slots_for(pivots, chips):
    mean = -(-pivots // chips)
    return min(LANES - 8, -(-(mean + max(12, mean // 2)) // 16) * 16)


def on_device(grid, eri_cols, old_factor, residual_diag, pivots, row_ids):
    steps, width = pivots.shape
    piv = steps * width
    chips = grid[0] * grid[1] * grid[2]
    slots = slots_for(piv, chips)
    cap = slots - 1
    ids = row_ids.reshape(-1, LANES)
    paged = pivots.reshape(-1, LANES)

    *gathered, most = gather(grid, paged, ids, old_factor, eri_cols, slots)
    panels, new = finish(steps, gathered, eri_cols, residual_diag)
    def again(state):
        windows = (most[0, 0].astype(jnp.int32) + cap - 1) // cap

        def add(w, held):
            mine = pack(jnp.full((1,), w, jnp.int32), paged, ids, old_factor, eri_cols, slots)
            every, other = spread(grid, mine, old_factor)
            every = every.reshape(2, 2, chips, slots, -1)
            line = every[0, 0, :, slots - 1, :slots].at[:, cap].set(0.0).reshape(1, -1)
            every = every.reshape(2, 2, chips * slots, -1)
            return held[0] + place(line, every, piv), other

        empty = jnp.zeros((2, 2, piv, (old_factor.shape[1] + piv // 2) // 2), F32)
        parts, other = lax.fori_loop(0, windows, add, (empty, jnp.zeros_like(old_factor)))
        return jnp.bool_(False), *rolled(steps, parts, old_factor, other, eri_cols, residual_diag)

    _, panels, new = lax.while_loop(lambda s: s[0], again, (most[0, 0] > cap, panels, new))
    return panels, new


def solution(mesh):
    grid = torus(mesh.shape["row"])
    placed = (P("row", None), P("row", "col"), P("row"), P(), P("row"))
    return jax.shard_map(
        functools.partial(on_device, grid),
        mesh=mesh, in_specs=placed, out_specs=(P("row", None), P("row")), check_vma=False,
    )
```

```python
import functools
import jax
import jax.numpy as jnp
from jax import lax
from jax.experimental import pallas as pl
from jax.experimental.pallas import tpu as pltpu
from jax.sharding import PartitionSpec as P

ROWS_T = (((1,), (1,)), ((), ()))
COLS_T = (((0,), (0,)), ((), ()))
SUB = 8
LANES = 128
MESH = pl.DeviceIdType.MESH
VMEM = pl.BlockSpec(memory_space=pltpu.VMEM)
SMEM = pl.BlockSpec(memory_space=pltpu.SMEM)
F32 = jnp.float32
BF16 = jnp.bfloat16


def split(x):
    hi = x.astype(BF16)
    return hi, (x - hi.astype(F32)).astype(BF16)


def dot_t(a, b):
    f = functools.partial(
        lax.dot_general, dimension_numbers=ROWS_T, preferred_element_type=F32
    )
    return f(a[0], b[0]) + (f(a[0], b[1]) + f(a[1], b[0]))


def inverse_factor(a):
    n = a.shape[0]
    groups = n // SUB
    row = lax.broadcasted_iota(jnp.int32, (SUB, n), 0)
    lane = lax.broadcasted_iota(jnp.int32, (SUB, n), 1)
    M = [a[SUB * i : SUB * i + SUB, :] for i in range(groups)]
    over = lambda v, k: jnp.broadcast_to(v[k : k + 1, :], (SUB, n))
    columns = lambda v, j: [jnp.broadcast_to(v[:, j + k : j + k + 1], (SUB, n)) for k in range(SUB)]
    out = []
    V = [jnp.where(row >= 0, v, 0.0) for v in columns(M[0], 0)]
    for g in range(groups):
        j = SUB * g
        ahead = g + 1 < groups
        if ahead:
            U = [jnp.where(row >= 0, v, 0.0) for v in columns(M[g + 1], j)]
            N = columns(M[g + 1], j + SUB)
        here = (lane >= j) & (lane < j + SUB)
        M[g] = jnp.where(here, jnp.where(lane == row + j, 1.0, 0.0), M[g])
        if ahead:
            M[g + 1] = jnp.where(here, 0.0, M[g + 1])
        roots = jnp.zeros((SUB, n), F32)
        invs = jnp.zeros((SUB, n), F32)
        for k in range(SUB):
            root = lax.rsqrt(over(V[k], k))
            inv = root * root
            roots = jnp.where(row == k, root, roots)
            invs = jnp.where(row == k, inv, invs)
            down = jnp.where(row > k, V[k], 0.0)
            top = [None] * SUB
            for l in range(k + 1, SUB):
                top[l] = over(V[k], l)
                V[l] = V[l] - (down * top[l]) * inv
            r = over(M[g], k)
            M[g] = M[g] - (down * inv) * r
            if ahead:
                u = U[k] * inv
                for l in range(k + 1, SUB):
                    U[l] = U[l] - u * top[l]
                M[g + 1] = M[g + 1] - u * r
                for l in range(SUB):
                    N[l] = N[l] - u * over(U[k], l)
        out.append(jnp.where(lane < j + SUB, M[g] * roots, 0.0))
        if not ahead:
            break
        if g + 2 < groups:
            S = M[g] * invs
            for i in reversed(range(1, SUB)):
                S = S - (jnp.where(row < i, V[i], 0.0) * invs) * over(S, i)
            S = [over(S, k) for k in range(SUB)]
            for i in range(g + 2, groups):
                C = columns(M[i], j)
                M[i] = jnp.where(here, 0.0, M[i])
                for k in range(SUB):
                    M[i] = M[i] - C[k] * S[k]
        V = N
    return jnp.concatenate(out, axis=0)


def pack_kernel(cap, window_ref, pivot_ref, ids_ref, old_ref, eri_ref, out_ref):
    steps, width = pivot_ref.shape
    slots = out_ref.shape[1]
    part = out_ref.shape[2]
    groups = ids_ref.shape[0]
    half = eri_ref.shape[1] // 2
    ids = ids_ref[...]

    def find(j, at):
        return jnp.where(ids == pivot_ref[j // width, j % width], j + 1, at)

    at = lax.fori_loop(0, steps * width, find, jnp.zeros_like(ids), unroll=16)
    owned = jnp.where(at > 0, 1.0, 0.0)
    below = lax.broadcasted_iota(jnp.int32, (LANES, LANES), 0)
    right = lax.broadcasted_iota(jnp.int32, (LANES, LANES), 1)
    ahead = jnp.where(below < right, 1.0, 0.0).astype(BF16)
    rank = lax.dot_general(
        owned.astype(BF16), ahead, (((1,), (0,)), ((), ())), preferred_element_type=F32
    )
    first = window_ref[0] * cap
    slot = lax.broadcasted_iota(jnp.int32, (slots, LANES), 0)
    passed = jnp.zeros((1, 1), F32)
    picks, numbers = [], []
    for g in range(groups):
        here = (rank[g : g + 1] + passed).astype(jnp.int32) - first
        passed = passed + jnp.sum(owned[g : g + 1], axis=1, keepdims=True)
        here = jnp.where((owned[g : g + 1] > 0) & (here >= 0) & (here < cap), here, -1)
        picks.append(jnp.where(slot == here, 1.0, 0.0))
        numbers.append(at[g : g + 1])
    pick = jnp.concatenate(picks, axis=1).astype(BF16)
    number = jnp.concatenate(numbers, axis=1)
    pair = jnp.concatenate([number // 16, number % 16] + [jnp.zeros_like(number)] * 6, axis=0)
    pair = pair.astype(F32).astype(BF16)
    lines = lax.dot_general(pair, pick, ROWS_T, preferred_element_type=F32)
    line = lines[0:1] * 16.0 + lines[1:2]
    line = jnp.concatenate([line, jnp.zeros((1, LANES - slots), F32)], axis=1)

    def take(x):
        f = functools.partial(
            lax.dot_general,
            dimension_numbers=(((1,), (0,)), ((), ())),
            preferred_element_type=F32,
        )
        hi, lo = split(x)
        return f(pick, hi) + f(pick, lo)

    core = lax.axis_index("col")
    out_ref[0] = take(old_ref[:, :part])
    out_ref[0, slots - 1 : slots, :LANES] = line
    rest = old_ref.shape[1] - part
    out_ref[1, :, :rest] = take(old_ref[:, part:])
    out_ref[1, :, rest:] = take(eri_ref[:, pl.ds(pl.multiple_of(core * half, LANES), half)])


def pack(window, pivots, ids, old, eri, slots):
    width = (old.shape[1] + eri.shape[1] // 2) // 2
    return pl.pallas_call(
        functools.partial(pack_kernel, slots - 1),
        out_shape=jax.ShapeDtypeStruct((2, slots, width), F32),
        in_specs=[SMEM, SMEM, VMEM, VMEM, VMEM],
        out_specs=VMEM,
        name="pack",
    )(window, pivots, ids, old, eri)


def spread_kernel(grid, mine_ref, old_ref, all_ref, other_ref, *sems):
    deep, high, wide = grid
    fine = deep * high * wide <= 16
    own_sem, first_send, near_send, far_send, core_send = sems[:5]
    first_recv, recv, core_recv, old_sems = sems[5:]
    me = lax.axis_index("row")
    core = lax.axis_index("col")
    z, y, x = me // (high * wide), me // wide % high, me % wide
    chip = lambda z, y, x: (z * high + y) * wide + x
    steps = lambda at, size: [lax.rem(at + o, size) for o in range(1, size)]
    partner = (me, 1 - core)

    barrier = pltpu.get_barrier_semaphore()
    greet = [(chip(o, y, x), core) for o in steps(z, deep)]
    greet += [(chip(z, o, x), core) for o in steps(y, high)]
    greet += [(chip(z, y, o), core) for o in steps(x, wide)]
    greet.append(partner)
    for device in greet:
        pl.semaphore_signal(barrier, inc=1, device_id=device, device_id_type=MESH)
    pl.semaphore_wait(barrier, len(greet))

    flying = []

    def send(src, dst, send_sem, recv_sem, device):
        copy = pltpu.make_async_remote_copy(
            src_ref=src, dst_ref=dst, send_sem=send_sem, recv_sem=recv_sem,
            device_id=device, device_id_type=MESH,
        )
        copy.start()
        flying.append(copy)

    def await_block(ref, sem):
        pltpu.make_async_remote_copy(
            src_ref=ref, dst_ref=ref, send_sem=sem, recv_sem=sem,
            device_id=partner, device_id_type=MESH,
        ).wait_recv()

    def block(colour, zs, y, x):
        return all_ref.at[core, colour, zs, y, x]

    own = [
        pltpu.make_async_copy(mine_ref.at[k], all_ref.at[core, k, z, y, x], own_sem.at[k])
        for k in range(2)
    ]
    for k in range(2):
        own[k].start()
    for k in range(2):
        for i, o in enumerate(steps(z, deep)):
            send(mine_ref.at[k], block(k, z, y, x), first_send.at[k, i], first_recv.at[k, z], (chip(o, y, x), core))

    chunks = [z] + steps(z, deep) if fine else [None]
    near = lambda k: [(y, o) for o in steps(x, wide)] if k == 0 else [(o, x) for o in steps(y, high)]
    far = lambda k: [(o, x) for o in steps(y, high)] if k == 0 else [(y, o) for o in steps(x, wide)]

    def to_core(k, q, i, zs, y, x):
        ref = block(k, zs, y, x)
        send(ref, ref, core_send.at[k, q, i], core_recv.at[k, chunk_at(zs), y, x], partner)

    def chunk_at(zs):
        return zs if fine else 0

    def rows(zs):
        return zs if fine else slice(None)

    for q, at in enumerate(chunks):
        zs = rows(at)
        mine = fine and q == 0
        for k in range(2):
            if q == 0:
                if not fine:
                    for o in steps(z, deep):
                        await_block(block(k, o, y, x), first_recv.at[k, o])
                    own[k].wait()
            else:
                await_block(block(k, zs, y, x), first_recv.at[k, zs])
            src = mine_ref.at[k] if mine else block(k, zs, y, x)
            sem = recv.at[k, chunk_at(zs), y, x]
            for i, (b, c) in enumerate(near(k)):
                send(src, block(k, zs, y, x), near_send.at[k, q, i], sem, (chip(z, b, c), core))
            for i, (b, c) in enumerate(far(k)):
                send(src, block(k, zs, y, x), far_send.at[k, q, 0, i], sem, (chip(z, b, c), core))
            send(src, block(k, zs, y, x), core_send.at[k, q, 0], core_recv.at[k, chunk_at(zs), y, x], partner)
    old_copy = pltpu.make_async_remote_copy(
        src_ref=old_ref, dst_ref=other_ref, send_sem=old_sems.at[0], recv_sem=old_sems.at[1],
        device_id=partner, device_id_type=MESH,
    )
    old_copy.start()
    flying.append(old_copy)
    for q, at in enumerate(chunks):
        zs = rows(at)
        for k in range(2):
            for n, (b, c) in enumerate(near(k)):
                ref = block(k, zs, b, c)
                await_block(ref, recv.at[k, chunk_at(zs), b, c])
                for i, (fb, fc) in enumerate(far(k)):
                    send(ref, ref, far_send.at[k, q, 1 + n, i], recv.at[k, chunk_at(zs), b, c], (chip(z, fb, fc), core))
                to_core(k, q, 1 + n, zs, b, c)
    for q, at in enumerate(chunks):
        zs = rows(at)
        for k in range(2):
            index = 1 + len(near(k))
            for fb, fc in far(k):
                for b, c in [(y, x)] + near(k):
                    there = (fb, c) if k == 0 else (b, fc)
                    ref = block(k, zs, *there)
                    await_block(ref, recv.at[k, chunk_at(zs), *there])
                    to_core(k, q, index, zs, *there)
                    index += 1
    if fine:
        for k in range(2):
            own[k].wait()
    for q, at in enumerate(chunks):
        zs = rows(at)
        for k in range(2):
            for b in range(high):
                for c in range(wide):
                    ref = all_ref.at[1 - core, k, zs, b, c]
                    await_block(ref, core_recv.at[k, chunk_at(zs), b, c])
    old_copy.wait_recv()
    for copy in flying:
        copy.wait_send()


def spread(grid, mine, old):
    deep, high, wide = grid
    _, slots, width = mine.shape
    chunks = deep if deep * high * wide <= 16 else 1
    cells = high * wide
    peers = max(high, wide)
    sem = pltpu.SemaphoreType.DMA
    return pl.pallas_call(
        functools.partial(spread_kernel, grid),
        out_shape=(
            jax.ShapeDtypeStruct((2, 2, deep, high, wide, slots, width), F32),
            jax.ShapeDtypeStruct(old.shape, F32),
        ),
        in_specs=[pl.BlockSpec(memory_space=pl.ANY)] * 2,
        out_specs=(VMEM, pl.BlockSpec(memory_space=pl.ANY)),
        scratch_shapes=[
            sem((2,)),
            sem((2, max(deep - 1, 1))),
            sem((2, chunks, max(peers - 1, 1))),
            sem((2, chunks, peers, max(peers - 1, 1))),
            sem((2, chunks, cells)),
            sem((2, deep)),
            sem((2, chunks, high, wide)),
            sem((2, chunks, high, wide)),
            sem((2,)),
        ],
        compiler_params=pltpu.CompilerParams(
            collective_id=0, has_side_effects=True, vmem_limit_bytes=48 * 1024 * 1024
        ),
        name="spread",
    )(mine, old)


def gather_kernel(
    grid, pivot_ref, ids_ref, old_hbm, eri_hbm,
    gram_ref, hi_ref, lo_ref, old_hi_ref, old_lo_ref, eri, most_ref,
    old, other, mine, every,
    in_sems, own_sem, z_send, near_send, far_send, core_send, recv, core_recv, old_sems,
):
    deep, high, wide = grid
    cells = high * wide
    slots, width = mine.shape
    cap = slots - 1
    part = width // 2
    half = old.shape[1]
    piv = gram_ref.shape[0]
    groups = ids_ref.shape[0]
    pages = pivot_ref.shape[0]
    me = lax.axis_index("row")
    core = lax.axis_index("col")
    z, y, x = me // cells, me // wide % high, me % wide
    partner = (me, 1 - core)
    chip = lambda z, y, x: ((z * high + y) * wide + x, core)
    around = lambda at, size: [lax.rem(at + o, size) for o in range(1, size)]

    barrier = pltpu.get_barrier_semaphore()
    signal = functools.partial(pl.semaphore_signal, barrier, inc=1, device_id_type=MESH)
    beside = [chip(z, o, x) for o in around(y, high)] + [chip(z, y, o) for o in around(x, wide)]
    for device in beside + [partner]:
        signal(device_id=device)

    @pl.when(z > 0)
    def _():
        signal(device_id=chip(z - 1, y, x))

    @pl.when(z < deep - 1)
    def _():
        signal(device_id=chip(z + 1, y, x))

    loads = [
        pltpu.make_async_copy(old_hbm, old, in_sems.at[0]),
        pltpu.make_async_copy(eri_hbm, eri, in_sems.at[1]),
    ]
    for load in loads:
        load.start()

    dot = functools.partial(
        lax.dot_general, dimension_numbers=(((1,), (0,)), ((), ())), preferred_element_type=F32
    )
    wanted = [
        jnp.transpose(jnp.broadcast_to(pivot_ref[b : b + 1].astype(F32), (LANES, LANES)))
        for b in range(pages)
    ]
    count = lax.broadcasted_iota(jnp.int32, (LANES, LANES), 0).astype(F32) + 1.0
    at = []
    for g in range(groups):
        ids = jnp.broadcast_to(ids_ref[g : g + 1].astype(F32), (LANES, LANES))
        found = [jnp.where(wanted[b] == ids, count + float(LANES * b), 0.0) for b in range(pages)]
        at.append(jnp.sum(functools.reduce(jnp.add, found), axis=0, keepdims=True))
    owned = [jnp.where(v > 0, 1.0, 0.0) for v in at]
    below = lax.broadcasted_iota(jnp.int32, (LANES, LANES), 0)
    right = lax.broadcasted_iota(jnp.int32, (LANES, LANES), 1)
    ahead = jnp.where(below < right, 1.0, 0.0).astype(BF16)
    rank = dot(jnp.concatenate(owned + [jnp.zeros((-groups % 8, LANES), F32)], axis=0).astype(BF16), ahead)
    passed = jnp.zeros((1, 1), F32)
    heres = []
    for g in range(groups):
        here = rank[g : g + 1] + passed
        passed = passed + jnp.sum(owned[g], axis=1, keepdims=True)
        heres.append(jnp.where((owned[g] > 0) & (here < cap), here, -1.0 - slots * cells))
    here = jnp.concatenate(heres, axis=1)
    number = jnp.concatenate(at, axis=1)
    rows = here.shape[1]
    slot = lax.broadcasted_iota(jnp.int32, (slots, rows), 0).astype(F32)
    pick = jnp.where(slot == here, 1.0, 0.0).astype(BF16)
    place = lax.broadcasted_iota(jnp.int32, (slots * cells, rows), 0)
    first = (lax.rem(me, cells) * slots).astype(F32)
    seat = jnp.where(place.astype(F32) == here + first, 1.0, 0.0).astype(BF16)
    high_part = jnp.floor(number * (1.0 / 16.0))
    pair = jnp.concatenate([high_part, number - 16.0 * high_part, jnp.zeros((6, rows), F32)], axis=0)
    lines = lax.dot_general(pair.astype(BF16), seat, ROWS_T, preferred_element_type=F32)
    line = lines[0:1] * 16.0 + lines[1:2]
    line = jnp.concatenate([line, jnp.broadcast_to(passed, (1, part - slots * cells))], axis=1)

    def take(v):
        hi, lo = split(v)
        return dot(pick, hi) + dot(pick, lo)

    loads[0].wait()
    mine[:, :half] = take(old[...])
    mine[slots - 1 : slots, :part] = line
    loads[1].wait()
    mine[:, half:] = take(eri[:, pl.ds(pl.multiple_of(core * (piv // 2), LANES), piv // 2)])

    ends = (z + deep - 1) // deep + (2 * deep - 2 - z) // deep
    pl.semaphore_wait(barrier, len(beside) + 1 + ends)

    colour = [slice(0, part), slice(part, width)]

    def block(k, zz, b, c):
        return every.at[core, zz, b, c, :, colour[k]]

    def remote(src, dst, send_sem, recv_sem, device):
        return pltpu.make_async_remote_copy(
            src_ref=src, dst_ref=dst, send_sem=send_sem, recv_sem=recv_sem,
            device_id=device, device_id_type=MESH,
        )

    def await_block(ref, sem):
        remote(ref, ref, sem, sem, partner).wait_recv()

    near = [[(y, o) for o in around(x, wide)], [(o, x) for o in around(y, high)]]
    far = [near[1], near[0]]

    def upward(k, zz, src):
        return remote(src, block(k, zz, y, x), z_send.at[k, 0, zz], recv.at[k, zz, y, x], chip(z + 1, y, x))

    def downward(k, zz, src):
        return remote(src, block(k, zz, y, x), z_send.at[k, 1, zz], recv.at[k, zz, y, x], chip(z - 1, y, x))

    def line_sends(k, zz, src):
        out = []
        for i, (b, c) in enumerate(near[k]):
            out.append(remote(src, block(k, zz, y, x), near_send.at[k, zz, i], recv.at[k, zz, y, x], chip(z, b, c)))
        for i, (b, c) in enumerate(far[k]):
            out.append(remote(src, block(k, zz, y, x), far_send.at[k, zz, 0, i], recv.at[k, zz, y, x], chip(z, b, c)))
        return out

    def onward(k, zz, n, b, c):
        ref = block(k, zz, b, c)
        return [
            remote(ref, ref, far_send.at[k, zz, 1 + n, i], recv.at[k, zz, b, c], chip(z, fb, fc))
            for i, (fb, fc) in enumerate(far[k])
        ]

    def across(zz, b, c, src=None):
        ref = every.at[core, zz, b, c]
        return remote(ref if src is None else src, ref, core_send.at[zz, b, c], core_recv.at[zz, b, c], partner)

    own = pltpu.make_async_copy(mine, every.at[core, z, y, x], own_sem)
    old_copy = remote(old, other, old_sems.at[0], old_sems.at[1], partner)

    def start(copies):
        for copy in copies:
            copy.start()

    def line_copies(zz, src_of):
        return [copy for k in range(2) for copy in line_sends(k, zz, src_of(k))]

    mine_of = lambda k: mine.at[:, colour[k]]
    held_of = lambda zz: lambda k: block(k, zz, y, x)

    @pl.when(z > 0)
    def _():
        start([downward(k, z, mine_of(k)) for k in range(2)])

    @pl.when(z < deep - 1)
    def _():
        start([upward(k, z, mine_of(k)) for k in range(2)])

    start(line_copies(z, mine_of))
    own.start()
    start([across(z, y, x, mine), old_copy])

    def lines_at(t):
        if t == 0:
            return [(z, None, None)]
        return [
            (z - t, z >= t, (upward, z < deep - 1)),
            (z + t, z < deep - t, (downward, z > 0)),
        ]

    def guarded(test, body):
        if test is None:
            body()
        else:
            pl.when(test)(body)

    def stage_line(t):
        for zz, test, (go, further) in lines_at(t):

            def body(zz=zz, go=go, further=further):
                for k in range(2):
                    await_block(block(k, zz, y, x), recv.at[k, zz, y, x])
                    pl.when(further)(lambda k=k: go(k, zz, block(k, zz, y, x)).start())
                    start(line_sends(k, zz, block(k, zz, y, x)))
                across(zz, y, x).start()

            guarded(test, body)

    def stage_near(t):
        for zz, test, _ in lines_at(t):

            def body(zz=zz):
                for k in range(2):
                    for n, (b, c) in enumerate(near[k]):
                        await_block(block(k, zz, b, c), recv.at[k, zz, b, c])
                        start(onward(k, zz, n, b, c))
                for k in range(2):
                    for b, c in far[k]:
                        await_block(block(k, zz, b, c), recv.at[k, zz, b, c])
                        across(zz, b, c).start()

            guarded(test, body)

    corner = [(b, c) for b in around(y, high) for c in around(x, wide)]

    def stage_far(t):
        for zz, test, _ in lines_at(t):

            def body(zz=zz):
                for b, c in corner:
                    for k in range(2):
                        await_block(block(k, zz, b, c), recv.at[k, zz, b, c])
                    across(zz, b, c).start()

            guarded(test, body)

    if deep == 4:
        order = [z, z + 1 - 2 * lax.rem(z, 2), 2 - z // 2, 3 - 3 * (z // 2)]
    else:
        order = [z] + around(z, deep)
    pivot = lax.broadcasted_iota(jnp.int32, (piv, slots * cells), 0).astype(F32) + 1.0
    most = []

    def put(i):
        zz = order[i]
        for b in range(high):
            for c in range(wide):
                ref = every.at[1 - core, zz, b, c]
                remote(ref, ref, core_recv.at[zz, b, c], core_recv.at[zz, b, c], partner).wait_recv()
        lines = [every[0, zz, b, c, slots - 1 : slots, :part] for b in range(high) for c in range(wide)]
        most.append(functools.reduce(jnp.maximum, [v[:, part - LANES :] for v in lines]))
        line = functools.reduce(jnp.add, [v[:, : slots * cells] for v in lines])
        seats = jnp.where(pivot == line, 1.0, 0.0).astype(BF16)
        for c in range(2):
            hi, lo = split(every[c, zz].reshape(cells * slots, width))
            hi, lo = dot(seats, hi), dot(seats, lo)
            cut = slice(c * (piv // 2), (c + 1) * (piv // 2))
            if i == 0:
                hi_ref[c] = hi[:, :half].astype(BF16)
                lo_ref[c] = lo[:, :half].astype(BF16)
                gram_ref[:, cut] = hi[:, half:] + lo[:, half:]
            else:
                hi_ref[c] += hi[:, :half].astype(BF16)
                lo_ref[c] += lo[:, :half].astype(BF16)
                gram_ref[:, cut] += hi[:, half:] + lo[:, half:]

    def keep_old():
        old_hi_ref[core], old_lo_ref[core] = split(old[...])
        old_copy.wait_recv()
        old_hi_ref[1 - core], old_lo_ref[1 - core] = split(other[...])

    for t in range(deep + 3):
        if 1 <= t < deep:
            stage_line(t)
        if 0 <= t - 1 < deep:
            stage_near(t - 1)
        if 0 <= t - 2 < deep:
            stage_far(t - 2)
        if t == 1:
            keep_old()
        if t == 2:
            own.wait()
        if 0 <= t - 3 < deep:
            put(t - 3)

    most_ref[...] = jnp.broadcast_to(functools.reduce(jnp.maximum, most), most_ref.shape)
    old_copy.wait_send()

    @pl.when(z > 0)
    def _():
        for k in range(2):
            downward(k, z, mine_of(k)).wait_send()

    @pl.when(z < deep - 1)
    def _():
        for k in range(2):
            upward(k, z, mine_of(k)).wait_send()

    for t in range(deep):
        for zz, test, go in lines_at(t):

            def body(zz=zz, go=go, t=t):
                for k in range(2):
                    src = mine_of(k) if t == 0 else block(k, zz, y, x)
                    if t:
                        pl.when(go[1])(lambda k=k: go[0](k, zz, block(k, zz, y, x)).wait_send())
                    for copy in line_sends(k, zz, src):
                        copy.wait_send()
                    for n, (b, c) in enumerate(near[k]):
                        for copy in onward(k, zz, n, b, c):
                            copy.wait_send()
                for b in range(high):
                    for c in range(wide):
                        across(zz, b, c).wait_send()

            guarded(test, body)


def gather(grid, pivots, ids, old, eri, slots):
    deep, high, wide = grid
    piv = eri.shape[1]
    width = old.shape[1] + piv // 2
    peers = max(high, wide)
    sem = pltpu.SemaphoreType.DMA
    wide_bf16 = jax.ShapeDtypeStruct((2, piv, old.shape[1]), BF16)
    any_space = pl.BlockSpec(memory_space=pl.ANY)
    return pl.pallas_call(
        functools.partial(gather_kernel, grid),
        out_shape=(
            jax.ShapeDtypeStruct((piv, piv), F32),
            wide_bf16,
            wide_bf16,
            jax.ShapeDtypeStruct((2, *old.shape), BF16),
            jax.ShapeDtypeStruct((2, *old.shape), BF16),
            jax.ShapeDtypeStruct(eri.shape, F32),
            jax.ShapeDtypeStruct((SUB, LANES), F32),
        ),
        in_specs=[VMEM, VMEM, any_space, any_space],
        out_specs=[VMEM] * 7,
        scratch_shapes=[
            pltpu.VMEM(old.shape, F32),
            pltpu.VMEM(old.shape, F32),
            pltpu.VMEM((slots, width), F32),
            pltpu.VMEM((2, deep, high, wide, slots, width), F32),
            sem((2,)),
            sem,
            sem((2, 2, deep)),
            sem((2, deep, max(peers - 1, 1))),
            sem((2, deep, peers, max(peers - 1, 1))),
            sem((deep, high, wide)),
            sem((2, deep, high, wide)),
            sem((deep, high, wide)),
            sem((2,)),
        ],
        compiler_params=pltpu.CompilerParams(
            collective_id=1, has_side_effects=True, vmem_limit_bytes=40 * 1024 * 1024
        ),
        name="gather",
    )(pivots, ids, old, eri)


def finish_kernel(
    steps, cap, gram_ref, hi_ref, lo_ref, old_hi_ref, old_lo_ref, eri_ref, most_ref, diag_ref,
    panel_hbm, new_ref, over_ref, gram, work, panel, sems,
):
    piv = gram.shape[0]
    width = piv // steps
    f = functools.partial(lax.dot_general, preferred_element_type=F32)
    over_ref[0] = jnp.where(jnp.max(most_ref[...]) > cap, 1, 0)
    rows = [(hi_ref[c], lo_ref[c]) for c in range(2)]
    old = [(old_hi_ref[c], old_lo_ref[c]) for c in range(2)]
    for s in range(steps):
        here, upto = slice(s * width, (s + 1) * width), slice(0, (s + 1) * width)
        both = [dot_t((v[0][here], v[1][here]), (v[0][upto], v[1][upto])) for v in rows]
        gram[here, upto] = gram_ref[here, upto] - (both[0] + both[1])
    ones = jnp.ones((SUB, width), BF16)
    new = diag_ref[...]
    stores = []
    for s in range(steps):
        at = slice(s * width, (s + 1) * width)
        inv = split(inverse_factor(gram[at, at]))
        later = [slice(t * width, (t + 1) * width) for t in range(s + 1, steps)]
        below = [split(dot_t(split(gram[t, at]), inv)) for t in later]
        for i, t in enumerate(later):
            for u in range(i + 1):
                gram[t, later[u]] -= dot_t(below[i], below[u])
        if s == 0:
            work[...] = eri_ref[...] - (dot_t(old[0], rows[0]) + dot_t(old[1], rows[1]))
        own = dot_t(split(work[:, at]), inv)
        panel[:, at] = own
        stores.append(pltpu.make_async_copy(panel.at[:, at], panel_hbm.at[:, at], sems.at[s]))
        stores[-1].start()
        hi, lo = split(own * own)
        new = new - (f(ones, hi, ROWS_T) + f(ones, lo, ROWS_T))[:1]
        own = split(own)
        for i, t in enumerate(later):
            work[:, t] -= dot_t(own, below[i])
    new_ref[...] = new
    for store in stores:
        store.wait()


def finish(steps, cap, gathered, diagonal):
    rows, piv = gathered[5].shape
    any_space = pl.BlockSpec(memory_space=pl.ANY)
    panels, new, over = pl.pallas_call(
        functools.partial(finish_kernel, steps, cap),
        out_shape=(
            jax.ShapeDtypeStruct((rows, piv), F32),
            jax.ShapeDtypeStruct((1, rows), F32),
            jax.ShapeDtypeStruct((1,), jnp.int32),
        ),
        in_specs=[VMEM] * 8,
        out_specs=[any_space, VMEM, SMEM],
        scratch_shapes=[
            pltpu.VMEM((piv, piv), F32),
            pltpu.VMEM((rows, piv), F32),
            pltpu.VMEM((rows, piv), F32),
            pltpu.SemaphoreType.DMA((steps,)),
        ],
        compiler_params=pltpu.CompilerParams(vmem_limit_bytes=24 * 1024 * 1024),
        name="finish",
    )(*gathered, diagonal[None, :])
    return over[0], panels, new[0]


def place_kernel(line_ref, every_ref, out_ref):
    pivot = lax.broadcasted_iota(jnp.int32, (out_ref.shape[2], line_ref.shape[1]), 0).astype(F32) + 1.0
    seats = jnp.where(pivot == line_ref[...], 1.0, 0.0).astype(BF16)
    dot = functools.partial(
        lax.dot_general, dimension_numbers=(((1,), (0,)), ((), ())), preferred_element_type=F32
    )

    def put(i, carry):
        hi, lo = split(every_ref[i // 2, i % 2])
        out_ref[i // 2, i % 2] = dot(seats, hi) + dot(seats, lo)
        return carry

    lax.fori_loop(0, 4, put, 0)


def place(line, every, piv):
    return pl.pallas_call(
        place_kernel,
        out_shape=jax.ShapeDtypeStruct((2, 2, piv, every.shape[-1]), F32),
        in_specs=[VMEM] * 2,
        out_specs=VMEM,
        compiler_params=pltpu.CompilerParams(vmem_limit_bytes=40 * 1024 * 1024),
        name="place",
    )(line, every)


def rolled_inverse(a):
    n = a.shape[0]
    row = lax.broadcasted_iota(jnp.int32, (n, n), 0)
    lane = lax.broadcasted_iota(jnp.int32, (n, n), 1)

    def pivot(j, held):
        a, w = held
        of_row = lambda v: jnp.sum(jnp.where(row == j, v, 0.0), axis=0, keepdims=True)
        column = jnp.sum(jnp.where(lane == j, a, 0.0), axis=1, keepdims=True)
        root = lax.rsqrt(jnp.sum(jnp.where((row == j) & (lane == j), a, 0.0), keepdims=True))
        m = jnp.where(row > j, column, 0.0) * (root * root)
        return a - m * of_row(a), jnp.where(row == j, w * root, w - m * of_row(w))

    return lax.fori_loop(0, n, pivot, (a, jnp.where(row == lane, 1.0, 0.0)))[1]


def rolled_kernel(
    steps, parts_ref, own_ref, other_ref, eri_ref, diag_ref, panel_ref, new_ref,
    hi, lo, work, solved,
):
    rows, piv = eri_ref.shape
    width = piv // steps
    half = own_ref.shape[1]
    core = lax.axis_index("col")
    for c in range(2):
        both = jnp.concatenate([parts_ref[c, 0], parts_ref[c, 1]], axis=1)
        hi[c], lo[c] = split(both[:, :half])
        work[:piv, c * (piv // 2) : (c + 1) * (piv // 2)] = both[:, half:]
    at_block = lambda b: pl.ds(pl.multiple_of(b * LANES, LANES), LANES)

    def gram(b, carry):
        at = at_block(b)
        work[at, :] -= dot_t((hi[0, at], lo[0, at]), (hi[0], lo[0])) + dot_t((hi[1, at], lo[1, at]), (hi[1], lo[1]))
        return carry

    def reduce(b, carry):
        at = at_block(b)
        work[pl.ds(pl.multiple_of(piv + b * LANES, LANES), LANES), :] = eri_ref[at, :] - (
            dot_t(split(own_ref[at, :]), (hi[core], lo[core]))
            + dot_t(split(other_ref[at, :]), (hi[1 - core], lo[1 - core]))
        )
        return carry

    lax.fori_loop(0, piv // LANES, gram, 0)
    lax.fori_loop(0, rows // LANES, reduce, 0)
    new_ref[...] = diag_ref[...]
    ones = jnp.ones((SUB, width), BF16)
    f = functools.partial(lax.dot_general, dimension_numbers=ROWS_T, preferred_element_type=F32)

    def step(s, carry):
        at = pl.ds(pl.multiple_of(s * width, width), width)
        inv = split(rolled_inverse(work[at, at]))

        def solve(b, carry):
            solved[at_block(b), :] = dot_t(split(work[at_block(b), at]), inv)
            return carry

        lax.fori_loop(0, (piv + rows) // LANES, solve, 0)
        own = solved[piv:, :]
        panel_ref[:, at] = own
        high, low = split(own * own)
        new_ref[...] -= (f(ones, high) + f(ones, low))[:1]
        above = split(solved[:piv, :])

        def update(b, carry):
            work[at_block(b), :] -= dot_t(split(solved[at_block(b), :]), above)
            return carry

        lax.fori_loop(0, (piv + rows) // LANES, update, 0)
        return carry

    lax.fori_loop(0, steps, step, 0)


def rolled(steps, parts, own, other, eri, diagonal):
    rows, piv = eri.shape
    panels, new = pl.pallas_call(
        functools.partial(rolled_kernel, steps),
        out_shape=(
            jax.ShapeDtypeStruct((rows, piv), F32),
            jax.ShapeDtypeStruct((1, rows), F32),
        ),
        in_specs=[VMEM] * 5,
        out_specs=[VMEM] * 2,
        scratch_shapes=[
            pltpu.VMEM((2, piv, own.shape[1]), BF16),
            pltpu.VMEM((2, piv, own.shape[1]), BF16),
            pltpu.VMEM((piv + rows, piv), F32),
            pltpu.VMEM((piv + rows, piv // steps), F32),
        ],
        compiler_params=pltpu.CompilerParams(vmem_limit_bytes=40 * 1024 * 1024),
        name="rolled",
    )(parts, own, other, eri, diagonal[None, :])
    return panels, new[0]


def torus(chips):
    side = 1
    while 2 * (side + 1) ** 3 <= chips:
        side += 1
    return (2 * side, side, side) if 2 * side**3 == chips else (chips, 1, 1)


def slots_for(pivots, chips):
    mean = -(-pivots // chips)
    return min(LANES - 8, -(-(mean + max(12, mean // 2)) // 16) * 16)


def on_device(grid, eri_cols, old_factor, residual_diag, pivots, row_ids):
    steps, width = pivots.shape
    piv = steps * width
    chips = grid[0] * grid[1] * grid[2]
    slots = slots_for(piv, chips)
    cap = slots - 1
    ids = row_ids.reshape(-1, LANES)
    paged = pivots.reshape(-1, LANES)

    gathered = gather(grid, paged, ids, old_factor, eri_cols, slots)
    most = gathered[-1]
    result = finish(steps, cap, gathered, residual_diag)
    def again(state):
        windows = (most[0, 0].astype(jnp.int32) + cap - 1) // cap

        def add(w, held):
            mine = pack(jnp.full((1,), w, jnp.int32), paged, ids, old_factor, eri_cols, slots)
            every, other = spread(grid, mine, old_factor)
            every = every.reshape(2, 2, chips, slots, -1)
            line = every[0, 0, :, slots - 1, :slots].at[:, cap].set(0.0).reshape(1, -1)
            every = every.reshape(2, 2, chips * slots, -1)
            return held[0] + place(line, every, piv), other

        empty = jnp.zeros((2, 2, piv, (old_factor.shape[1] + piv // 2) // 2), F32)
        parts, other = lax.fori_loop(0, windows, add, (empty, jnp.zeros_like(old_factor)))
        return jnp.int32(0), *rolled(steps, parts, old_factor, other, eri_cols, residual_diag)

    return lax.while_loop(lambda s: s[0] > 0, again, result)[1:]


def solution(mesh):
    grid = torus(mesh.shape["row"])
    placed = (P("row", None), P("row", "col"), P("row"), P(), P("row"))
    return jax.shard_map(
        functools.partial(on_device, grid),
        mesh=mesh, in_specs=placed, out_specs=(P("row", None), P("row")), check_vma=False,
    )
```

```python
import functools
import jax
import jax.numpy as jnp
from jax import lax
from jax.experimental import pallas as pl
from jax.experimental.pallas import tpu as pltpu
from jax.sharding import PartitionSpec as P

ROWS_T = (((1,), (1,)), ((), ()))
COLS_T = (((0,), (0,)), ((), ()))
SUB = 8
LANES = 128
MESH = pl.DeviceIdType.MESH
VMEM = pl.BlockSpec(memory_space=pltpu.VMEM)
SMEM = pl.BlockSpec(memory_space=pltpu.SMEM)
F32 = jnp.float32
BF16 = jnp.bfloat16


def split(x):
    hi = x.astype(BF16)
    return hi, (x - hi.astype(F32)).astype(BF16)


def dot_t(a, b):
    f = functools.partial(
        lax.dot_general, dimension_numbers=ROWS_T, preferred_element_type=F32
    )
    return f(a[0], b[0]) + (f(a[0], b[1]) + f(a[1], b[0]))


def inverse_factor(a):
    n = a.shape[0]
    groups = n // SUB
    row = lax.broadcasted_iota(jnp.int32, (SUB, n), 0)
    lane = lax.broadcasted_iota(jnp.int32, (SUB, n), 1)
    M = [a[SUB * i : SUB * i + SUB, :] for i in range(groups)]
    over = lambda v, k: jnp.broadcast_to(v[k : k + 1, :], (SUB, n))
    columns = lambda v, j: [jnp.broadcast_to(v[:, j + k : j + k + 1], (SUB, n)) for k in range(SUB)]
    out = []
    V = [jnp.where(row >= 0, v, 0.0) for v in columns(M[0], 0)]
    for g in range(groups):
        j = SUB * g
        ahead = g + 1 < groups
        if ahead:
            U = [jnp.where(row >= 0, v, 0.0) for v in columns(M[g + 1], j)]
            N = columns(M[g + 1], j + SUB)
        second = g + 2 < groups
        if second:
            U2 = [jnp.where(row >= 0, v, 0.0) for v in columns(M[g + 2], j)]
        here = (lane >= j) & (lane < j + SUB)
        M[g] = jnp.where(here, jnp.where(lane == row + j, 1.0, 0.0), M[g])
        for i in range(g + 1, min(g + 3, groups)):
            M[i] = jnp.where(here, 0.0, M[i])
        roots = jnp.zeros((SUB, n), F32)
        invs = jnp.zeros((SUB, n), F32)
        for k in range(SUB):
            root = lax.rsqrt(over(V[k], k))
            inv = root * root
            roots = jnp.where(row == k, root, roots)
            invs = jnp.where(row == k, inv, invs)
            down = jnp.where(row > k, V[k], 0.0)
            top = [None] * SUB
            for l in range(k + 1, SUB):
                top[l] = over(V[k], l)
                V[l] = V[l] - (down * top[l]) * inv
            r = over(M[g], k)
            M[g] = M[g] - (down * inv) * r
            if ahead:
                u = U[k] * inv
                for l in range(k + 1, SUB):
                    U[l] = U[l] - u * top[l]
                M[g + 1] = M[g + 1] - u * r
                for l in range(SUB):
                    N[l] = N[l] - u * over(U[k], l)
            if second:
                u = U2[k] * inv
                for l in range(k + 1, SUB):
                    U2[l] = U2[l] - u * top[l]
                M[g + 2] = M[g + 2] - u * r
        out.append(jnp.where(lane < j + SUB, M[g] * roots, 0.0))
        if not ahead:
            break
        if g + 3 < groups:
            S = M[g] * invs
            for i in reversed(range(1, SUB)):
                S = S - (jnp.where(row < i, V[i], 0.0) * invs) * over(S, i)
            S = [over(S, k) for k in range(SUB)]
            for i in range(g + 3, groups):
                C = columns(M[i], j)
                M[i] = jnp.where(here, 0.0, M[i])
                for k in range(SUB):
                    M[i] = M[i] - C[k] * S[k]
        V = N
    return jnp.concatenate(out, axis=0)


def pack_kernel(cap, window_ref, pivot_ref, ids_ref, old_ref, eri_ref, out_ref):
    steps, width = pivot_ref.shape
    slots = out_ref.shape[1]
    part = out_ref.shape[2]
    groups = ids_ref.shape[0]
    half = eri_ref.shape[1] // 2
    ids = ids_ref[...]

    def find(j, at):
        return jnp.where(ids == pivot_ref[j // width, j % width], j + 1, at)

    at = lax.fori_loop(0, steps * width, find, jnp.zeros_like(ids), unroll=16)
    owned = jnp.where(at > 0, 1.0, 0.0)
    below = lax.broadcasted_iota(jnp.int32, (LANES, LANES), 0)
    right = lax.broadcasted_iota(jnp.int32, (LANES, LANES), 1)
    ahead = jnp.where(below < right, 1.0, 0.0).astype(BF16)
    rank = lax.dot_general(
        owned.astype(BF16), ahead, (((1,), (0,)), ((), ())), preferred_element_type=F32
    )
    first = window_ref[0] * cap
    slot = lax.broadcasted_iota(jnp.int32, (slots, LANES), 0)
    passed = jnp.zeros((1, 1), F32)
    picks, numbers = [], []
    for g in range(groups):
        here = (rank[g : g + 1] + passed).astype(jnp.int32) - first
        passed = passed + jnp.sum(owned[g : g + 1], axis=1, keepdims=True)
        here = jnp.where((owned[g : g + 1] > 0) & (here >= 0) & (here < cap), here, -1)
        picks.append(jnp.where(slot == here, 1.0, 0.0))
        numbers.append(at[g : g + 1])
    pick = jnp.concatenate(picks, axis=1).astype(BF16)
    number = jnp.concatenate(numbers, axis=1)
    pair = jnp.concatenate([number // 16, number % 16] + [jnp.zeros_like(number)] * 6, axis=0)
    pair = pair.astype(F32).astype(BF16)
    lines = lax.dot_general(pair, pick, ROWS_T, preferred_element_type=F32)
    line = lines[0:1] * 16.0 + lines[1:2]
    line = jnp.concatenate([line, jnp.zeros((1, LANES - slots), F32)], axis=1)

    def take(x):
        f = functools.partial(
            lax.dot_general,
            dimension_numbers=(((1,), (0,)), ((), ())),
            preferred_element_type=F32,
        )
        hi, lo = split(x)
        return f(pick, hi) + f(pick, lo)

    core = lax.axis_index("col")
    out_ref[0] = take(old_ref[:, :part])
    out_ref[0, slots - 1 : slots, :LANES] = line
    rest = old_ref.shape[1] - part
    out_ref[1, :, :rest] = take(old_ref[:, part:])
    out_ref[1, :, rest:] = take(eri_ref[:, pl.ds(pl.multiple_of(core * half, LANES), half)])


def pack(window, pivots, ids, old, eri, slots):
    width = (old.shape[1] + eri.shape[1] // 2) // 2
    return pl.pallas_call(
        functools.partial(pack_kernel, slots - 1),
        out_shape=jax.ShapeDtypeStruct((2, slots, width), F32),
        in_specs=[SMEM, SMEM, VMEM, VMEM, VMEM],
        out_specs=VMEM,
        name="pack",
    )(window, pivots, ids, old, eri)


def spread_kernel(grid, mine_ref, old_ref, all_ref, other_ref, *sems):
    deep, high, wide = grid
    fine = deep * high * wide <= 16
    own_sem, first_send, near_send, far_send, core_send = sems[:5]
    first_recv, recv, core_recv, old_sems = sems[5:]
    me = lax.axis_index("row")
    core = lax.axis_index("col")
    z, y, x = me // (high * wide), me // wide % high, me % wide
    chip = lambda z, y, x: (z * high + y) * wide + x
    steps = lambda at, size: [lax.rem(at + o, size) for o in range(1, size)]
    partner = (me, 1 - core)

    barrier = pltpu.get_barrier_semaphore()
    greet = [(chip(o, y, x), core) for o in steps(z, deep)]
    greet += [(chip(z, o, x), core) for o in steps(y, high)]
    greet += [(chip(z, y, o), core) for o in steps(x, wide)]
    greet.append(partner)
    for device in greet:
        pl.semaphore_signal(barrier, inc=1, device_id=device, device_id_type=MESH)
    pl.semaphore_wait(barrier, len(greet))

    flying = []

    def send(src, dst, send_sem, recv_sem, device):
        copy = pltpu.make_async_remote_copy(
            src_ref=src, dst_ref=dst, send_sem=send_sem, recv_sem=recv_sem,
            device_id=device, device_id_type=MESH,
        )
        copy.start()
        flying.append(copy)

    def await_block(ref, sem):
        pltpu.make_async_remote_copy(
            src_ref=ref, dst_ref=ref, send_sem=sem, recv_sem=sem,
            device_id=partner, device_id_type=MESH,
        ).wait_recv()

    def block(colour, zs, y, x):
        return all_ref.at[core, colour, zs, y, x]

    own = [
        pltpu.make_async_copy(mine_ref.at[k], all_ref.at[core, k, z, y, x], own_sem.at[k])
        for k in range(2)
    ]
    for k in range(2):
        own[k].start()
    for k in range(2):
        for i, o in enumerate(steps(z, deep)):
            send(mine_ref.at[k], block(k, z, y, x), first_send.at[k, i], first_recv.at[k, z], (chip(o, y, x), core))

    chunks = [z] + steps(z, deep) if fine else [None]
    near = lambda k: [(y, o) for o in steps(x, wide)] if k == 0 else [(o, x) for o in steps(y, high)]
    far = lambda k: [(o, x) for o in steps(y, high)] if k == 0 else [(y, o) for o in steps(x, wide)]

    def to_core(k, q, i, zs, y, x):
        ref = block(k, zs, y, x)
        send(ref, ref, core_send.at[k, q, i], core_recv.at[k, chunk_at(zs), y, x], partner)

    def chunk_at(zs):
        return zs if fine else 0

    def rows(zs):
        return zs if fine else slice(None)

    for q, at in enumerate(chunks):
        zs = rows(at)
        mine = fine and q == 0
        for k in range(2):
            if q == 0:
                if not fine:
                    for o in steps(z, deep):
                        await_block(block(k, o, y, x), first_recv.at[k, o])
                    own[k].wait()
            else:
                await_block(block(k, zs, y, x), first_recv.at[k, zs])
            src = mine_ref.at[k] if mine else block(k, zs, y, x)
            sem = recv.at[k, chunk_at(zs), y, x]
            for i, (b, c) in enumerate(near(k)):
                send(src, block(k, zs, y, x), near_send.at[k, q, i], sem, (chip(z, b, c), core))
            for i, (b, c) in enumerate(far(k)):
                send(src, block(k, zs, y, x), far_send.at[k, q, 0, i], sem, (chip(z, b, c), core))
            send(src, block(k, zs, y, x), core_send.at[k, q, 0], core_recv.at[k, chunk_at(zs), y, x], partner)
    old_copy = pltpu.make_async_remote_copy(
        src_ref=old_ref, dst_ref=other_ref, send_sem=old_sems.at[0], recv_sem=old_sems.at[1],
        device_id=partner, device_id_type=MESH,
    )
    old_copy.start()
    flying.append(old_copy)
    for q, at in enumerate(chunks):
        zs = rows(at)
        for k in range(2):
            for n, (b, c) in enumerate(near(k)):
                ref = block(k, zs, b, c)
                await_block(ref, recv.at[k, chunk_at(zs), b, c])
                for i, (fb, fc) in enumerate(far(k)):
                    send(ref, ref, far_send.at[k, q, 1 + n, i], recv.at[k, chunk_at(zs), b, c], (chip(z, fb, fc), core))
                to_core(k, q, 1 + n, zs, b, c)
    for q, at in enumerate(chunks):
        zs = rows(at)
        for k in range(2):
            index = 1 + len(near(k))
            for fb, fc in far(k):
                for b, c in [(y, x)] + near(k):
                    there = (fb, c) if k == 0 else (b, fc)
                    ref = block(k, zs, *there)
                    await_block(ref, recv.at[k, chunk_at(zs), *there])
                    to_core(k, q, index, zs, *there)
                    index += 1
    if fine:
        for k in range(2):
            own[k].wait()
    for q, at in enumerate(chunks):
        zs = rows(at)
        for k in range(2):
            for b in range(high):
                for c in range(wide):
                    ref = all_ref.at[1 - core, k, zs, b, c]
                    await_block(ref, core_recv.at[k, chunk_at(zs), b, c])
    old_copy.wait_recv()
    for copy in flying:
        copy.wait_send()


def spread(grid, mine, old):
    deep, high, wide = grid
    _, slots, width = mine.shape
    chunks = deep if deep * high * wide <= 16 else 1
    cells = high * wide
    peers = max(high, wide)
    sem = pltpu.SemaphoreType.DMA
    return pl.pallas_call(
        functools.partial(spread_kernel, grid),
        out_shape=(
            jax.ShapeDtypeStruct((2, 2, deep, high, wide, slots, width), F32),
            jax.ShapeDtypeStruct(old.shape, F32),
        ),
        in_specs=[pl.BlockSpec(memory_space=pl.ANY)] * 2,
        out_specs=(VMEM, pl.BlockSpec(memory_space=pl.ANY)),
        scratch_shapes=[
            sem((2,)),
            sem((2, max(deep - 1, 1))),
            sem((2, chunks, max(peers - 1, 1))),
            sem((2, chunks, peers, max(peers - 1, 1))),
            sem((2, chunks, cells)),
            sem((2, deep)),
            sem((2, chunks, high, wide)),
            sem((2, chunks, high, wide)),
            sem((2,)),
        ],
        compiler_params=pltpu.CompilerParams(
            collective_id=0, has_side_effects=True, vmem_limit_bytes=48 * 1024 * 1024
        ),
        name="spread",
    )(mine, old)


def gather_kernel(
    grid, pivot_ref, ids_ref, old_hbm, eri_hbm, diag_hbm,
    gram_ref, hi_ref, lo_ref, old_hi_ref, old_lo_ref, eri, most_ref, diag,
    old, other, mine, every,
    in_sems, own_sem, z_send, cell_send, near_send, far_send, core_send, recv, core_recv, old_sems,
):
    deep, high, wide = grid
    cells = high * wide
    slots, width = mine.shape
    cap = slots - 1
    part = width // 2
    half = old.shape[1]
    piv = gram_ref.shape[0]
    groups = ids_ref.shape[0]
    pages = pivot_ref.shape[0]
    me = lax.axis_index("row")
    core = lax.axis_index("col")
    z, y, x = me // cells, me // wide % high, me % wide
    partner = (me, 1 - core)
    chip = lambda z, y, x: ((z * high + y) * wide + x, core)
    around = lambda at, size: [lax.rem(at + o, size) for o in range(1, size)]

    barrier = pltpu.get_barrier_semaphore()
    signal = functools.partial(pl.semaphore_signal, barrier, inc=1, device_id_type=MESH)
    beside = [chip(z, o, x) for o in around(y, high)] + [chip(z, y, o) for o in around(x, wide)]
    for device in beside + [partner]:
        signal(device_id=device)

    @pl.when(z > 0)
    def _():
        signal(device_id=chip(z - 1, y, x))

    @pl.when(z < deep - 1)
    def _():
        signal(device_id=chip(z + 1, y, x))

    loads = [
        pltpu.make_async_copy(old_hbm, old, in_sems.at[0]),
        pltpu.make_async_copy(eri_hbm, eri, in_sems.at[1]),
        pltpu.make_async_copy(diag_hbm, diag, in_sems.at[2]),
    ]
    for load in loads:
        load.start()

    dot = functools.partial(
        lax.dot_general, dimension_numbers=(((1,), (0,)), ((), ())), preferred_element_type=F32
    )
    wanted = [
        jnp.transpose(jnp.broadcast_to(pivot_ref[b : b + 1].astype(F32), (LANES, LANES)))
        for b in range(pages)
    ]
    count = lax.broadcasted_iota(jnp.int32, (LANES, LANES), 0).astype(F32) + 1.0
    at = []
    for g in range(groups):
        ids = jnp.broadcast_to(ids_ref[g : g + 1].astype(F32), (LANES, LANES))
        found = [jnp.where(wanted[b] == ids, count + float(LANES * b), 0.0) for b in range(pages)]
        at.append(jnp.sum(functools.reduce(jnp.add, found), axis=0, keepdims=True))
    owned = [jnp.where(v > 0, 1.0, 0.0) for v in at]
    below = lax.broadcasted_iota(jnp.int32, (LANES, LANES), 0)
    right = lax.broadcasted_iota(jnp.int32, (LANES, LANES), 1)
    ahead = jnp.where(below < right, 1.0, 0.0).astype(BF16)
    rank = dot(jnp.concatenate(owned + [jnp.zeros((-groups % 8, LANES), F32)], axis=0).astype(BF16), ahead)
    passed = jnp.zeros((1, 1), F32)
    heres = []
    for g in range(groups):
        here = rank[g : g + 1] + passed
        passed = passed + jnp.sum(owned[g], axis=1, keepdims=True)
        heres.append(jnp.where((owned[g] > 0) & (here < cap), here, -1.0 - slots * cells))
    here = jnp.concatenate(heres, axis=1)
    number = jnp.concatenate(at, axis=1)
    rows = here.shape[1]
    slot = lax.broadcasted_iota(jnp.int32, (slots, rows), 0).astype(F32)
    pick = jnp.where(slot == here, 1.0, 0.0).astype(BF16)
    place = lax.broadcasted_iota(jnp.int32, (slots * cells, rows), 0)
    first = (lax.rem(me, cells) * slots).astype(F32)
    seat = jnp.where(place.astype(F32) == here + first, 1.0, 0.0).astype(BF16)
    high_part = jnp.floor(number * (1.0 / 16.0))
    pair = jnp.concatenate([high_part, number - 16.0 * high_part, jnp.zeros((6, rows), F32)], axis=0)
    lines = lax.dot_general(pair.astype(BF16), seat, ROWS_T, preferred_element_type=F32)
    line = lines[0:1] * 16.0 + lines[1:2]
    line = jnp.concatenate([line, jnp.broadcast_to(passed, (1, part - slots * cells))], axis=1)

    def take(v):
        hi, lo = split(v)
        return dot(pick, hi) + dot(pick, lo)

    loads[0].wait()
    mine[:, :half] = take(old[...])
    mine[slots - 1 : slots, :part] = line
    loads[1].wait()
    mine[:, half:] = take(eri[:, pl.ds(pl.multiple_of(core * (piv // 2), LANES), piv // 2)])

    ends = (z + deep - 1) // deep + (2 * deep - 2 - z) // deep
    pl.semaphore_wait(barrier, len(beside) + 1 + ends)

    last = width - LANES
    colour = [slice(0, part), slice(part, last), slice(last, width)]

    def block(k, zz, b, c):
        return every.at[core, zz, b, c, :, colour[k]]

    def remote(src, dst, send_sem, recv_sem, device):
        return pltpu.make_async_remote_copy(
            src_ref=src, dst_ref=dst, send_sem=send_sem, recv_sem=recv_sem,
            device_id=device, device_id_type=MESH,
        )

    def await_block(ref, sem):
        remote(ref, ref, sem, sem, partner).wait_recv()

    aside = lambda o, along: (lax.rem(y + o * (1 - along), high), lax.rem(x + o * along, wide))
    near = [[aside(o, 1 - core) for o in range(1, wide)], [aside(o, core) for o in range(1, wide)]]
    near.append(near[0])
    far = [near[1], near[0], near[1]]

    def upward(k, zz, src):
        return remote(src, block(k, zz, y, x), z_send.at[k, 0, zz], recv.at[k, zz, y, x], chip(z + 1, y, x))

    def downward(k, zz, src):
        return remote(src, block(k, zz, y, x), z_send.at[k, 1, zz], recv.at[k, zz, y, x], chip(z - 1, y, x))

    def cell_on(way, zz, b, c, src=None):
        ref = block(2, zz, b, c)
        return remote(
            ref if src is None else src, ref, cell_send.at[way, zz, b, c], recv.at[2, zz, b, c],
            chip(z - 1 if way else z + 1, y, x),
        )

    def line_sends(k, zz, src):
        out = []
        for i, (b, c) in enumerate(near[k]):
            out.append(remote(src, block(k, zz, y, x), near_send.at[k, zz, i], recv.at[k, zz, y, x], chip(z, b, c)))
        for i, (b, c) in enumerate(far[k]):
            out.append(remote(src, block(k, zz, y, x), far_send.at[k, zz, 0, i], recv.at[k, zz, y, x], chip(z, b, c)))
        return out

    def onward(k, zz, n, b, c):
        ref = block(k, zz, b, c)
        return [
            remote(ref, ref, far_send.at[k, zz, 1 + n, i], recv.at[k, zz, b, c], chip(z, fb, fc))
            for i, (fb, fc) in enumerate(far[k])
        ]

    def across(zz, b, c, src=None):
        ref = every.at[core, zz, b, c]
        return remote(ref if src is None else src, ref, core_send.at[zz, b, c], core_recv.at[zz, b, c], partner)

    own = pltpu.make_async_copy(mine, every.at[core, z, y, x], own_sem)
    old_copy = remote(old, other, old_sems.at[0], old_sems.at[1], partner)

    def start(copies):
        for copy in copies:
            copy.start()

    def line_copies(zz, src_of):
        return [copy for k in range(2) for copy in line_sends(k, zz, src_of(k))]

    mine_of = lambda k: mine.at[:, colour[k]]
    held_of = lambda zz: lambda k: block(k, zz, y, x)

    start(line_sends(2, z, mine_of(2)))

    @pl.when(z > 0)
    def _():
        start([downward(k, z, mine_of(k)) for k in range(2)])

    @pl.when(z < deep - 1)
    def _():
        start([upward(k, z, mine_of(k)) for k in range(2)])

    start(line_copies(z, mine_of))
    own.start()
    start([across(z, y, x, mine), old_copy])

    def lines_at(t):
        if t == 0:
            return [(z, None, None)]
        return [
            (z - t, z >= t, (upward, z < deep - 1, 0)),
            (z + t, z < deep - t, (downward, z > 0, 1)),
        ]

    def guarded(test, body):
        if test is None:
            body()
        else:
            pl.when(test)(body)

    corner = [(b, c) for b in around(y, high) for c in around(x, wide)]
    everywhere = [(b, c) for b in range(high) for c in range(wide)]

    def stage_plane():
        for n, (b, c) in enumerate(near[2]):
            await_block(block(2, z, b, c), recv.at[2, z, b, c])
            start(onward(2, z, n, b, c))

    def stage_cells(t):
        if t == 0:
            for b, c in far[2] + corner:
                await_block(block(2, z, b, c), recv.at[2, z, b, c])

            @pl.when(z > 0)
            def _():
                start([cell_on(1, z, y, x, mine_of(2))] + [cell_on(1, z, b, c) for b, c in near[2] + far[2] + corner])

            @pl.when(z < deep - 1)
            def _():
                start([cell_on(0, z, y, x, mine_of(2))] + [cell_on(0, z, b, c) for b, c in near[2] + far[2] + corner])

            return
        for zz, test, step in lines_at(t):

            def body(zz=zz, step=step):
                _, further, way = step
                for b, c in everywhere:
                    await_block(block(2, zz, b, c), recv.at[2, zz, b, c])
                    pl.when(further)(lambda b=b, c=c: cell_on(way, zz, b, c).start())
                across(zz, y, x).start()

            guarded(test, body)

    def stage_line(t):
        for zz, test, step in lines_at(t):

            def body(zz=zz, step=step):
                go, further, _ = step
                for k in range(2):
                    await_block(block(k, zz, y, x), recv.at[k, zz, y, x])
                    pl.when(further)(lambda k=k: go(k, zz, block(k, zz, y, x)).start())
                    start(line_sends(k, zz, block(k, zz, y, x)))

            guarded(test, body)

    def stage_near(t):
        for zz, test, _ in lines_at(t):

            def body(zz=zz):
                for k in range(2):
                    for n, (b, c) in enumerate(near[k]):
                        await_block(block(k, zz, b, c), recv.at[k, zz, b, c])
                        start(onward(k, zz, n, b, c))
                for k in range(2):
                    for b, c in far[k]:
                        await_block(block(k, zz, b, c), recv.at[k, zz, b, c])
                        across(zz, b, c).start()

            guarded(test, body)

    def stage_far(t):
        for zz, test, _ in lines_at(t):

            def body(zz=zz):
                for b, c in corner:
                    for k in range(2):
                        await_block(block(k, zz, b, c), recv.at[k, zz, b, c])
                    across(zz, b, c).start()

            guarded(test, body)

    if deep == 4:
        order = [z, z + 1 - 2 * lax.rem(z, 2), 2 - z // 2, 3 - 3 * (z // 2)]
    else:
        order = [z] + around(z, deep)
    pivot = lax.broadcasted_iota(jnp.int32, (piv, slots * cells), 0).astype(F32) + 1.0
    most = []

    def put(i):
        zz = order[i]
        for b in range(high):
            for c in range(wide):
                ref = every.at[1 - core, zz, b, c]
                remote(ref, ref, core_recv.at[zz, b, c], core_recv.at[zz, b, c], partner).wait_recv()
        lines = [every[0, zz, b, c, slots - 1 : slots, :part] for b in range(high) for c in range(wide)]
        most.append(functools.reduce(jnp.maximum, [v[:, part - LANES :] for v in lines]))
        line = functools.reduce(jnp.add, [v[:, : slots * cells] for v in lines])
        seats = jnp.where(pivot == line, 1.0, 0.0).astype(BF16)
        for c in range(2):
            hi, lo = split(every[c, zz].reshape(cells * slots, width))
            hi, lo = dot(seats, hi), dot(seats, lo)
            cut = slice(c * (piv // 2), (c + 1) * (piv // 2))
            if i == 0:
                hi_ref[c] = hi[:, :half].astype(BF16)
                lo_ref[c] = lo[:, :half].astype(BF16)
                gram_ref[:, cut] = hi[:, half:] + lo[:, half:]
            else:
                hi_ref[c] += hi[:, :half].astype(BF16)
                lo_ref[c] += lo[:, :half].astype(BF16)
                gram_ref[:, cut] += hi[:, half:] + lo[:, half:]

    stage_plane()
    old_hi_ref[core], old_lo_ref[core] = split(old[...])
    for t in range(deep + 3):
        if 1 <= t < deep:
            stage_line(t)
        if 0 <= t - 1 < deep:
            stage_cells(t - 1)
            stage_near(t - 1)
        if t == 1:
            old_copy.wait_recv()
            old_hi_ref[1 - core], old_lo_ref[1 - core] = split(other[...])
            own.wait()
        if t == deep + 1:
            for i in range(deep - 2):
                put(i)
        if 0 <= t - 2 < deep:
            stage_far(t - 2)
    for i in range(max(deep - 2, 0), deep):
        put(i)

    most_ref[...] = jnp.broadcast_to(functools.reduce(jnp.maximum, most), most_ref.shape)
    loads[2].wait()
    old_copy.wait_send()

    def cells_sent(way, zz):
        for b, c in everywhere:
            cell_on(way, zz, b, c).wait_send()

    @pl.when(z > 0)
    def _():
        for k in range(2):
            downward(k, z, mine_of(k)).wait_send()
        cells_sent(1, z)

    @pl.when(z < deep - 1)
    def _():
        for k in range(2):
            upward(k, z, mine_of(k)).wait_send()
        cells_sent(0, z)

    for t in range(deep):
        for zz, test, step in lines_at(t):

            def body(zz=zz, step=step, t=t):
                if t:
                    go, further, way = step

                    @pl.when(further)
                    def _():
                        for k in range(2):
                            go(k, zz, block(k, zz, y, x)).wait_send()
                        cells_sent(way, zz)

                for k in range(2 if t else 3):
                    src = block(k, zz, y, x) if t else mine_of(k)
                    for copy in line_sends(k, zz, src):
                        copy.wait_send()
                    for n, (b, c) in enumerate(near[k]):
                        for copy in onward(k, zz, n, b, c):
                            copy.wait_send()
                for b, c in everywhere:
                    across(zz, b, c).wait_send()

            guarded(test, body)


def gather(grid, pivots, ids, old, eri, diagonal, slots):
    deep, high, wide = grid
    piv = eri.shape[1]
    width = old.shape[1] + piv // 2
    peers = max(high, wide)
    sem = pltpu.SemaphoreType.DMA
    wide_bf16 = jax.ShapeDtypeStruct((2, piv, old.shape[1]), BF16)
    any_space = pl.BlockSpec(memory_space=pl.ANY)
    return pl.pallas_call(
        functools.partial(gather_kernel, grid),
        out_shape=(
            jax.ShapeDtypeStruct((piv, piv), F32),
            wide_bf16,
            wide_bf16,
            jax.ShapeDtypeStruct((2, *old.shape), BF16),
            jax.ShapeDtypeStruct((2, *old.shape), BF16),
            jax.ShapeDtypeStruct(eri.shape, F32),
            jax.ShapeDtypeStruct((SUB, LANES), F32),
            jax.ShapeDtypeStruct((1, eri.shape[0]), F32),
        ),
        in_specs=[VMEM, VMEM] + [any_space] * 3,
        out_specs=[VMEM] * 8,
        scratch_shapes=[
            pltpu.VMEM(old.shape, F32),
            pltpu.VMEM(old.shape, F32),
            pltpu.VMEM((slots, width), F32),
            pltpu.VMEM((2, deep, high, wide, slots, width), F32),
            sem((3,)),
            sem,
            sem((2, 2, deep)),
            sem((2, deep, high, wide)),
            sem((3, deep, max(peers - 1, 1))),
            sem((3, deep, peers, max(peers - 1, 1))),
            sem((deep, high, wide)),
            sem((3, deep, high, wide)),
            sem((deep, high, wide)),
            sem((2,)),
        ],
        compiler_params=pltpu.CompilerParams(
            collective_id=1, has_side_effects=True, vmem_limit_bytes=40 * 1024 * 1024
        ),
        name="gather",
    )(pivots, ids, old, eri, diagonal[None, :])


def finish_kernel(
    steps, cap, gram_ref, hi_ref, lo_ref, old_hi_ref, old_lo_ref, eri_ref, most_ref, diag_ref,
    panel_hbm, new_hbm, over_ref, gram, work, panel, new_ref, sems,
):
    piv = gram.shape[0]
    width = piv // steps
    f = functools.partial(lax.dot_general, preferred_element_type=F32)
    over_ref[0] = jnp.where(jnp.max(most_ref[...]) > cap, 1, 0)
    rows = [(hi_ref[c], lo_ref[c]) for c in range(2)]
    old = [(old_hi_ref[c], old_lo_ref[c]) for c in range(2)]
    for s in range(steps):
        here, upto = slice(s * width, (s + 1) * width), slice(0, (s + 1) * width)
        both = [dot_t((v[0][here], v[1][here]), (v[0][upto], v[1][upto])) for v in rows]
        gram[here, upto] = gram_ref[here, upto] - (both[0] + both[1])
    ones = jnp.ones((SUB, width), BF16)
    new = diag_ref[...]
    stores = []
    for s in range(steps):
        at = slice(s * width, (s + 1) * width)
        inv = split(inverse_factor(gram[at, at]))
        later = [slice(t * width, (t + 1) * width) for t in range(s + 1, steps)]
        below = [split(dot_t(split(gram[t, at]), inv)) for t in later]
        for i, t in enumerate(later):
            for u in range(i + 1):
                gram[t, later[u]] -= dot_t(below[i], below[u])
        if s == 0:
            work[...] = eri_ref[...] - (dot_t(old[0], rows[0]) + dot_t(old[1], rows[1]))
        own = dot_t(split(work[:, at]), inv)
        panel[:, at] = own
        stores.append(pltpu.make_async_copy(panel.at[:, at], panel_hbm.at[:, at], sems.at[s]))
        stores[-1].start()
        hi, lo = split(own * own)
        new = new - (f(ones, hi, ROWS_T) + f(ones, lo, ROWS_T))[:1]
        own = split(own)
        for i, t in enumerate(later):
            work[:, t] -= dot_t(own, below[i])
    new_ref[...] = new
    stores.append(pltpu.make_async_copy(new_ref, new_hbm, sems.at[steps]))
    stores[-1].start()
    for store in stores:
        store.wait()


def finish(steps, cap, gathered):
    rows, piv = gathered[5].shape
    any_space = pl.BlockSpec(memory_space=pl.ANY)
    panels, new, over = pl.pallas_call(
        functools.partial(finish_kernel, steps, cap),
        out_shape=(
            jax.ShapeDtypeStruct((rows, piv), F32),
            jax.ShapeDtypeStruct((1, rows), F32),
            jax.ShapeDtypeStruct((1,), jnp.int32),
        ),
        in_specs=[VMEM] * 8,
        out_specs=[any_space, any_space, SMEM],
        scratch_shapes=[
            pltpu.VMEM((piv, piv), F32),
            pltpu.VMEM((rows, piv), F32),
            pltpu.VMEM((rows, piv), F32),
            pltpu.VMEM((1, rows), F32),
            pltpu.SemaphoreType.DMA((steps + 1,)),
        ],
        compiler_params=pltpu.CompilerParams(vmem_limit_bytes=24 * 1024 * 1024),
        name="finish",
    )(*gathered)
    return over[0], panels, new[0]


def place_kernel(line_ref, every_ref, out_ref):
    pivot = lax.broadcasted_iota(jnp.int32, (out_ref.shape[2], line_ref.shape[1]), 0).astype(F32) + 1.0
    seats = jnp.where(pivot == line_ref[...], 1.0, 0.0).astype(BF16)
    dot = functools.partial(
        lax.dot_general, dimension_numbers=(((1,), (0,)), ((), ())), preferred_element_type=F32
    )

    def put(i, carry):
        hi, lo = split(every_ref[i // 2, i % 2])
        out_ref[i // 2, i % 2] = dot(seats, hi) + dot(seats, lo)
        return carry

    lax.fori_loop(0, 4, put, 0)


def place(line, every, piv):
    return pl.pallas_call(
        place_kernel,
        out_shape=jax.ShapeDtypeStruct((2, 2, piv, every.shape[-1]), F32),
        in_specs=[VMEM] * 2,
        out_specs=VMEM,
        compiler_params=pltpu.CompilerParams(vmem_limit_bytes=40 * 1024 * 1024),
        name="place",
    )(line, every)


def rolled_inverse(a):
    n = a.shape[0]
    row = lax.broadcasted_iota(jnp.int32, (n, n), 0)
    lane = lax.broadcasted_iota(jnp.int32, (n, n), 1)

    def pivot(j, held):
        a, w = held
        of_row = lambda v: jnp.sum(jnp.where(row == j, v, 0.0), axis=0, keepdims=True)
        column = jnp.sum(jnp.where(lane == j, a, 0.0), axis=1, keepdims=True)
        root = lax.rsqrt(jnp.sum(jnp.where((row == j) & (lane == j), a, 0.0), keepdims=True))
        m = jnp.where(row > j, column, 0.0) * (root * root)
        return a - m * of_row(a), jnp.where(row == j, w * root, w - m * of_row(w))

    return lax.fori_loop(0, n, pivot, (a, jnp.where(row == lane, 1.0, 0.0)))[1]


def rolled_kernel(
    steps, parts_ref, own_ref, other_ref, eri_ref, diag_ref, panel_ref, new_ref,
    hi, lo, work, solved,
):
    rows, piv = eri_ref.shape
    width = piv // steps
    half = own_ref.shape[1]
    core = lax.axis_index("col")
    for c in range(2):
        both = jnp.concatenate([parts_ref[c, 0], parts_ref[c, 1]], axis=1)
        hi[c], lo[c] = split(both[:, :half])
        work[:piv, c * (piv // 2) : (c + 1) * (piv // 2)] = both[:, half:]
    at_block = lambda b: pl.ds(pl.multiple_of(b * LANES, LANES), LANES)

    def gram(b, carry):
        at = at_block(b)
        work[at, :] -= dot_t((hi[0, at], lo[0, at]), (hi[0], lo[0])) + dot_t((hi[1, at], lo[1, at]), (hi[1], lo[1]))
        return carry

    def reduce(b, carry):
        at = at_block(b)
        work[pl.ds(pl.multiple_of(piv + b * LANES, LANES), LANES), :] = eri_ref[at, :] - (
            dot_t(split(own_ref[at, :]), (hi[core], lo[core]))
            + dot_t(split(other_ref[at, :]), (hi[1 - core], lo[1 - core]))
        )
        return carry

    lax.fori_loop(0, piv // LANES, gram, 0)
    lax.fori_loop(0, rows // LANES, reduce, 0)
    new_ref[...] = diag_ref[...]
    ones = jnp.ones((SUB, width), BF16)
    f = functools.partial(lax.dot_general, dimension_numbers=ROWS_T, preferred_element_type=F32)

    def step(s, carry):
        at = pl.ds(pl.multiple_of(s * width, width), width)
        inv = split(rolled_inverse(work[at, at]))

        def solve(b, carry):
            solved[at_block(b), :] = dot_t(split(work[at_block(b), at]), inv)
            return carry

        lax.fori_loop(0, (piv + rows) // LANES, solve, 0)
        own = solved[piv:, :]
        panel_ref[:, at] = own
        high, low = split(own * own)
        new_ref[...] -= (f(ones, high) + f(ones, low))[:1]
        above = split(solved[:piv, :])

        def update(b, carry):
            work[at_block(b), :] -= dot_t(split(solved[at_block(b), :]), above)
            return carry

        lax.fori_loop(0, (piv + rows) // LANES, update, 0)
        return carry

    lax.fori_loop(0, steps, step, 0)


def rolled(steps, parts, own, other, eri, diagonal):
    rows, piv = eri.shape
    panels, new = pl.pallas_call(
        functools.partial(rolled_kernel, steps),
        out_shape=(
            jax.ShapeDtypeStruct((rows, piv), F32),
            jax.ShapeDtypeStruct((1, rows), F32),
        ),
        in_specs=[VMEM] * 5,
        out_specs=[VMEM] * 2,
        scratch_shapes=[
            pltpu.VMEM((2, piv, own.shape[1]), BF16),
            pltpu.VMEM((2, piv, own.shape[1]), BF16),
            pltpu.VMEM((piv + rows, piv), F32),
            pltpu.VMEM((piv + rows, piv // steps), F32),
        ],
        compiler_params=pltpu.CompilerParams(vmem_limit_bytes=40 * 1024 * 1024),
        name="rolled",
    )(parts, own, other, eri, diagonal[None, :])
    return panels, new[0]


def torus(chips):
    side = 1
    while 2 * (side + 1) ** 3 <= chips:
        side += 1
    return (2 * side, side, side) if 2 * side**3 == chips else (chips, 1, 1)


def slots_for(pivots, chips):
    mean = -(-pivots // chips)
    return min(LANES - 8, -(-(mean + max(12, mean // 2)) // 16) * 16)


def on_device(grid, eri_cols, old_factor, residual_diag, pivots, row_ids):
    steps, width = pivots.shape
    piv = steps * width
    chips = grid[0] * grid[1] * grid[2]
    slots = slots_for(piv, chips)
    cap = slots - 1
    ids = row_ids.reshape(-1, LANES)
    paged = pivots.reshape(-1, LANES)

    gathered = gather(grid, paged, ids, old_factor, eri_cols, residual_diag, slots)
    most = gathered[6]
    result = finish(steps, cap, gathered)
    def again(state):
        windows = (most[0, 0].astype(jnp.int32) + cap - 1) // cap

        def add(w, held):
            mine = pack(jnp.full((1,), w, jnp.int32), paged, ids, old_factor, eri_cols, slots)
            every, other = spread(grid, mine, old_factor)
            every = every.reshape(2, 2, chips, slots, -1)
            line = every[0, 0, :, slots - 1, :slots].at[:, cap].set(0.0).reshape(1, -1)
            every = every.reshape(2, 2, chips * slots, -1)
            return held[0] + place(line, every, piv), other

        empty = jnp.zeros((2, 2, piv, (old_factor.shape[1] + piv // 2) // 2), F32)
        parts, other = lax.fori_loop(0, windows, add, (empty, jnp.zeros_like(old_factor)))
        return jnp.int32(0), *rolled(steps, parts, old_factor, other, eri_cols, residual_diag)

    return lax.while_loop(lambda s: s[0] > 0, again, result)[1:]


def solution(mesh):
    grid = torus(mesh.shape["row"])
    placed = (P("row", None), P("row", "col"), P("row"), P(), P("row"))
    return jax.shard_map(
        functools.partial(on_device, grid),
        mesh=mesh, in_specs=placed, out_specs=(P("row", None), P("row")), check_vma=False,
    )
```

```python
import functools
import jax
import jax.numpy as jnp
from jax import lax
from jax.experimental import pallas as pl
from jax.experimental.pallas import tpu as pltpu
from jax.sharding import PartitionSpec as P

ROWS_T = (((1,), (1,)), ((), ()))
COLS_T = (((0,), (0,)), ((), ()))
SUB = 8
LANES = 128
MESH = pl.DeviceIdType.MESH
VMEM = pl.BlockSpec(memory_space=pltpu.VMEM)
SMEM = pl.BlockSpec(memory_space=pltpu.SMEM)
F32 = jnp.float32
BF16 = jnp.bfloat16


def split(x):
    hi = x.astype(BF16)
    return hi, (x - hi.astype(F32)).astype(BF16)


def dot_t(a, b):
    f = functools.partial(
        lax.dot_general, dimension_numbers=ROWS_T, preferred_element_type=F32
    )
    return f(a[0], b[0]) + (f(a[0], b[1]) + f(a[1], b[0]))


def inverse_factor(a):
    n = a.shape[0]
    groups = n // SUB
    row = lax.broadcasted_iota(jnp.int32, (SUB, n), 0)
    lane = lax.broadcasted_iota(jnp.int32, (SUB, n), 1)
    M = [a[SUB * i : SUB * i + SUB, :] for i in range(groups)]
    over = lambda v, k: jnp.broadcast_to(v[k : k + 1, :], (SUB, n))
    columns = lambda v, j: [jnp.broadcast_to(v[:, j + k : j + k + 1], (SUB, n)) for k in range(SUB)]
    out = []
    V = [jnp.where(row >= 0, v, 0.0) for v in columns(M[0], 0)]
    for g in range(groups):
        j = SUB * g
        ahead = g + 1 < groups
        if ahead:
            U = [jnp.where(row >= 0, v, 0.0) for v in columns(M[g + 1], j)]
            N = columns(M[g + 1], j + SUB)
        second = g + 2 < groups
        if second:
            U2 = [jnp.where(row >= 0, v, 0.0) for v in columns(M[g + 2], j)]
        here = (lane >= j) & (lane < j + SUB)
        M[g] = jnp.where(here, jnp.where(lane == row + j, 1.0, 0.0), M[g])
        for i in range(g + 1, min(g + 3, groups)):
            M[i] = jnp.where(here, 0.0, M[i])
        roots = jnp.zeros((SUB, n), F32)
        invs = jnp.zeros((SUB, n), F32)
        for k in range(SUB):
            root = lax.rsqrt(over(V[k], k))
            inv = root * root
            roots = jnp.where(row == k, root, roots)
            invs = jnp.where(row == k, inv, invs)
            down = jnp.where(row > k, V[k], 0.0)
            top = [None] * SUB
            for l in range(k + 1, SUB):
                top[l] = over(V[k], l)
                V[l] = V[l] - (down * top[l]) * inv
            r = over(M[g], k)
            M[g] = M[g] - (down * inv) * r
            if ahead:
                u = U[k] * inv
                for l in range(k + 1, SUB):
                    U[l] = U[l] - u * top[l]
                M[g + 1] = M[g + 1] - u * r
                for l in range(SUB):
                    N[l] = N[l] - u * over(U[k], l)
            if second:
                u = U2[k] * inv
                for l in range(k + 1, SUB):
                    U2[l] = U2[l] - u * top[l]
                M[g + 2] = M[g + 2] - u * r
        out.append(jnp.where(lane < j + SUB, M[g] * roots, 0.0))
        if not ahead:
            break
        if g + 3 < groups:
            S = M[g] * invs
            for i in reversed(range(1, SUB)):
                S = S - (jnp.where(row < i, V[i], 0.0) * invs) * over(S, i)
            S = [over(S, k) for k in range(SUB)]
            for i in range(g + 3, groups):
                C = columns(M[i], j)
                M[i] = jnp.where(here, 0.0, M[i])
                for k in range(SUB):
                    M[i] = M[i] - C[k] * S[k]
        V = N
    return jnp.concatenate(out, axis=0)


def pack_kernel(cap, window_ref, pivot_ref, ids_ref, old_ref, eri_ref, out_ref):
    steps, width = pivot_ref.shape
    slots = out_ref.shape[1]
    part = out_ref.shape[2]
    groups = ids_ref.shape[0]
    half = eri_ref.shape[1] // 2
    ids = ids_ref[...]

    def find(j, at):
        return jnp.where(ids == pivot_ref[j // width, j % width], j + 1, at)

    at = lax.fori_loop(0, steps * width, find, jnp.zeros_like(ids), unroll=16)
    owned = jnp.where(at > 0, 1.0, 0.0)
    below = lax.broadcasted_iota(jnp.int32, (LANES, LANES), 0)
    right = lax.broadcasted_iota(jnp.int32, (LANES, LANES), 1)
    ahead = jnp.where(below < right, 1.0, 0.0).astype(BF16)
    rank = lax.dot_general(
        owned.astype(BF16), ahead, (((1,), (0,)), ((), ())), preferred_element_type=F32
    )
    first = window_ref[0] * cap
    slot = lax.broadcasted_iota(jnp.int32, (slots, LANES), 0)
    passed = jnp.zeros((1, 1), F32)
    picks, numbers = [], []
    for g in range(groups):
        here = (rank[g : g + 1] + passed).astype(jnp.int32) - first
        passed = passed + jnp.sum(owned[g : g + 1], axis=1, keepdims=True)
        here = jnp.where((owned[g : g + 1] > 0) & (here >= 0) & (here < cap), here, -1)
        picks.append(jnp.where(slot == here, 1.0, 0.0))
        numbers.append(at[g : g + 1])
    pick = jnp.concatenate(picks, axis=1).astype(BF16)
    number = jnp.concatenate(numbers, axis=1)
    pair = jnp.concatenate([number // 16, number % 16] + [jnp.zeros_like(number)] * 6, axis=0)
    pair = pair.astype(F32).astype(BF16)
    lines = lax.dot_general(pair, pick, ROWS_T, preferred_element_type=F32)
    line = lines[0:1] * 16.0 + lines[1:2]
    line = jnp.concatenate([line, jnp.zeros((1, LANES - slots), F32)], axis=1)

    def take(x):
        f = functools.partial(
            lax.dot_general,
            dimension_numbers=(((1,), (0,)), ((), ())),
            preferred_element_type=F32,
        )
        hi, lo = split(x)
        return f(pick, hi) + f(pick, lo)

    core = lax.axis_index("col")
    out_ref[0] = take(old_ref[:, :part])
    out_ref[0, slots - 1 : slots, :LANES] = line
    rest = old_ref.shape[1] - part
    out_ref[1, :, :rest] = take(old_ref[:, part:])
    out_ref[1, :, rest:] = take(eri_ref[:, pl.ds(pl.multiple_of(core * half, LANES), half)])


def pack(window, pivots, ids, old, eri, slots):
    width = (old.shape[1] + eri.shape[1] // 2) // 2
    return pl.pallas_call(
        functools.partial(pack_kernel, slots - 1),
        out_shape=jax.ShapeDtypeStruct((2, slots, width), F32),
        in_specs=[SMEM, SMEM, VMEM, VMEM, VMEM],
        out_specs=VMEM,
        name="pack",
    )(window, pivots, ids, old, eri)


def spread_kernel(grid, mine_ref, old_ref, all_ref, other_ref, *sems):
    deep, high, wide = grid
    fine = deep * high * wide <= 16
    own_sem, first_send, near_send, far_send, core_send = sems[:5]
    first_recv, recv, core_recv, old_sems = sems[5:]
    me = lax.axis_index("row")
    core = lax.axis_index("col")
    z, y, x = me // (high * wide), me // wide % high, me % wide
    chip = lambda z, y, x: (z * high + y) * wide + x
    steps = lambda at, size: [lax.rem(at + o, size) for o in range(1, size)]
    partner = (me, 1 - core)

    barrier = pltpu.get_barrier_semaphore()
    greet = [(chip(o, y, x), core) for o in steps(z, deep)]
    greet += [(chip(z, o, x), core) for o in steps(y, high)]
    greet += [(chip(z, y, o), core) for o in steps(x, wide)]
    greet.append(partner)
    for device in greet:
        pl.semaphore_signal(barrier, inc=1, device_id=device, device_id_type=MESH)
    pl.semaphore_wait(barrier, len(greet))

    flying = []

    def send(src, dst, send_sem, recv_sem, device):
        copy = pltpu.make_async_remote_copy(
            src_ref=src, dst_ref=dst, send_sem=send_sem, recv_sem=recv_sem,
            device_id=device, device_id_type=MESH,
        )
        copy.start()
        flying.append(copy)

    def await_block(ref, sem):
        pltpu.make_async_remote_copy(
            src_ref=ref, dst_ref=ref, send_sem=sem, recv_sem=sem,
            device_id=partner, device_id_type=MESH,
        ).wait_recv()

    def block(colour, zs, y, x):
        return all_ref.at[core, colour, zs, y, x]

    own = [
        pltpu.make_async_copy(mine_ref.at[k], all_ref.at[core, k, z, y, x], own_sem.at[k])
        for k in range(2)
    ]
    for k in range(2):
        own[k].start()
    for k in range(2):
        for i, o in enumerate(steps(z, deep)):
            send(mine_ref.at[k], block(k, z, y, x), first_send.at[k, i], first_recv.at[k, z], (chip(o, y, x), core))

    chunks = [z] + steps(z, deep) if fine else [None]
    near = lambda k: [(y, o) for o in steps(x, wide)] if k == 0 else [(o, x) for o in steps(y, high)]
    far = lambda k: [(o, x) for o in steps(y, high)] if k == 0 else [(y, o) for o in steps(x, wide)]

    def to_core(k, q, i, zs, y, x):
        ref = block(k, zs, y, x)
        send(ref, ref, core_send.at[k, q, i], core_recv.at[k, chunk_at(zs), y, x], partner)

    def chunk_at(zs):
        return zs if fine else 0

    def rows(zs):
        return zs if fine else slice(None)

    for q, at in enumerate(chunks):
        zs = rows(at)
        mine = fine and q == 0
        for k in range(2):
            if q == 0:
                if not fine:
                    for o in steps(z, deep):
                        await_block(block(k, o, y, x), first_recv.at[k, o])
                    own[k].wait()
            else:
                await_block(block(k, zs, y, x), first_recv.at[k, zs])
            src = mine_ref.at[k] if mine else block(k, zs, y, x)
            sem = recv.at[k, chunk_at(zs), y, x]
            for i, (b, c) in enumerate(near(k)):
                send(src, block(k, zs, y, x), near_send.at[k, q, i], sem, (chip(z, b, c), core))
            for i, (b, c) in enumerate(far(k)):
                send(src, block(k, zs, y, x), far_send.at[k, q, 0, i], sem, (chip(z, b, c), core))
            send(src, block(k, zs, y, x), core_send.at[k, q, 0], core_recv.at[k, chunk_at(zs), y, x], partner)
    old_copy = pltpu.make_async_remote_copy(
        src_ref=old_ref, dst_ref=other_ref, send_sem=old_sems.at[0], recv_sem=old_sems.at[1],
        device_id=partner, device_id_type=MESH,
    )
    old_copy.start()
    flying.append(old_copy)
    for q, at in enumerate(chunks):
        zs = rows(at)
        for k in range(2):
            for n, (b, c) in enumerate(near(k)):
                ref = block(k, zs, b, c)
                await_block(ref, recv.at[k, chunk_at(zs), b, c])
                for i, (fb, fc) in enumerate(far(k)):
                    send(ref, ref, far_send.at[k, q, 1 + n, i], recv.at[k, chunk_at(zs), b, c], (chip(z, fb, fc), core))
                to_core(k, q, 1 + n, zs, b, c)
    for q, at in enumerate(chunks):
        zs = rows(at)
        for k in range(2):
            index = 1 + len(near(k))
            for fb, fc in far(k):
                for b, c in [(y, x)] + near(k):
                    there = (fb, c) if k == 0 else (b, fc)
                    ref = block(k, zs, *there)
                    await_block(ref, recv.at[k, chunk_at(zs), *there])
                    to_core(k, q, index, zs, *there)
                    index += 1
    if fine:
        for k in range(2):
            own[k].wait()
    for q, at in enumerate(chunks):
        zs = rows(at)
        for k in range(2):
            for b in range(high):
                for c in range(wide):
                    ref = all_ref.at[1 - core, k, zs, b, c]
                    await_block(ref, core_recv.at[k, chunk_at(zs), b, c])
    old_copy.wait_recv()
    for copy in flying:
        copy.wait_send()


def spread(grid, mine, old):
    deep, high, wide = grid
    _, slots, width = mine.shape
    chunks = deep if deep * high * wide <= 16 else 1
    cells = high * wide
    peers = max(high, wide)
    sem = pltpu.SemaphoreType.DMA
    return pl.pallas_call(
        functools.partial(spread_kernel, grid),
        out_shape=(
            jax.ShapeDtypeStruct((2, 2, deep, high, wide, slots, width), F32),
            jax.ShapeDtypeStruct(old.shape, F32),
        ),
        in_specs=[pl.BlockSpec(memory_space=pl.ANY)] * 2,
        out_specs=(VMEM, pl.BlockSpec(memory_space=pl.ANY)),
        scratch_shapes=[
            sem((2,)),
            sem((2, max(deep - 1, 1))),
            sem((2, chunks, max(peers - 1, 1))),
            sem((2, chunks, peers, max(peers - 1, 1))),
            sem((2, chunks, cells)),
            sem((2, deep)),
            sem((2, chunks, high, wide)),
            sem((2, chunks, high, wide)),
            sem((2,)),
        ],
        compiler_params=pltpu.CompilerParams(
            collective_id=0, has_side_effects=True, vmem_limit_bytes=48 * 1024 * 1024
        ),
        name="spread",
    )(mine, old)


def gather_kernel(
    grid, pivot_hbm, ids_hbm, old_hbm, eri_hbm, diag_hbm,
    gram_ref, hi_ref, lo_ref, old_hi_ref, old_lo_ref, eri, most_ref, diag,
    pivot_ref, ids_ref, old, other, mine, every,
    in_sems, own_sem, z_send, cell_send, near_send, far_send, core_send, recv, core_recv, old_sems,
):
    deep, high, wide = grid
    cells = high * wide
    slots, width = mine.shape
    cap = slots - 1
    part = width // 2
    half = old.shape[1]
    piv = gram_ref.shape[0]
    groups = ids_ref.shape[0]
    pages = pivot_ref.shape[0]
    me = lax.axis_index("row")
    core = lax.axis_index("col")
    z, y, x = me // cells, me // wide % high, me % wide
    partner = (me, 1 - core)
    chip = lambda z, y, x: ((z * high + y) * wide + x, core)
    around = lambda at, size: [lax.rem(at + o, size) for o in range(1, size)]

    loads = [
        pltpu.make_async_copy(old_hbm, old, in_sems.at[0]),
        pltpu.make_async_copy(eri_hbm, eri, in_sems.at[1]),
        pltpu.make_async_copy(diag_hbm, diag, in_sems.at[2]),
        pltpu.make_async_copy(pivot_hbm, pivot_ref, in_sems.at[3]),
        pltpu.make_async_copy(ids_hbm, ids_ref, in_sems.at[4]),
    ]
    for load in loads[3:] + loads[:3]:
        load.start()

    barrier = pltpu.get_barrier_semaphore()
    signal = functools.partial(pl.semaphore_signal, barrier, inc=1, device_id_type=MESH)
    beside = [chip(z, o, x) for o in around(y, high)] + [chip(z, y, o) for o in around(x, wide)]
    for device in beside + [partner]:
        signal(device_id=device)

    @pl.when(z > 0)
    def _():
        signal(device_id=chip(z - 1, y, x))

    @pl.when(z < deep - 1)
    def _():
        signal(device_id=chip(z + 1, y, x))

    dot = functools.partial(
        lax.dot_general, dimension_numbers=(((1,), (0,)), ((), ())), preferred_element_type=F32
    )
    loads[3].wait()
    loads[4].wait()
    wanted = [
        jnp.transpose(jnp.broadcast_to(pivot_ref[b : b + 1].astype(F32), (LANES, LANES)))
        for b in range(pages)
    ]
    count = lax.broadcasted_iota(jnp.int32, (LANES, LANES), 0).astype(F32) + 1.0
    at = []
    for g in range(groups):
        ids = jnp.broadcast_to(ids_ref[g : g + 1].astype(F32), (LANES, LANES))
        found = [jnp.where(wanted[b] == ids, count + float(LANES * b), 0.0) for b in range(pages)]
        at.append(jnp.sum(functools.reduce(jnp.add, found), axis=0, keepdims=True))
    owned = [jnp.where(v > 0, 1.0, 0.0) for v in at]
    below = lax.broadcasted_iota(jnp.int32, (LANES, LANES), 0)
    right = lax.broadcasted_iota(jnp.int32, (LANES, LANES), 1)
    ahead = jnp.where(below < right, 1.0, 0.0).astype(BF16)
    rank = dot(jnp.concatenate(owned + [jnp.zeros((-groups % 8, LANES), F32)], axis=0).astype(BF16), ahead)
    passed = jnp.zeros((1, 1), F32)
    heres = []
    for g in range(groups):
        here = rank[g : g + 1] + passed
        passed = passed + jnp.sum(owned[g], axis=1, keepdims=True)
        heres.append(jnp.where((owned[g] > 0) & (here < cap), here, -1.0 - slots * cells))
    here = jnp.concatenate(heres, axis=1)
    number = jnp.concatenate(at, axis=1)
    rows = here.shape[1]
    slot = lax.broadcasted_iota(jnp.int32, (slots, rows), 0).astype(F32)
    pick = jnp.where(slot == here, 1.0, 0.0).astype(BF16)
    place = lax.broadcasted_iota(jnp.int32, (slots * cells, rows), 0)
    first = (lax.rem(me, cells) * slots).astype(F32)
    seat = jnp.where(place.astype(F32) == here + first, 1.0, 0.0).astype(BF16)
    high_part = jnp.floor(number * (1.0 / 16.0))
    pair = jnp.concatenate([high_part, number - 16.0 * high_part, jnp.zeros((6, rows), F32)], axis=0)
    lines = lax.dot_general(pair.astype(BF16), seat, ROWS_T, preferred_element_type=F32)
    line = lines[0:1] * 16.0 + lines[1:2]
    line = jnp.concatenate([line, jnp.broadcast_to(passed, (1, part - slots * cells))], axis=1)

    def take(v):
        hi, lo = split(v)
        return dot(pick, hi) + dot(pick, lo)

    loads[0].wait()
    mine[:, :half] = take(old[...])
    mine[slots - 1 : slots, :part] = line
    loads[1].wait()
    mine[:, half:] = take(eri[:, pl.ds(pl.multiple_of(core * (piv // 2), LANES), piv // 2)])

    ends = (z + deep - 1) // deep + (2 * deep - 2 - z) // deep
    pl.semaphore_wait(barrier, len(beside) + 1 + ends)

    last = width - LANES
    colour = [slice(0, part), slice(part, last), slice(last, width)]

    def block(k, zz, b, c):
        return every.at[core, zz, b, c, :, colour[k]]

    def remote(src, dst, send_sem, recv_sem, device):
        return pltpu.make_async_remote_copy(
            src_ref=src, dst_ref=dst, send_sem=send_sem, recv_sem=recv_sem,
            device_id=device, device_id_type=MESH,
        )

    def await_block(ref, sem):
        remote(ref, ref, sem, sem, partner).wait_recv()

    aside = lambda o, along: (lax.rem(y + o * (1 - along), high), lax.rem(x + o * along, wide))
    near = [[aside(o, 1 - core) for o in range(1, wide)], [aside(o, core) for o in range(1, wide)]]
    near.append(near[0])
    far = [near[1], near[0], near[1]]

    def upward(k, zz, src):
        return remote(src, block(k, zz, y, x), z_send.at[k, 0, zz], recv.at[k, zz, y, x], chip(z + 1, y, x))

    def downward(k, zz, src):
        return remote(src, block(k, zz, y, x), z_send.at[k, 1, zz], recv.at[k, zz, y, x], chip(z - 1, y, x))

    def cell_on(way, zz, b, c, src=None):
        ref = block(2, zz, b, c)
        return remote(
            ref if src is None else src, ref, cell_send.at[way, zz, b, c], recv.at[2, zz, b, c],
            chip(z - 1 if way else z + 1, y, x),
        )

    def line_sends(k, zz, src):
        out = []
        for i, (b, c) in enumerate(near[k]):
            out.append(remote(src, block(k, zz, y, x), near_send.at[k, zz, i], recv.at[k, zz, y, x], chip(z, b, c)))
        for i, (b, c) in enumerate(far[k]):
            out.append(remote(src, block(k, zz, y, x), far_send.at[k, zz, 0, i], recv.at[k, zz, y, x], chip(z, b, c)))
        return out

    def onward(k, zz, n, b, c):
        ref = block(k, zz, b, c)
        return [
            remote(ref, ref, far_send.at[k, zz, 1 + n, i], recv.at[k, zz, b, c], chip(z, fb, fc))
            for i, (fb, fc) in enumerate(far[k])
        ]

    def across(zz, b, c, src=None):
        ref = every.at[core, zz, b, c]
        return remote(ref if src is None else src, ref, core_send.at[zz, b, c], core_recv.at[zz, b, c], partner)

    own = pltpu.make_async_copy(mine, every.at[core, z, y, x], own_sem)
    old_copy = remote(old, other, old_sems.at[0], old_sems.at[1], partner)

    def start(copies):
        for copy in copies:
            copy.start()

    def line_copies(zz, src_of):
        return [copy for k in range(2) for copy in line_sends(k, zz, src_of(k))]

    mine_of = lambda k: mine.at[:, colour[k]]
    held_of = lambda zz: lambda k: block(k, zz, y, x)

    start(line_sends(2, z, mine_of(2)))

    @pl.when(z > 0)
    def _():
        start([downward(k, z, mine_of(k)) for k in range(2)])

    @pl.when(z < deep - 1)
    def _():
        start([upward(k, z, mine_of(k)) for k in range(2)])

    start(line_copies(z, mine_of))
    own.start()
    start([across(z, y, x, mine), old_copy])

    def lines_at(t):
        if t == 0:
            return [(z, None, None)]
        return [
            (z - t, z >= t, (upward, z < deep - 1, 0)),
            (z + t, z < deep - t, (downward, z > 0, 1)),
        ]

    def guarded(test, body):
        if test is None:
            body()
        else:
            pl.when(test)(body)

    corner = [(b, c) for b in around(y, high) for c in around(x, wide)]
    everywhere = [(b, c) for b in range(high) for c in range(wide)]

    def stage_plane():
        for n, (b, c) in enumerate(near[2]):
            await_block(block(2, z, b, c), recv.at[2, z, b, c])
            start(onward(2, z, n, b, c))

    def stage_cells(t):
        if t == 0:
            for b, c in far[2] + corner:
                await_block(block(2, z, b, c), recv.at[2, z, b, c])

            @pl.when(z > 0)
            def _():
                start([cell_on(1, z, y, x, mine_of(2))] + [cell_on(1, z, b, c) for b, c in near[2] + far[2] + corner])

            @pl.when(z < deep - 1)
            def _():
                start([cell_on(0, z, y, x, mine_of(2))] + [cell_on(0, z, b, c) for b, c in near[2] + far[2] + corner])

            return
        for zz, test, step in lines_at(t):

            def body(zz=zz, step=step):
                _, further, way = step
                for b, c in everywhere:
                    await_block(block(2, zz, b, c), recv.at[2, zz, b, c])
                    pl.when(further)(lambda b=b, c=c: cell_on(way, zz, b, c).start())
                across(zz, y, x).start()

            guarded(test, body)

    def stage_line(t):
        for zz, test, step in lines_at(t):

            def body(zz=zz, step=step):
                go, further, _ = step
                for k in range(2):
                    await_block(block(k, zz, y, x), recv.at[k, zz, y, x])
                    pl.when(further)(lambda k=k: go(k, zz, block(k, zz, y, x)).start())
                    start(line_sends(k, zz, block(k, zz, y, x)))

            guarded(test, body)

    def stage_near(t):
        for zz, test, _ in lines_at(t):

            def body(zz=zz):
                for k in range(2):
                    for n, (b, c) in enumerate(near[k]):
                        await_block(block(k, zz, b, c), recv.at[k, zz, b, c])
                        start(onward(k, zz, n, b, c))
                for k in range(2):
                    for b, c in far[k]:
                        await_block(block(k, zz, b, c), recv.at[k, zz, b, c])
                        across(zz, b, c).start()

            guarded(test, body)

    def stage_far(t):
        for zz, test, _ in lines_at(t):

            def body(zz=zz):
                for b, c in corner:
                    for k in range(2):
                        await_block(block(k, zz, b, c), recv.at[k, zz, b, c])
                    across(zz, b, c).start()

            guarded(test, body)

    if deep == 4:
        order = [z, z + 1 - 2 * lax.rem(z, 2), 2 - z // 2, 3 - 3 * (z // 2)]
    else:
        order = [z] + around(z, deep)
    pivot = lax.broadcasted_iota(jnp.int32, (piv, slots * cells), 0).astype(F32) + 1.0
    most = []

    def put(i):
        zz = order[i]
        for b in range(high):
            for c in range(wide):
                ref = every.at[1 - core, zz, b, c]
                remote(ref, ref, core_recv.at[zz, b, c], core_recv.at[zz, b, c], partner).wait_recv()
        lines = [every[0, zz, b, c, slots - 1 : slots, :part] for b in range(high) for c in range(wide)]
        most.append(functools.reduce(jnp.maximum, [v[:, part - LANES :] for v in lines]))
        line = functools.reduce(jnp.add, [v[:, : slots * cells] for v in lines])
        seats = jnp.where(pivot == line, 1.0, 0.0).astype(BF16)
        for c in range(2):
            hi, lo = split(every[c, zz].reshape(cells * slots, width))
            hi, lo = dot(seats, hi), dot(seats, lo)
            cut = slice(c * (piv // 2), (c + 1) * (piv // 2))
            if i == 0:
                hi_ref[c] = hi[:, :half].astype(BF16)
                lo_ref[c] = lo[:, :half].astype(BF16)
                gram_ref[:, cut] = hi[:, half:] + lo[:, half:]
            else:
                hi_ref[c] += hi[:, :half].astype(BF16)
                lo_ref[c] += lo[:, :half].astype(BF16)
                gram_ref[:, cut] += hi[:, half:] + lo[:, half:]

    stage_plane()
    old_hi_ref[core], old_lo_ref[core] = split(old[...])
    for t in range(deep + 3):
        if 1 <= t < deep:
            stage_line(t)
        if 0 <= t - 1 < deep:
            stage_cells(t - 1)
            stage_near(t - 1)
        if t == 1:
            old_copy.wait_recv()
            old_hi_ref[1 - core], old_lo_ref[1 - core] = split(other[...])
            own.wait()
        if t == deep + 1:
            for i in range(deep - 2):
                put(i)
        if 0 <= t - 2 < deep:
            stage_far(t - 2)
    for i in range(max(deep - 2, 0), deep):
        put(i)

    most_ref[...] = jnp.broadcast_to(functools.reduce(jnp.maximum, most), most_ref.shape)
    loads[2].wait()
    old_copy.wait_send()

    def cells_sent(way, zz):
        for b, c in everywhere:
            cell_on(way, zz, b, c).wait_send()

    @pl.when(z > 0)
    def _():
        for k in range(2):
            downward(k, z, mine_of(k)).wait_send()
        cells_sent(1, z)

    @pl.when(z < deep - 1)
    def _():
        for k in range(2):
            upward(k, z, mine_of(k)).wait_send()
        cells_sent(0, z)

    for t in range(deep):
        for zz, test, step in lines_at(t):

            def body(zz=zz, step=step, t=t):
                if t:
                    go, further, way = step

                    @pl.when(further)
                    def _():
                        for k in range(2):
                            go(k, zz, block(k, zz, y, x)).wait_send()
                        cells_sent(way, zz)

                for k in range(2 if t else 3):
                    src = block(k, zz, y, x) if t else mine_of(k)
                    for copy in line_sends(k, zz, src):
                        copy.wait_send()
                    for n, (b, c) in enumerate(near[k]):
                        for copy in onward(k, zz, n, b, c):
                            copy.wait_send()
                for b, c in everywhere:
                    across(zz, b, c).wait_send()

            guarded(test, body)


def gather(grid, pivots, ids, old, eri, diagonal, slots):
    deep, high, wide = grid
    piv = eri.shape[1]
    width = old.shape[1] + piv // 2
    peers = max(high, wide)
    sem = pltpu.SemaphoreType.DMA
    wide_bf16 = jax.ShapeDtypeStruct((2, piv, old.shape[1]), BF16)
    any_space = pl.BlockSpec(memory_space=pl.ANY)
    return pl.pallas_call(
        functools.partial(gather_kernel, grid),
        out_shape=(
            jax.ShapeDtypeStruct((piv, piv), F32),
            wide_bf16,
            wide_bf16,
            jax.ShapeDtypeStruct((2, *old.shape), BF16),
            jax.ShapeDtypeStruct((2, *old.shape), BF16),
            jax.ShapeDtypeStruct(eri.shape, F32),
            jax.ShapeDtypeStruct((SUB, LANES), F32),
            jax.ShapeDtypeStruct((1, eri.shape[0]), F32),
        ),
        in_specs=[any_space] * 5,
        out_specs=[VMEM] * 8,
        scratch_shapes=[
            pltpu.VMEM(pivots.shape, jnp.int32),
            pltpu.VMEM(ids.shape, jnp.int32),
            pltpu.VMEM(old.shape, F32),
            pltpu.VMEM(old.shape, F32),
            pltpu.VMEM((slots, width), F32),
            pltpu.VMEM((2, deep, high, wide, slots, width), F32),
            sem((5,)),
            sem,
            sem((2, 2, deep)),
            sem((2, deep, high, wide)),
            sem((3, deep, max(peers - 1, 1))),
            sem((3, deep, peers, max(peers - 1, 1))),
            sem((deep, high, wide)),
            sem((3, deep, high, wide)),
            sem((deep, high, wide)),
            sem((2,)),
        ],
        compiler_params=pltpu.CompilerParams(
            collective_id=1, has_side_effects=True, vmem_limit_bytes=40 * 1024 * 1024
        ),
        name="gather",
    )(pivots, ids, old, eri, diagonal[None, :])


def finish_kernel(
    steps, cap, gram_ref, hi_ref, lo_ref, old_hi_ref, old_lo_ref, eri_ref, most_ref, diag_ref,
    panel_hbm, new_hbm, over_ref, gram, work, panel, new_ref, sems,
):
    piv = gram.shape[0]
    width = piv // steps
    f = functools.partial(lax.dot_general, preferred_element_type=F32)
    over_ref[0] = jnp.where(jnp.max(most_ref[...]) > cap, 1, 0)
    rows = [(hi_ref[c], lo_ref[c]) for c in range(2)]
    old = [(old_hi_ref[c], old_lo_ref[c]) for c in range(2)]
    for s in range(steps):
        here, upto = slice(s * width, (s + 1) * width), slice(0, (s + 1) * width)
        both = [dot_t((v[0][here], v[1][here]), (v[0][upto], v[1][upto])) for v in rows]
        gram[here, upto] = gram_ref[here, upto] - (both[0] + both[1])
    ones = jnp.ones((SUB, width), BF16)
    new = diag_ref[...]
    stores = []
    for s in range(steps):
        at = slice(s * width, (s + 1) * width)
        inv = split(inverse_factor(gram[at, at]))
        later = [slice(t * width, (t + 1) * width) for t in range(s + 1, steps)]
        below = [split(dot_t(split(gram[t, at]), inv)) for t in later]
        for i, t in enumerate(later):
            for u in range(i + 1):
                gram[t, later[u]] -= dot_t(below[i], below[u])
        if s == 0:
            work[...] = eri_ref[...] - (dot_t(old[0], rows[0]) + dot_t(old[1], rows[1]))
        own = dot_t(split(work[:, at]), inv)
        panel[:, at] = own
        stores.append(pltpu.make_async_copy(panel.at[:, at], panel_hbm.at[:, at], sems.at[s]))
        stores[-1].start()
        hi, lo = split(own * own)
        new = new - (f(ones, hi, ROWS_T) + f(ones, lo, ROWS_T))[:1]
        own = split(own)
        for i, t in enumerate(later):
            work[:, t] -= dot_t(own, below[i])
    new_ref[...] = new
    stores.append(pltpu.make_async_copy(new_ref, new_hbm, sems.at[steps]))
    stores[-1].start()
    for store in stores:
        store.wait()


def finish(steps, cap, gathered):
    rows, piv = gathered[5].shape
    any_space = pl.BlockSpec(memory_space=pl.ANY)
    panels, new, over = pl.pallas_call(
        functools.partial(finish_kernel, steps, cap),
        out_shape=(
            jax.ShapeDtypeStruct((rows, piv), F32),
            jax.ShapeDtypeStruct((1, rows), F32),
            jax.ShapeDtypeStruct((1,), jnp.int32),
        ),
        in_specs=[VMEM] * 8,
        out_specs=[any_space, any_space, SMEM],
        scratch_shapes=[
            pltpu.VMEM((piv, piv), F32),
            pltpu.VMEM((rows, piv), F32),
            pltpu.VMEM((rows, piv), F32),
            pltpu.VMEM((1, rows), F32),
            pltpu.SemaphoreType.DMA((steps + 1,)),
        ],
        compiler_params=pltpu.CompilerParams(vmem_limit_bytes=24 * 1024 * 1024),
        name="finish",
    )(*gathered)
    return over[0], panels, new[0]


def place_kernel(line_ref, every_ref, out_ref):
    pivot = lax.broadcasted_iota(jnp.int32, (out_ref.shape[2], line_ref.shape[1]), 0).astype(F32) + 1.0
    seats = jnp.where(pivot == line_ref[...], 1.0, 0.0).astype(BF16)
    dot = functools.partial(
        lax.dot_general, dimension_numbers=(((1,), (0,)), ((), ())), preferred_element_type=F32
    )

    def put(i, carry):
        hi, lo = split(every_ref[i // 2, i % 2])
        out_ref[i // 2, i % 2] = dot(seats, hi) + dot(seats, lo)
        return carry

    lax.fori_loop(0, 4, put, 0)


def place(line, every, piv):
    return pl.pallas_call(
        place_kernel,
        out_shape=jax.ShapeDtypeStruct((2, 2, piv, every.shape[-1]), F32),
        in_specs=[VMEM] * 2,
        out_specs=VMEM,
        compiler_params=pltpu.CompilerParams(vmem_limit_bytes=40 * 1024 * 1024),
        name="place",
    )(line, every)


def rolled_inverse(a):
    n = a.shape[0]
    row = lax.broadcasted_iota(jnp.int32, (n, n), 0)
    lane = lax.broadcasted_iota(jnp.int32, (n, n), 1)

    def pivot(j, held):
        a, w = held
        of_row = lambda v: jnp.sum(jnp.where(row == j, v, 0.0), axis=0, keepdims=True)
        column = jnp.sum(jnp.where(lane == j, a, 0.0), axis=1, keepdims=True)
        root = lax.rsqrt(jnp.sum(jnp.where((row == j) & (lane == j), a, 0.0), keepdims=True))
        m = jnp.where(row > j, column, 0.0) * (root * root)
        return a - m * of_row(a), jnp.where(row == j, w * root, w - m * of_row(w))

    return lax.fori_loop(0, n, pivot, (a, jnp.where(row == lane, 1.0, 0.0)))[1]


def rolled_kernel(
    steps, parts_ref, own_ref, other_ref, eri_ref, diag_ref, panel_ref, new_ref,
    hi, lo, work, solved,
):
    rows, piv = eri_ref.shape
    width = piv // steps
    half = own_ref.shape[1]
    core = lax.axis_index("col")
    for c in range(2):
        both = jnp.concatenate([parts_ref[c, 0], parts_ref[c, 1]], axis=1)
        hi[c], lo[c] = split(both[:, :half])
        work[:piv, c * (piv // 2) : (c + 1) * (piv // 2)] = both[:, half:]
    at_block = lambda b: pl.ds(pl.multiple_of(b * LANES, LANES), LANES)

    def gram(b, carry):
        at = at_block(b)
        work[at, :] -= dot_t((hi[0, at], lo[0, at]), (hi[0], lo[0])) + dot_t((hi[1, at], lo[1, at]), (hi[1], lo[1]))
        return carry

    def reduce(b, carry):
        at = at_block(b)
        work[pl.ds(pl.multiple_of(piv + b * LANES, LANES), LANES), :] = eri_ref[at, :] - (
            dot_t(split(own_ref[at, :]), (hi[core], lo[core]))
            + dot_t(split(other_ref[at, :]), (hi[1 - core], lo[1 - core]))
        )
        return carry

    lax.fori_loop(0, piv // LANES, gram, 0)
    lax.fori_loop(0, rows // LANES, reduce, 0)
    new_ref[...] = diag_ref[...]
    ones = jnp.ones((SUB, width), BF16)
    f = functools.partial(lax.dot_general, dimension_numbers=ROWS_T, preferred_element_type=F32)

    def step(s, carry):
        at = pl.ds(pl.multiple_of(s * width, width), width)
        inv = split(rolled_inverse(work[at, at]))

        def solve(b, carry):
            solved[at_block(b), :] = dot_t(split(work[at_block(b), at]), inv)
            return carry

        lax.fori_loop(0, (piv + rows) // LANES, solve, 0)
        own = solved[piv:, :]
        panel_ref[:, at] = own
        high, low = split(own * own)
        new_ref[...] -= (f(ones, high) + f(ones, low))[:1]
        above = split(solved[:piv, :])

        def update(b, carry):
            work[at_block(b), :] -= dot_t(split(solved[at_block(b), :]), above)
            return carry

        lax.fori_loop(0, (piv + rows) // LANES, update, 0)
        return carry

    lax.fori_loop(0, steps, step, 0)


def rolled(steps, parts, own, other, eri, diagonal):
    rows, piv = eri.shape
    panels, new = pl.pallas_call(
        functools.partial(rolled_kernel, steps),
        out_shape=(
            jax.ShapeDtypeStruct((rows, piv), F32),
            jax.ShapeDtypeStruct((1, rows), F32),
        ),
        in_specs=[VMEM] * 5,
        out_specs=[VMEM] * 2,
        scratch_shapes=[
            pltpu.VMEM((2, piv, own.shape[1]), BF16),
            pltpu.VMEM((2, piv, own.shape[1]), BF16),
            pltpu.VMEM((piv + rows, piv), F32),
            pltpu.VMEM((piv + rows, piv // steps), F32),
        ],
        compiler_params=pltpu.CompilerParams(vmem_limit_bytes=40 * 1024 * 1024),
        name="rolled",
    )(parts, own, other, eri, diagonal[None, :])
    return panels, new[0]


def torus(chips):
    side = 1
    while 2 * (side + 1) ** 3 <= chips:
        side += 1
    return (2 * side, side, side) if 2 * side**3 == chips else (chips, 1, 1)


def slots_for(pivots, chips):
    mean = -(-pivots // chips)
    return min(LANES - 8, -(-(mean + max(12, mean // 2)) // 16) * 16)


def on_device(grid, eri_cols, old_factor, residual_diag, pivots, row_ids):
    steps, width = pivots.shape
    piv = steps * width
    chips = grid[0] * grid[1] * grid[2]
    slots = slots_for(piv, chips)
    cap = slots - 1
    ids = row_ids.reshape(-1, LANES)
    paged = pivots.reshape(-1, LANES)

    gathered = gather(grid, paged, ids, old_factor, eri_cols, residual_diag, slots)
    most = gathered[6]
    result = finish(steps, cap, gathered)
    def again(state):
        windows = (most[0, 0].astype(jnp.int32) + cap - 1) // cap

        def add(w, held):
            mine = pack(jnp.full((1,), w, jnp.int32), paged, ids, old_factor, eri_cols, slots)
            every, other = spread(grid, mine, old_factor)
            every = every.reshape(2, 2, chips, slots, -1)
            line = every[0, 0, :, slots - 1, :slots].at[:, cap].set(0.0).reshape(1, -1)
            every = every.reshape(2, 2, chips * slots, -1)
            return held[0] + place(line, every, piv), other

        empty = jnp.zeros((2, 2, piv, (old_factor.shape[1] + piv // 2) // 2), F32)
        parts, other = lax.fori_loop(0, windows, add, (empty, jnp.zeros_like(old_factor)))
        return jnp.int32(0), *rolled(steps, parts, old_factor, other, eri_cols, residual_diag)

    return lax.while_loop(lambda s: s[0] > 0, again, result)[1:]


def solution(mesh):
    grid = torus(mesh.shape["row"])
    placed = (P("row", None), P("row", "col"), P("row"), P(), P("row"))
    return jax.shard_map(
        functools.partial(on_device, grid),
        mesh=mesh, in_specs=placed, out_specs=(P("row", None), P("row")), check_vma=False,
    )
```

```python
import functools
import jax
import jax.numpy as jnp
from jax import lax
from jax.experimental import pallas as pl
from jax.experimental.pallas import tpu as pltpu
from jax.sharding import PartitionSpec as P

ROWS_T = (((1,), (1,)), ((), ()))
COLS_T = (((0,), (0,)), ((), ()))
SUB = 8
LANES = 128
MESH = pl.DeviceIdType.MESH
VMEM = pl.BlockSpec(memory_space=pltpu.VMEM)
SMEM = pl.BlockSpec(memory_space=pltpu.SMEM)
F32 = jnp.float32
BF16 = jnp.bfloat16


def split(x):
    hi = x.astype(BF16)
    return hi, (x - hi.astype(F32)).astype(BF16)


def dot_t(a, b):
    f = functools.partial(
        lax.dot_general, dimension_numbers=ROWS_T, preferred_element_type=F32
    )
    return f(a[0], b[0]) + (f(a[0], b[1]) + f(a[1], b[0]))


def inverse_factor(a):
    n = a.shape[0]
    groups = n // SUB
    row = lax.broadcasted_iota(jnp.int32, (SUB, n), 0)
    lane = lax.broadcasted_iota(jnp.int32, (SUB, n), 1)
    M = [a[SUB * i : SUB * i + SUB, :] for i in range(groups)]
    over = lambda v, k: jnp.broadcast_to(v[k : k + 1, :], (SUB, n))
    columns = lambda v, j: [jnp.broadcast_to(v[:, j + k : j + k + 1], (SUB, n)) for k in range(SUB)]
    out = []
    V = [jnp.where(row >= 0, v, 0.0) for v in columns(M[0], 0)]
    for g in range(groups):
        j = SUB * g
        ahead = g + 1 < groups
        if ahead:
            U = [jnp.where(row >= 0, v, 0.0) for v in columns(M[g + 1], j)]
            N = columns(M[g + 1], j + SUB)
        second = g + 2 < groups
        if second:
            U2 = [jnp.where(row >= 0, v, 0.0) for v in columns(M[g + 2], j)]
        here = (lane >= j) & (lane < j + SUB)
        M[g] = jnp.where(here, jnp.where(lane == row + j, 1.0, 0.0), M[g])
        for i in range(g + 1, min(g + 3, groups)):
            M[i] = jnp.where(here, 0.0, M[i])
        roots = jnp.zeros((SUB, n), F32)
        invs = jnp.zeros((SUB, n), F32)
        for k in range(SUB):
            root = lax.rsqrt(over(V[k], k))
            inv = root * root
            roots = jnp.where(row == k, root, roots)
            invs = jnp.where(row == k, inv, invs)
            down = jnp.where(row > k, V[k], 0.0)
            top = [None] * SUB
            for l in range(k + 1, SUB):
                top[l] = over(V[k], l)
                V[l] = V[l] - (down * top[l]) * inv
            r = over(M[g], k)
            M[g] = M[g] - (down * inv) * r
            if ahead:
                u = U[k] * inv
                for l in range(k + 1, SUB):
                    U[l] = U[l] - u * top[l]
                M[g + 1] = M[g + 1] - u * r
                for l in range(SUB):
                    N[l] = N[l] - u * over(U[k], l)
            if second:
                u = U2[k] * inv
                for l in range(k + 1, SUB):
                    U2[l] = U2[l] - u * top[l]
                M[g + 2] = M[g + 2] - u * r
        out.append(jnp.where(lane < j + SUB, M[g] * roots, 0.0))
        if not ahead:
            break
        if g + 3 < groups:
            S = M[g] * invs
            for i in reversed(range(1, SUB)):
                S = S - (jnp.where(row < i, V[i], 0.0) * invs) * over(S, i)
            S = [over(S, k) for k in range(SUB)]
            for i in range(g + 3, groups):
                C = columns(M[i], j)
                M[i] = jnp.where(here, 0.0, M[i])
                for k in range(SUB):
                    M[i] = M[i] - C[k] * S[k]
        V = N
    return jnp.concatenate(out, axis=0)


def pack_kernel(cap, window_ref, pivot_ref, ids_ref, old_ref, eri_ref, out_ref):
    steps, width = pivot_ref.shape
    slots = out_ref.shape[1]
    part = out_ref.shape[2]
    groups = ids_ref.shape[0]
    half = eri_ref.shape[1] // 2
    ids = ids_ref[...]

    def find(j, at):
        return jnp.where(ids == pivot_ref[j // width, j % width], j + 1, at)

    at = lax.fori_loop(0, steps * width, find, jnp.zeros_like(ids), unroll=16)
    owned = jnp.where(at > 0, 1.0, 0.0)
    below = lax.broadcasted_iota(jnp.int32, (LANES, LANES), 0)
    right = lax.broadcasted_iota(jnp.int32, (LANES, LANES), 1)
    ahead = jnp.where(below < right, 1.0, 0.0).astype(BF16)
    rank = lax.dot_general(
        owned.astype(BF16), ahead, (((1,), (0,)), ((), ())), preferred_element_type=F32
    )
    first = window_ref[0] * cap
    slot = lax.broadcasted_iota(jnp.int32, (slots, LANES), 0)
    passed = jnp.zeros((1, 1), F32)
    picks, numbers = [], []
    for g in range(groups):
        here = (rank[g : g + 1] + passed).astype(jnp.int32) - first
        passed = passed + jnp.sum(owned[g : g + 1], axis=1, keepdims=True)
        here = jnp.where((owned[g : g + 1] > 0) & (here >= 0) & (here < cap), here, -1)
        picks.append(jnp.where(slot == here, 1.0, 0.0))
        numbers.append(at[g : g + 1])
    pick = jnp.concatenate(picks, axis=1).astype(BF16)
    number = jnp.concatenate(numbers, axis=1)
    pair = jnp.concatenate([number // 16, number % 16] + [jnp.zeros_like(number)] * 6, axis=0)
    pair = pair.astype(F32).astype(BF16)
    lines = lax.dot_general(pair, pick, ROWS_T, preferred_element_type=F32)
    line = lines[0:1] * 16.0 + lines[1:2]
    line = jnp.concatenate([line, jnp.zeros((1, LANES - slots), F32)], axis=1)

    def take(x):
        f = functools.partial(
            lax.dot_general,
            dimension_numbers=(((1,), (0,)), ((), ())),
            preferred_element_type=F32,
        )
        hi, lo = split(x)
        return f(pick, hi) + f(pick, lo)

    core = lax.axis_index("col")
    out_ref[0] = take(old_ref[:, :part])
    out_ref[0, slots - 1 : slots, :LANES] = line
    rest = old_ref.shape[1] - part
    out_ref[1, :, :rest] = take(old_ref[:, part:])
    out_ref[1, :, rest:] = take(eri_ref[:, pl.ds(pl.multiple_of(core * half, LANES), half)])


def pack(window, pivots, ids, old, eri, slots):
    width = (old.shape[1] + eri.shape[1] // 2) // 2
    return pl.pallas_call(
        functools.partial(pack_kernel, slots - 1),
        out_shape=jax.ShapeDtypeStruct((2, slots, width), F32),
        in_specs=[SMEM, SMEM, VMEM, VMEM, VMEM],
        out_specs=VMEM,
        name="pack",
    )(window, pivots, ids, old, eri)


def spread_kernel(grid, mine_ref, old_ref, all_ref, other_ref, *sems):
    deep, high, wide = grid
    fine = deep * high * wide <= 16
    own_sem, first_send, near_send, far_send, core_send = sems[:5]
    first_recv, recv, core_recv, old_sems = sems[5:]
    me = lax.axis_index("row")
    core = lax.axis_index("col")
    z, y, x = me // (high * wide), me // wide % high, me % wide
    chip = lambda z, y, x: (z * high + y) * wide + x
    steps = lambda at, size: [lax.rem(at + o, size) for o in range(1, size)]
    partner = (me, 1 - core)

    barrier = pltpu.get_barrier_semaphore()
    greet = [(chip(o, y, x), core) for o in steps(z, deep)]
    greet += [(chip(z, o, x), core) for o in steps(y, high)]
    greet += [(chip(z, y, o), core) for o in steps(x, wide)]
    greet.append(partner)
    for device in greet:
        pl.semaphore_signal(barrier, inc=1, device_id=device, device_id_type=MESH)
    pl.semaphore_wait(barrier, len(greet))

    flying = []

    def send(src, dst, send_sem, recv_sem, device):
        copy = pltpu.make_async_remote_copy(
            src_ref=src, dst_ref=dst, send_sem=send_sem, recv_sem=recv_sem,
            device_id=device, device_id_type=MESH,
        )
        copy.start()
        flying.append(copy)

    def await_block(ref, sem):
        pltpu.make_async_remote_copy(
            src_ref=ref, dst_ref=ref, send_sem=sem, recv_sem=sem,
            device_id=partner, device_id_type=MESH,
        ).wait_recv()

    def block(colour, zs, y, x):
        return all_ref.at[core, colour, zs, y, x]

    own = [
        pltpu.make_async_copy(mine_ref.at[k], all_ref.at[core, k, z, y, x], own_sem.at[k])
        for k in range(2)
    ]
    for k in range(2):
        own[k].start()
    for k in range(2):
        for i, o in enumerate(steps(z, deep)):
            send(mine_ref.at[k], block(k, z, y, x), first_send.at[k, i], first_recv.at[k, z], (chip(o, y, x), core))

    chunks = [z] + steps(z, deep) if fine else [None]
    near = lambda k: [(y, o) for o in steps(x, wide)] if k == 0 else [(o, x) for o in steps(y, high)]
    far = lambda k: [(o, x) for o in steps(y, high)] if k == 0 else [(y, o) for o in steps(x, wide)]

    def to_core(k, q, i, zs, y, x):
        ref = block(k, zs, y, x)
        send(ref, ref, core_send.at[k, q, i], core_recv.at[k, chunk_at(zs), y, x], partner)

    def chunk_at(zs):
        return zs if fine else 0

    def rows(zs):
        return zs if fine else slice(None)

    for q, at in enumerate(chunks):
        zs = rows(at)
        mine = fine and q == 0
        for k in range(2):
            if q == 0:
                if not fine:
                    for o in steps(z, deep):
                        await_block(block(k, o, y, x), first_recv.at[k, o])
                    own[k].wait()
            else:
                await_block(block(k, zs, y, x), first_recv.at[k, zs])
            src = mine_ref.at[k] if mine else block(k, zs, y, x)
            sem = recv.at[k, chunk_at(zs), y, x]
            for i, (b, c) in enumerate(near(k)):
                send(src, block(k, zs, y, x), near_send.at[k, q, i], sem, (chip(z, b, c), core))
            for i, (b, c) in enumerate(far(k)):
                send(src, block(k, zs, y, x), far_send.at[k, q, 0, i], sem, (chip(z, b, c), core))
            send(src, block(k, zs, y, x), core_send.at[k, q, 0], core_recv.at[k, chunk_at(zs), y, x], partner)
    old_copy = pltpu.make_async_remote_copy(
        src_ref=old_ref, dst_ref=other_ref, send_sem=old_sems.at[0], recv_sem=old_sems.at[1],
        device_id=partner, device_id_type=MESH,
    )
    old_copy.start()
    flying.append(old_copy)
    for q, at in enumerate(chunks):
        zs = rows(at)
        for k in range(2):
            for n, (b, c) in enumerate(near(k)):
                ref = block(k, zs, b, c)
                await_block(ref, recv.at[k, chunk_at(zs), b, c])
                for i, (fb, fc) in enumerate(far(k)):
                    send(ref, ref, far_send.at[k, q, 1 + n, i], recv.at[k, chunk_at(zs), b, c], (chip(z, fb, fc), core))
                to_core(k, q, 1 + n, zs, b, c)
    for q, at in enumerate(chunks):
        zs = rows(at)
        for k in range(2):
            index = 1 + len(near(k))
            for fb, fc in far(k):
                for b, c in [(y, x)] + near(k):
                    there = (fb, c) if k == 0 else (b, fc)
                    ref = block(k, zs, *there)
                    await_block(ref, recv.at[k, chunk_at(zs), *there])
                    to_core(k, q, index, zs, *there)
                    index += 1
    if fine:
        for k in range(2):
            own[k].wait()
    for q, at in enumerate(chunks):
        zs = rows(at)
        for k in range(2):
            for b in range(high):
                for c in range(wide):
                    ref = all_ref.at[1 - core, k, zs, b, c]
                    await_block(ref, core_recv.at[k, chunk_at(zs), b, c])
    old_copy.wait_recv()
    for copy in flying:
        copy.wait_send()


def spread(grid, mine, old):
    deep, high, wide = grid
    _, slots, width = mine.shape
    chunks = deep if deep * high * wide <= 16 else 1
    cells = high * wide
    peers = max(high, wide)
    sem = pltpu.SemaphoreType.DMA
    return pl.pallas_call(
        functools.partial(spread_kernel, grid),
        out_shape=(
            jax.ShapeDtypeStruct((2, 2, deep, high, wide, slots, width), F32),
            jax.ShapeDtypeStruct(old.shape, F32),
        ),
        in_specs=[pl.BlockSpec(memory_space=pl.ANY)] * 2,
        out_specs=(VMEM, pl.BlockSpec(memory_space=pl.ANY)),
        scratch_shapes=[
            sem((2,)),
            sem((2, max(deep - 1, 1))),
            sem((2, chunks, max(peers - 1, 1))),
            sem((2, chunks, peers, max(peers - 1, 1))),
            sem((2, chunks, cells)),
            sem((2, deep)),
            sem((2, chunks, high, wide)),
            sem((2, chunks, high, wide)),
            sem((2,)),
        ],
        compiler_params=pltpu.CompilerParams(
            collective_id=0, has_side_effects=True, vmem_limit_bytes=48 * 1024 * 1024
        ),
        name="spread",
    )(mine, old)


def gather_kernel(
    grid, pivot_hbm, ids_hbm, old_hbm, eri_hbm, diag_hbm,
    gram_ref, hi_ref, lo_ref, old_hi_ref, old_lo_ref, eri, most_ref, diag,
    pivot_ref, ids_ref, old, other, mine, every,
    in_sems, own_sem, z_send, cell_send, near_send, far_send, core_send, recv, core_recv, old_sems,
):
    deep, high, wide = grid
    cells = high * wide
    slots, width = mine.shape
    cap = slots - 1
    part = width // 2
    half = old.shape[1]
    piv = gram_ref.shape[0]
    groups = ids_ref.shape[0]
    pages = pivot_ref.shape[0]
    me = lax.axis_index("row")
    core = lax.axis_index("col")
    z, y, x = me // cells, me // wide % high, me % wide
    partner = (me, 1 - core)
    chip = lambda z, y, x: ((z * high + y) * wide + x, core)
    around = lambda at, size: [lax.rem(at + o, size) for o in range(1, size)]

    loads = [
        pltpu.make_async_copy(old_hbm, old, in_sems.at[0]),
        pltpu.make_async_copy(eri_hbm, eri, in_sems.at[1]),
        pltpu.make_async_copy(diag_hbm, diag, in_sems.at[2]),
        pltpu.make_async_copy(pivot_hbm, pivot_ref, in_sems.at[3]),
        pltpu.make_async_copy(ids_hbm, ids_ref, in_sems.at[4]),
    ]
    for load in loads[3:] + loads[:3]:
        load.start()

    barrier = pltpu.get_barrier_semaphore()
    signal = functools.partial(pl.semaphore_signal, barrier, inc=1, device_id_type=MESH)
    beside = [chip(z, o, x) for o in around(y, high)] + [chip(z, y, o) for o in around(x, wide)]
    for device in beside + [partner]:
        signal(device_id=device)

    @pl.when(z > 0)
    def _():
        signal(device_id=chip(z - 1, y, x))

    @pl.when(z < deep - 1)
    def _():
        signal(device_id=chip(z + 1, y, x))

    dot = functools.partial(
        lax.dot_general, dimension_numbers=(((1,), (0,)), ((), ())), preferred_element_type=F32
    )
    loads[3].wait()
    loads[4].wait()
    wanted = [
        jnp.transpose(jnp.broadcast_to(pivot_ref[b : b + 1].astype(F32), (LANES, LANES)))
        for b in range(pages)
    ]
    count = lax.broadcasted_iota(jnp.int32, (LANES, LANES), 0).astype(F32) + 1.0
    at = []
    for g in range(groups):
        ids = jnp.broadcast_to(ids_ref[g : g + 1].astype(F32), (LANES, LANES))
        found = [jnp.where(wanted[b] == ids, count + float(LANES * b), 0.0) for b in range(pages)]
        at.append(jnp.sum(functools.reduce(jnp.add, found), axis=0, keepdims=True))
    owned = [jnp.where(v > 0, 1.0, 0.0) for v in at]
    below = lax.broadcasted_iota(jnp.int32, (LANES, LANES), 0)
    right = lax.broadcasted_iota(jnp.int32, (LANES, LANES), 1)
    ahead = jnp.where(below < right, 1.0, 0.0).astype(BF16)
    rank = dot(jnp.concatenate(owned + [jnp.zeros((-groups % 8, LANES), F32)], axis=0).astype(BF16), ahead)
    passed = jnp.zeros((1, 1), F32)
    heres = []
    for g in range(groups):
        here = rank[g : g + 1] + passed
        passed = passed + jnp.sum(owned[g], axis=1, keepdims=True)
        heres.append(jnp.where((owned[g] > 0) & (here < cap), here, -1.0 - slots * cells))
    here = jnp.concatenate(heres, axis=1)
    number = jnp.concatenate(at, axis=1)
    rows = here.shape[1]
    slot = lax.broadcasted_iota(jnp.int32, (slots, rows), 0).astype(F32)
    pick = jnp.where(slot == here, 1.0, 0.0).astype(BF16)
    place = lax.broadcasted_iota(jnp.int32, (slots * cells, rows), 0)
    first = (lax.rem(me, cells) * slots).astype(F32)
    seat = jnp.where(place.astype(F32) == here + first, 1.0, 0.0).astype(BF16)
    high_part = jnp.floor(number * (1.0 / 16.0))
    pair = jnp.concatenate([high_part, number - 16.0 * high_part, jnp.zeros((6, rows), F32)], axis=0)
    lines = lax.dot_general(pair.astype(BF16), seat, ROWS_T, preferred_element_type=F32)
    line = lines[0:1] * 16.0 + lines[1:2]
    line = jnp.concatenate([line, jnp.broadcast_to(passed, (1, part - slots * cells))], axis=1)

    def take(v):
        hi, lo = split(v)
        return dot(pick, hi) + dot(pick, lo)

    loads[0].wait()
    mine[:, :half] = take(old[...])
    mine[slots - 1 : slots, :part] = line
    loads[1].wait()
    mine[:, half:] = take(eri[:, pl.ds(pl.multiple_of(core * (piv // 2), LANES), piv // 2)])

    ends = (z + deep - 1) // deep + (2 * deep - 2 - z) // deep
    pl.semaphore_wait(barrier, len(beside) + 1 + ends)

    last = width - LANES
    colour = [slice(0, part), slice(part, last), slice(last, width)]

    def block(k, zz, b, c):
        return every.at[core, zz, b, c, :, colour[k]]

    def remote(src, dst, send_sem, recv_sem, device):
        return pltpu.make_async_remote_copy(
            src_ref=src, dst_ref=dst, send_sem=send_sem, recv_sem=recv_sem,
            device_id=device, device_id_type=MESH,
        )

    def await_block(ref, sem):
        remote(ref, ref, sem, sem, partner).wait_recv()

    aside = lambda o, along: (lax.rem(y + o * (1 - along), high), lax.rem(x + o * along, wide))
    near = [[aside(o, 1 - core) for o in range(1, wide)], [aside(o, core) for o in range(1, wide)]]
    near.append(near[0])
    far = [near[1], near[0], near[1]]

    def upward(k, zz, src):
        return remote(src, block(k, zz, y, x), z_send.at[k, 0, zz], recv.at[k, zz, y, x], chip(z + 1, y, x))

    def downward(k, zz, src):
        return remote(src, block(k, zz, y, x), z_send.at[k, 1, zz], recv.at[k, zz, y, x], chip(z - 1, y, x))

    def cell_on(way, zz, b, c, src=None):
        ref = block(2, zz, b, c)
        return remote(
            ref if src is None else src, ref, cell_send.at[way, zz, b, c], recv.at[2, zz, b, c],
            chip(z - 1 if way else z + 1, y, x),
        )

    def line_sends(k, zz, src):
        out = []
        for i, (b, c) in enumerate(near[k]):
            out.append(remote(src, block(k, zz, y, x), near_send.at[k, zz, i], recv.at[k, zz, y, x], chip(z, b, c)))
        for i, (b, c) in enumerate(far[k]):
            out.append(remote(src, block(k, zz, y, x), far_send.at[k, zz, 0, i], recv.at[k, zz, y, x], chip(z, b, c)))
        return out

    def onward(k, zz, n, b, c):
        ref = block(k, zz, b, c)
        return [
            remote(ref, ref, far_send.at[k, zz, 1 + n, i], recv.at[k, zz, b, c], chip(z, fb, fc))
            for i, (fb, fc) in enumerate(far[k])
        ]

    def across(zz, b, c, src=None):
        ref = every.at[core, zz, b, c]
        return remote(ref if src is None else src, ref, core_send.at[zz, b, c], core_recv.at[zz, b, c], partner)

    own = pltpu.make_async_copy(mine, every.at[core, z, y, x], own_sem)
    old_copy = remote(old, other, old_sems.at[0], old_sems.at[1], partner)

    def start(copies):
        for copy in copies:
            copy.start()

    def line_copies(zz, src_of):
        return [copy for k in range(2) for copy in line_sends(k, zz, src_of(k))]

    mine_of = lambda k: mine.at[:, colour[k]]
    held_of = lambda zz: lambda k: block(k, zz, y, x)

    start(line_sends(2, z, mine_of(2)))

    @pl.when(z > 0)
    def _():
        start([downward(k, z, mine_of(k)) for k in range(2)])

    @pl.when(z < deep - 1)
    def _():
        start([upward(k, z, mine_of(k)) for k in range(2)])

    start(line_copies(z, mine_of))
    own.start()
    start([across(z, y, x, mine), old_copy])

    def lines_at(t):
        if t == 0:
            return [(z, None, None)]
        return [
            (z - t, z >= t, (upward, z < deep - 1, 0)),
            (z + t, z < deep - t, (downward, z > 0, 1)),
        ]

    def guarded(test, body):
        if test is None:
            body()
        else:
            pl.when(test)(body)

    corner = [(b, c) for b in around(y, high) for c in around(x, wide)]
    everywhere = [(b, c) for b in range(high) for c in range(wide)]

    def stage_plane():
        for n, (b, c) in enumerate(near[2]):
            await_block(block(2, z, b, c), recv.at[2, z, b, c])
            start(onward(2, z, n, b, c))

    def stage_cells(t):
        if t == 0:
            for b, c in far[2] + corner:
                await_block(block(2, z, b, c), recv.at[2, z, b, c])

            @pl.when(z > 0)
            def _():
                start([cell_on(1, z, y, x, mine_of(2))] + [cell_on(1, z, b, c) for b, c in near[2] + far[2] + corner])

            @pl.when(z < deep - 1)
            def _():
                start([cell_on(0, z, y, x, mine_of(2))] + [cell_on(0, z, b, c) for b, c in near[2] + far[2] + corner])

            return
        for zz, test, step in lines_at(t):

            def body(zz=zz, step=step):
                _, further, way = step
                for b, c in everywhere:
                    await_block(block(2, zz, b, c), recv.at[2, zz, b, c])
                    pl.when(further)(lambda b=b, c=c: cell_on(way, zz, b, c).start())
                across(zz, y, x).start()

            guarded(test, body)

    def stage_line(t):
        for zz, test, step in lines_at(t):

            def body(zz=zz, step=step):
                go, further, _ = step
                for k in range(2):
                    await_block(block(k, zz, y, x), recv.at[k, zz, y, x])
                    pl.when(further)(lambda k=k: go(k, zz, block(k, zz, y, x)).start())
                    start(line_sends(k, zz, block(k, zz, y, x)))

            guarded(test, body)

    def stage_near(t):
        for zz, test, _ in lines_at(t):

            def body(zz=zz):
                for k in range(2):
                    for n, (b, c) in enumerate(near[k]):
                        await_block(block(k, zz, b, c), recv.at[k, zz, b, c])
                        start(onward(k, zz, n, b, c))

            guarded(test, body)

    def stage_beside(t):
        for zz, test, _ in lines_at(t):

            def body(zz=zz):
                for k in range(2):
                    for b, c in far[k]:
                        await_block(block(k, zz, b, c), recv.at[k, zz, b, c])
                        across(zz, b, c).start()

            guarded(test, body)

    def stage_far(t):
        for zz, test, _ in lines_at(t):

            def body(zz=zz):
                for b, c in corner:
                    for k in range(2):
                        await_block(block(k, zz, b, c), recv.at[k, zz, b, c])
                    across(zz, b, c).start()

            guarded(test, body)

    if deep == 4:
        order = [z, z + 1 - 2 * lax.rem(z, 2), 2 - z // 2, 3 - 3 * (z // 2)]
    else:
        order = [z] + around(z, deep)
    pivot = lax.broadcasted_iota(jnp.int32, (piv, slots * cells), 0).astype(F32) + 1.0
    most = []

    def put(i):
        zz = order[i]
        for b in range(high):
            for c in range(wide):
                ref = every.at[1 - core, zz, b, c]
                remote(ref, ref, core_recv.at[zz, b, c], core_recv.at[zz, b, c], partner).wait_recv()
        lines = [every[0, zz, b, c, slots - 1 : slots, :part] for b in range(high) for c in range(wide)]
        most.append(functools.reduce(jnp.maximum, [v[:, part - LANES :] for v in lines]))
        line = functools.reduce(jnp.add, [v[:, : slots * cells] for v in lines])
        seats = jnp.where(pivot == line, 1.0, 0.0).astype(BF16)
        for c in range(2):
            hi, lo = split(every[c, zz].reshape(cells * slots, width))
            hi, lo = dot(seats, hi), dot(seats, lo)
            cut = slice(c * (piv // 2), (c + 1) * (piv // 2))
            if i == 0:
                hi_ref[c] = hi[:, :half].astype(BF16)
                lo_ref[c] = lo[:, :half].astype(BF16)
                gram_ref[:, cut] = hi[:, half:] + lo[:, half:]
            else:
                hi_ref[c] += hi[:, :half].astype(BF16)
                lo_ref[c] += lo[:, :half].astype(BF16)
                gram_ref[:, cut] += hi[:, half:] + lo[:, half:]

    stage_plane()
    old_hi_ref[core], old_lo_ref[core] = split(old[...])
    for t in range(deep + 3):
        if 1 <= t < deep:
            stage_line(t)
        if 0 <= t - 1 < deep:
            stage_near(t - 1)
            stage_cells(t - 1)
            stage_beside(t - 1)
        if t == 1:
            old_copy.wait_recv()
            old_hi_ref[1 - core], old_lo_ref[1 - core] = split(other[...])
            own.wait()
        if t == deep + 1:
            for i in range(deep - 2):
                put(i)
        if 0 <= t - 2 < deep:
            stage_far(t - 2)
    for i in range(max(deep - 2, 0), deep):
        put(i)

    most_ref[...] = jnp.broadcast_to(functools.reduce(jnp.maximum, most), most_ref.shape)
    loads[2].wait()
    old_copy.wait_send()

    def cells_sent(way, zz):
        for b, c in everywhere:
            cell_on(way, zz, b, c).wait_send()

    @pl.when(z > 0)
    def _():
        for k in range(2):
            downward(k, z, mine_of(k)).wait_send()
        cells_sent(1, z)

    @pl.when(z < deep - 1)
    def _():
        for k in range(2):
            upward(k, z, mine_of(k)).wait_send()
        cells_sent(0, z)

    for t in range(deep):
        for zz, test, step in lines_at(t):

            def body(zz=zz, step=step, t=t):
                if t:
                    go, further, way = step

                    @pl.when(further)
                    def _():
                        for k in range(2):
                            go(k, zz, block(k, zz, y, x)).wait_send()
                        cells_sent(way, zz)

                for k in range(2 if t else 3):
                    src = block(k, zz, y, x) if t else mine_of(k)
                    for copy in line_sends(k, zz, src):
                        copy.wait_send()
                    for n, (b, c) in enumerate(near[k]):
                        for copy in onward(k, zz, n, b, c):
                            copy.wait_send()
                for b, c in everywhere:
                    across(zz, b, c).wait_send()

            guarded(test, body)


def gather(grid, pivots, ids, old, eri, diagonal, slots):
    deep, high, wide = grid
    piv = eri.shape[1]
    width = old.shape[1] + piv // 2
    peers = max(high, wide)
    sem = pltpu.SemaphoreType.DMA
    wide_bf16 = jax.ShapeDtypeStruct((2, piv, old.shape[1]), BF16)
    any_space = pl.BlockSpec(memory_space=pl.ANY)
    return pl.pallas_call(
        functools.partial(gather_kernel, grid),
        out_shape=(
            jax.ShapeDtypeStruct((piv, piv), F32),
            wide_bf16,
            wide_bf16,
            jax.ShapeDtypeStruct((2, *old.shape), BF16),
            jax.ShapeDtypeStruct((2, *old.shape), BF16),
            jax.ShapeDtypeStruct(eri.shape, F32),
            jax.ShapeDtypeStruct((SUB, LANES), F32),
            jax.ShapeDtypeStruct((1, eri.shape[0]), F32),
        ),
        in_specs=[any_space] * 5,
        out_specs=[VMEM] * 8,
        scratch_shapes=[
            pltpu.VMEM(pivots.shape, jnp.int32),
            pltpu.VMEM(ids.shape, jnp.int32),
            pltpu.VMEM(old.shape, F32),
            pltpu.VMEM(old.shape, F32),
            pltpu.VMEM((slots, width), F32),
            pltpu.VMEM((2, deep, high, wide, slots, width), F32),
            sem((5,)),
            sem,
            sem((2, 2, deep)),
            sem((2, deep, high, wide)),
            sem((3, deep, max(peers - 1, 1))),
            sem((3, deep, peers, max(peers - 1, 1))),
            sem((deep, high, wide)),
            sem((3, deep, high, wide)),
            sem((deep, high, wide)),
            sem((2,)),
        ],
        compiler_params=pltpu.CompilerParams(
            collective_id=1, has_side_effects=True, vmem_limit_bytes=40 * 1024 * 1024
        ),
        name="gather",
    )(pivots, ids, old, eri, diagonal[None, :])


def finish_kernel(
    steps, cap, gram_ref, hi_ref, lo_ref, old_hi_ref, old_lo_ref, eri_ref, most_ref, diag_ref,
    panel_hbm, new_hbm, over_ref, gram, work, panel, new_ref, sems,
):
    piv = gram.shape[0]
    width = piv // steps
    f = functools.partial(lax.dot_general, preferred_element_type=F32)
    over_ref[0] = jnp.where(jnp.max(most_ref[...]) > cap, 1, 0)
    rows = [(hi_ref[c], lo_ref[c]) for c in range(2)]
    old = [(old_hi_ref[c], old_lo_ref[c]) for c in range(2)]
    for s in range(steps):
        here, upto = slice(s * width, (s + 1) * width), slice(0, (s + 1) * width)
        both = [dot_t((v[0][here], v[1][here]), (v[0][upto], v[1][upto])) for v in rows]
        gram[here, upto] = gram_ref[here, upto] - (both[0] + both[1])
    ones = jnp.ones((SUB, width), BF16)
    new = diag_ref[...]
    stores = []
    for s in range(steps):
        at = slice(s * width, (s + 1) * width)
        inv = split(inverse_factor(gram[at, at]))
        later = [slice(t * width, (t + 1) * width) for t in range(s + 1, steps)]
        below = [split(dot_t(split(gram[t, at]), inv)) for t in later]
        for i, t in enumerate(later):
            for u in range(i + 1):
                gram[t, later[u]] -= dot_t(below[i], below[u])
        if s == 0:
            work[...] = eri_ref[...] - (dot_t(old[0], rows[0]) + dot_t(old[1], rows[1]))
        own = dot_t(split(work[:, at]), inv)
        panel[:, at] = own
        stores.append(pltpu.make_async_copy(panel.at[:, at], panel_hbm.at[:, at], sems.at[s]))
        stores[-1].start()
        hi, lo = split(own * own)
        new = new - (f(ones, hi, ROWS_T) + f(ones, lo, ROWS_T))[:1]
        own = split(own)
        for i, t in enumerate(later):
            work[:, t] -= dot_t(own, below[i])
    new_ref[...] = new
    stores.append(pltpu.make_async_copy(new_ref, new_hbm, sems.at[steps]))
    stores[-1].start()
    for store in stores:
        store.wait()


def finish(steps, cap, gathered):
    rows, piv = gathered[5].shape
    any_space = pl.BlockSpec(memory_space=pl.ANY)
    panels, new, over = pl.pallas_call(
        functools.partial(finish_kernel, steps, cap),
        out_shape=(
            jax.ShapeDtypeStruct((rows, piv), F32),
            jax.ShapeDtypeStruct((1, rows), F32),
            jax.ShapeDtypeStruct((1,), jnp.int32),
        ),
        in_specs=[VMEM] * 8,
        out_specs=[any_space, any_space, SMEM],
        scratch_shapes=[
            pltpu.VMEM((piv, piv), F32),
            pltpu.VMEM((rows, piv), F32),
            pltpu.VMEM((rows, piv), F32),
            pltpu.VMEM((1, rows), F32),
            pltpu.SemaphoreType.DMA((steps + 1,)),
        ],
        compiler_params=pltpu.CompilerParams(vmem_limit_bytes=24 * 1024 * 1024),
        name="finish",
    )(*gathered)
    return over[0], panels, new[0]


def place_kernel(line_ref, every_ref, out_ref):
    pivot = lax.broadcasted_iota(jnp.int32, (out_ref.shape[2], line_ref.shape[1]), 0).astype(F32) + 1.0
    seats = jnp.where(pivot == line_ref[...], 1.0, 0.0).astype(BF16)
    dot = functools.partial(
        lax.dot_general, dimension_numbers=(((1,), (0,)), ((), ())), preferred_element_type=F32
    )

    def put(i, carry):
        hi, lo = split(every_ref[i // 2, i % 2])
        out_ref[i // 2, i % 2] = dot(seats, hi) + dot(seats, lo)
        return carry

    lax.fori_loop(0, 4, put, 0)


def place(line, every, piv):
    return pl.pallas_call(
        place_kernel,
        out_shape=jax.ShapeDtypeStruct((2, 2, piv, every.shape[-1]), F32),
        in_specs=[VMEM] * 2,
        out_specs=VMEM,
        compiler_params=pltpu.CompilerParams(vmem_limit_bytes=40 * 1024 * 1024),
        name="place",
    )(line, every)


def rolled_inverse(a):
    n = a.shape[0]
    row = lax.broadcasted_iota(jnp.int32, (n, n), 0)
    lane = lax.broadcasted_iota(jnp.int32, (n, n), 1)

    def pivot(j, held):
        a, w = held
        of_row = lambda v: jnp.sum(jnp.where(row == j, v, 0.0), axis=0, keepdims=True)
        column = jnp.sum(jnp.where(lane == j, a, 0.0), axis=1, keepdims=True)
        root = lax.rsqrt(jnp.sum(jnp.where((row == j) & (lane == j), a, 0.0), keepdims=True))
        m = jnp.where(row > j, column, 0.0) * (root * root)
        return a - m * of_row(a), jnp.where(row == j, w * root, w - m * of_row(w))

    return lax.fori_loop(0, n, pivot, (a, jnp.where(row == lane, 1.0, 0.0)))[1]


def rolled_kernel(
    steps, parts_ref, own_ref, other_ref, eri_ref, diag_ref, panel_ref, new_ref,
    hi, lo, work, solved,
):
    rows, piv = eri_ref.shape
    width = piv // steps
    half = own_ref.shape[1]
    core = lax.axis_index("col")
    for c in range(2):
        both = jnp.concatenate([parts_ref[c, 0], parts_ref[c, 1]], axis=1)
        hi[c], lo[c] = split(both[:, :half])
        work[:piv, c * (piv // 2) : (c + 1) * (piv // 2)] = both[:, half:]
    at_block = lambda b: pl.ds(pl.multiple_of(b * LANES, LANES), LANES)

    def gram(b, carry):
        at = at_block(b)
        work[at, :] -= dot_t((hi[0, at], lo[0, at]), (hi[0], lo[0])) + dot_t((hi[1, at], lo[1, at]), (hi[1], lo[1]))
        return carry

    def reduce(b, carry):
        at = at_block(b)
        work[pl.ds(pl.multiple_of(piv + b * LANES, LANES), LANES), :] = eri_ref[at, :] - (
            dot_t(split(own_ref[at, :]), (hi[core], lo[core]))
            + dot_t(split(other_ref[at, :]), (hi[1 - core], lo[1 - core]))
        )
        return carry

    lax.fori_loop(0, piv // LANES, gram, 0)
    lax.fori_loop(0, rows // LANES, reduce, 0)
    new_ref[...] = diag_ref[...]
    ones = jnp.ones((SUB, width), BF16)
    f = functools.partial(lax.dot_general, dimension_numbers=ROWS_T, preferred_element_type=F32)

    def step(s, carry):
        at = pl.ds(pl.multiple_of(s * width, width), width)
        inv = split(rolled_inverse(work[at, at]))

        def solve(b, carry):
            solved[at_block(b), :] = dot_t(split(work[at_block(b), at]), inv)
            return carry

        lax.fori_loop(0, (piv + rows) // LANES, solve, 0)
        own = solved[piv:, :]
        panel_ref[:, at] = own
        high, low = split(own * own)
        new_ref[...] -= (f(ones, high) + f(ones, low))[:1]
        above = split(solved[:piv, :])

        def update(b, carry):
            work[at_block(b), :] -= dot_t(split(solved[at_block(b), :]), above)
            return carry

        lax.fori_loop(0, (piv + rows) // LANES, update, 0)
        return carry

    lax.fori_loop(0, steps, step, 0)


def rolled(steps, parts, own, other, eri, diagonal):
    rows, piv = eri.shape
    panels, new = pl.pallas_call(
        functools.partial(rolled_kernel, steps),
        out_shape=(
            jax.ShapeDtypeStruct((rows, piv), F32),
            jax.ShapeDtypeStruct((1, rows), F32),
        ),
        in_specs=[VMEM] * 5,
        out_specs=[VMEM] * 2,
        scratch_shapes=[
            pltpu.VMEM((2, piv, own.shape[1]), BF16),
            pltpu.VMEM((2, piv, own.shape[1]), BF16),
            pltpu.VMEM((piv + rows, piv), F32),
            pltpu.VMEM((piv + rows, piv // steps), F32),
        ],
        compiler_params=pltpu.CompilerParams(vmem_limit_bytes=40 * 1024 * 1024),
        name="rolled",
    )(parts, own, other, eri, diagonal[None, :])
    return panels, new[0]


def torus(chips):
    side = 1
    while 2 * (side + 1) ** 3 <= chips:
        side += 1
    return (2 * side, side, side) if 2 * side**3 == chips else (chips, 1, 1)


def slots_for(pivots, chips):
    mean = -(-pivots // chips)
    return min(LANES - 8, -(-(mean + max(12, mean // 2)) // 16) * 16)


def on_device(grid, eri_cols, old_factor, residual_diag, pivots, row_ids):
    steps, width = pivots.shape
    piv = steps * width
    chips = grid[0] * grid[1] * grid[2]
    slots = slots_for(piv, chips)
    cap = slots - 1
    ids = row_ids.reshape(-1, LANES)
    paged = pivots.reshape(-1, LANES)

    gathered = gather(grid, paged, ids, old_factor, eri_cols, residual_diag, slots)
    most = gathered[6]
    result = finish(steps, cap, gathered)
    def again(state):
        windows = (most[0, 0].astype(jnp.int32) + cap - 1) // cap

        def add(w, held):
            mine = pack(jnp.full((1,), w, jnp.int32), paged, ids, old_factor, eri_cols, slots)
            every, other = spread(grid, mine, old_factor)
            every = every.reshape(2, 2, chips, slots, -1)
            line = every[0, 0, :, slots - 1, :slots].at[:, cap].set(0.0).reshape(1, -1)
            every = every.reshape(2, 2, chips * slots, -1)
            return held[0] + place(line, every, piv), other

        empty = jnp.zeros((2, 2, piv, (old_factor.shape[1] + piv // 2) // 2), F32)
        parts, other = lax.fori_loop(0, windows, add, (empty, jnp.zeros_like(old_factor)))
        return jnp.int32(0), *rolled(steps, parts, old_factor, other, eri_cols, residual_diag)

    return lax.while_loop(lambda s: s[0] > 0, again, result)[1:]


def solution(mesh):
    grid = torus(mesh.shape["row"])
    placed = (P("row", None), P("row", "col"), P("row"), P(), P("row"))
    return jax.shard_map(
        functools.partial(on_device, grid),
        mesh=mesh, in_specs=placed, out_specs=(P("row", None), P("row")), check_vma=False,
    )
```
